32 devices in a mesh: dp: 8 (over y, x, core), blk: 4 (over z).
Axes of the slice: x: 2, y: 2, z: 4, core: 2. Of those that a mesh axis runs over, the one named last changes fastest.
Arguments:
- cell_states: bfloat16 [12288, 1024], P(('dp', 'blk')), may hold values from -16 to 16
- slide_lengths: int32 [8, 4], P('dp'), may hold values from 1 to 1024, 1536 in all within a row
- cell_mask: int32 [12288], P(('dp', 'blk')), may hold values from 0 to 1, as said below
- latent_noise: bfloat16 [12288, 512], P(('dp', 'blk')), may hold values from -4 to 4
- train_step: int32 [1], replicated, may hold values from 0 to 1999
- attn_gain: float32 [1024], replicated, may hold values from 0.5 to 1.5
- attn_shift: float32 [1024], replicated, may hold values from -0.3125 to 0.3125
- query_weight: bfloat16 [1024, 1024], replicated, may hold values from -0.1875 to 0.1875
- key_weight: bfloat16 [1024, 1024], replicated, may hold values from -0.1875 to 0.1875
- value_weight: bfloat16 [1024, 1024], replicated, may hold values from -0.1875 to 0.1875
- out_weight: bfloat16 [1024, 1024], replicated, may hold values from -3 to 3
- ffn_gain: float32 [1024], replicated, may hold values from 0.5 to 1.5
- ffn_shift: float32 [1024], replicated, may hold values from -1.75 to 1.75
- up_weight: bfloat16 [1024, 4096], replicated, may hold values from -0.1875 to 0.1875
- up_bias: float32 [4096], replicated, may hold values from -3 to 3
- down_weight: bfloat16 [4096, 1024], replicated, may hold values from -0.09375 to 0.09375
- down_bias: float32 [1024], replicated, may hold values from -1.75 to 1.75
- encode_weight: bfloat16 [1024, 1024], replicated, may hold values from -0.046875 to 0.046875
- encode_bias: float32 [1024], replicated, may hold values from -2 to 2
- decode_weight: bfloat16 [512, 1024], replicated, may hold values from -0.25 to 0.25
- prior_means: float32 [16, 512], replicated, may hold values from -6 to 6
- prior_logits: float32 [16], replicated, may hold values from -6 to 6
- out_grad: bfloat16 [12288, 1024], P(('dp', 'blk')), may hold values from -6 to 6
Outputs:
- layer_out: bfloat16 [12288, 1024], P(('dp', 'blk'))
- states_grad: float32 [12288, 1024], P(('dp', 'blk'))
- kl_per_dim: float32 [1], replicated
- attn_gain_grad: float32 [1024], P('blk')
- attn_shift_grad: float32 [1024], P('blk')
- query_weight_grad: float32 [1024, 1024], P('blk')
- key_weight_grad: float32 [1024, 1024], P('blk')
- value_weight_grad: float32 [1024, 1024], P('blk')
- out_weight_grad: float32 [1024, 1024], P('blk')
- ffn_gain_grad: float32 [1024], P('blk')
- ffn_shift_grad: float32 [1024], P('blk')
- up_weight_grad: float32 [1024, 4096], P('blk')
- up_bias_grad: float32 [4096], P('blk')
- down_weight_grad: float32 [4096, 1024], P('blk')
- down_bias_grad: float32 [1024], P('blk')
- encode_weight_grad: float32 [1024, 1024], P('blk')
- encode_bias_grad: float32 [1024], P('blk')
- decode_weight_grad: float32 [512, 1024], P('blk')
- prior_means_grad: float32 [16, 512], P(None, 'blk')
- prior_logits_grad: float32 [16], P('blk')
The draws below stay inside these ranges and needn't reach their ends.
Inputs may be any that keep to these rules, and one draw needn't show every extreme that they name: `slide_lengths`: row g holds the lengths of the 4 slides of group g in order; they sum to 1536, and the longest is exactly 1024. `cell_mask`: the last cell, 12287, is real.
All inputs are finite; a program needn't handle non-finite values.
Results may differ from the reference program's by a relative error of at most 0.035.
Values may be sent and summed in bfloat16 or wider, within the bound.
No kernel may reach another device: no remote copies, remote signals or barrier semaphores. Data moves between devices by JAX's collectives and lax.ppermute only.
A program may use at most 192 MiB of HBM per device.

```python
import math
import jax
import jax.numpy as jnp
import numpy as np
from jax import lax

D = 1024
H = 16
HD = 64
FF = 4096
LAT = 512
K = 16
C = 4
WARM = 2000
GROUP = 1536
TOKENS = 12288
MOST = 1024
N_DP = 8


def draw_cell_mask(key, part):
    place = jnp.arange(TOKENS, dtype=jnp.int32)
    ticket = jax.random.randint(key, (TOKENS,), 0, 4 * TOKENS, dtype=jnp.int32)
    return (ticket < TOKENS + 3 * place + 3).astype(jnp.int32)


def draw_cell_states(key, part):
    own_key = jax.random.fold_in(key, 7)
    place = jnp.arange(TOKENS, dtype=jnp.float32) / max(TOKENS - 1, 1)
    scale = jnp.exp(math.log(4.0) * place)
    raw = jnp.clip(jax.random.normal(own_key, (TOKENS, D), jnp.float32), -4.0, 4.0)
    return (raw * scale[:, None]).astype(jnp.bfloat16)


def block_levels(stream_key, dims, shards, smallest, top_value):
    level, own = 1.0, jax.random.fold_in(stream_key, 6)
    for dim, blocks in shards:
        draws = jnp.exp(jax.random.uniform(jax.random.fold_in(own, dim), (blocks,), jnp.float32, smallest / len(shards), top_value / len(shards)))
        level = level * jnp.repeat(draws, dims[dim] // blocks).reshape([-1 if axis == dim else 1 for axis in range(len(dims))])
    return level


def profile(count, total, reach, slope):
    loads = [(1 << 20) // math.isqrt(grade ** slope) + 1 for grade in range(2, count + 1)]
    rest, holding = total - reach - (count - 1), [1] * (count - 1)
    while rest > 0:
        free = [i for i in range(count - 1) if holding[i] < reach]
        mass, left = sum([loads[i] for i in free]), rest
        for i in free:
            more = min(reach - holding[i], max(1, left * loads[i] // mass), rest)
            holding[i] = holding[i] + more
            rest = rest - more
    return np.array([reach] + holding)


def uneven_parts(stream_key, number_of, total, bound, lean):
    if number_of == 2:
        one = jax.random.randint(stream_key, (), max(1, total - bound), min(bound, total - 1) + 1)
        return jnp.stack([one, total - one])
    lengths = jnp.asarray(profile(number_of, total, bound, lean), jnp.int32)
    couples = (number_of - 1) // 2
    source_of, sink = lengths[1:1 + 2 * couples:2], lengths[2:2 + 2 * couples:2]
    margin = jnp.minimum(source_of - 1, bound - sink)
    moved = jax.random.randint(jax.random.fold_in(stream_key, 1), (couples,), 0, 1 << 20) % (margin + 1)
    lengths = lengths.at[1:1 + 2 * couples:2].set(source_of - moved).at[2:2 + 2 * couples:2].set(sink + moved)
    return lengths[jax.random.permutation(jax.random.fold_in(stream_key, 2), number_of)]


def gaussian(rng, shape, scale, limit, cuts=(), kind=jnp.bfloat16):
    level = block_levels(rng, shape, cuts, -0.22, 0.18) if cuts else 1.0
    result = jax.random.normal(rng, shape, jnp.float32) * scale * level
    return jnp.minimum(jnp.maximum(result, -limit), limit).astype(kind)


def setup_inputs(seed: int = 0) -> dict:
    seeds = jax.random.split(jax.random.key(seed), 24)
    return {
        "cell_states": draw_cell_states(jax.random.fold_in(seeds[23], 71), 0),
        "slide_lengths": jax.vmap(lambda own: uneven_parts(own, C, GROUP, MOST, 2))(jax.random.split(seeds[1], N_DP)).reshape((N_DP, C)).astype(jnp.int32),
        "cell_mask": draw_cell_mask(jax.random.fold_in(seeds[23], 71), 0),
        "latent_noise": gaussian(seeds[3], (TOKENS, LAT), 1.0, 4.0, ((0, 32),)),
        "train_step": jax.random.randint(seeds[4], (1,), 0, WARM).astype(jnp.int32),
        "attn_gain": jnp.clip(1.0 + 0.1 * jax.random.normal(seeds[5], (D,), jnp.float32), 0.5, 1.5),
        "attn_shift": gaussian(seeds[6], (D,), 0.05, 0.3125, (), jnp.float32),
        "query_weight": gaussian(seeds[7], (D, D), D ** -0.5, 0.1875),
        "key_weight": gaussian(seeds[8], (D, D), D ** -0.5, 0.1875),
        "value_weight": gaussian(seeds[9], (D, D), D ** -0.5, 0.1875),
        "out_weight": gaussian(seeds[10], (D, D), 4 ** -0.5, 3.0),
        "ffn_gain": jnp.clip(1.0 + 0.1 * jax.random.normal(seeds[11], (D,), jnp.float32), 0.5, 1.5),
        "ffn_shift": gaussian(seeds[12], (D,), 0.3, 1.75, (), jnp.float32),
        "up_weight": gaussian(seeds[13], (D, FF), D ** -0.5, 0.1875),
        "up_bias": gaussian(seeds[14], (FF,), 0.5, 3.0, (), jnp.float32),
        "down_weight": gaussian(seeds[15], (FF, D), FF ** -0.5, 0.09375),
        "down_bias": gaussian(seeds[16], (D,), 0.3, 1.75, (), jnp.float32),
        "encode_weight": gaussian(seeds[17], (D, 2 * LAT), (16 * D) ** -0.5, 0.046875),
        "encode_bias": jnp.clip(jax.random.uniform(seeds[18], (2 * LAT,), jnp.float32, -2.0, 2.0), -2.0, 2.0),
        "decode_weight": gaussian(seeds[19], (LAT, D), LAT ** -0.5, 0.25),
        "prior_means": gaussian(seeds[20], (K, LAT), 1.0, 6.0, (), jnp.float32),
        "prior_logits": gaussian(seeds[21], (K,), 1.0, 6.0, (), jnp.float32),
        "out_grad": gaussian(seeds[22], (TOKENS, D), 1.0, 6.0, ((0, 32),)),
    }


ln_eps = 1e-05
free_floor = 1.3
neg_fill = -1e+30

@jax.custom_vjp
def low(v):
    return lax.optimization_barrier(v.astype(jnp.bfloat16)).astype(jnp.float32)

@jax.custom_vjp
def low_back(v):
    return v

def low_keep(v):
    return (low(v), None)

def low_pass(kept, grad):
    return (grad,)

def back_keep(v):
    return (v, None)

def back_low(kept, grad):
    return (low(grad),)
low.defvjp(low_keep, low_pass)
low_back.defvjp(back_keep, back_low)

def exact_dot(left, right):
    return jnp.dot(left, right, precision=lax.Precision.HIGHEST, preferred_element_type=jnp.float32)

def layer_norm(values, gain, shift):
    center = values - lax.optimization_barrier(jnp.mean(values, axis=-1, keepdims=True))
    spread = lax.optimization_barrier(jnp.mean(center * center, axis=-1, keepdims=True))
    return center * lax.rsqrt(spread + ln_eps) * gain + shift

def slide_index(position, lengths_row):
    ends = jnp.cumsum(lengths_row)
    return lax.optimization_barrier(jnp.sum((position[:, None] >= ends[None, :]).astype(jnp.int32), axis=1))

def kl_terms(latent_mean, latent_logvar, prior_means, prior_logits):
    log_prior = jax.nn.log_softmax(prior_logits)
    logits = exact_dot(latent_mean, prior_means.T) * LAT ** (-0.5) + log_prior[None, :]
    resp = jax.nn.softmax(logits, axis=-1)
    log_resp = jax.nn.log_softmax(logits, axis=-1)
    mixed_mean = exact_dot(resp, prior_means)
    mixed_square = exact_dot(resp, prior_means * prior_means)
    kl_dim = 0.5 * (jnp.exp(latent_logvar) + latent_mean * latent_mean - 2.0 * latent_mean * mixed_mean + mixed_square - 1.0 - latent_logvar)
    categorical = lax.optimization_barrier(jnp.sum(resp * (log_resp - log_prior[None, :]), axis=-1))
    return (kl_dim, categorical)

def attend_rows(query_rows, row_start, keys, values, key_slide, key_mask, lengths_row):
    rows = query_rows.shape[0]
    cells = keys.shape[0]
    row_pos = row_start + jnp.arange(rows, dtype=jnp.int32)
    key_pos = jnp.arange(cells, dtype=jnp.int32)
    row_slide = slide_index(row_pos, lengths_row)
    allowed = (row_slide[:, None] == key_slide[None, :]) & ((key_mask[None, :] == 1) | (row_pos[:, None] == key_pos[None, :]))
    heads_q = query_rows.reshape(rows, H, HD)
    heads_k = keys.reshape(cells, H, HD)
    heads_v = values.reshape(cells, H, HD)
    scores = low_back(jnp.einsum('qhd,khd->hqk', heads_q, heads_k, precision=lax.Precision.HIGHEST) * HD ** (-0.5))
    scores = jnp.where(allowed[None], scores, neg_fill)
    weights = low(jax.nn.softmax(scores, axis=-1))
    context = jnp.einsum('hqk,khd->qhd', weights, heads_v, precision=lax.Precision.HIGHEST)
    return context.reshape(rows, H * HD)

def group_forward(weights, x_rows, noise_rows, mask_rows, lengths_row):
    attn_gain, attn_shift, query_weight, key_weight, value_weight, out_weight, ffn_gain, ffn_shift, up_weight, up_bias, down_weight, down_bias, encode_weight, encode_bias, decode_weight, prior_means, prior_logits = weights
    cells = x_rows.shape[0]
    normed = low(layer_norm(x_rows, attn_gain, attn_shift))
    queries = low_back(low(exact_dot(normed, query_weight)))
    keys = low_back(low(exact_dot(normed, key_weight)))
    values = low_back(low(exact_dot(normed, value_weight)))
    key_slide = slide_index(jnp.arange(cells, dtype=jnp.int32), lengths_row)
    block = math.gcd(cells, 512)
    starts = jnp.arange(cells // block, dtype=jnp.int32) * block
    attend = jax.checkpoint(attend_rows)
    context = lax.map(lambda item: attend(item[0], item[1], keys, values, key_slide, mask_rows, lengths_row), (queries.reshape(cells // block, block, H * HD), starts)).reshape(cells, H * HD)
    context = low_back(low(context))
    hidden = x_rows + low_back(exact_dot(context, out_weight))
    normed_two = low(layer_norm(hidden, ffn_gain, ffn_shift))
    inner = low_back(exact_dot(normed_two, up_weight) + up_bias)
    activated = low(jax.nn.gelu(inner, approximate=False))
    hidden_two = hidden + low_back(exact_dot(activated, down_weight)) + down_bias
    encoded = low_back(exact_dot(low(hidden_two), encode_weight) + encode_bias)
    latent_mean = encoded[:, :LAT]
    latent_logvar = encoded[:, LAT:]
    latent = low(latent_mean + jnp.exp(0.5 * latent_logvar) * noise_rows)
    output = hidden_two + exact_dot(latent, decode_weight)
    kl_dim, categorical = kl_terms(latent_mean, latent_logvar, prior_means, prior_logits)
    real = mask_rows.astype(jnp.float32)
    return (output, lax.optimization_barrier(jnp.sum(kl_dim * real[:, None], axis=0)), jnp.sum(categorical * real), jnp.sum(real))

def reference(cell_states, slide_lengths, cell_mask, latent_noise, train_step, attn_gain, attn_shift, query_weight, key_weight, value_weight, out_weight, ffn_gain, ffn_shift, up_weight, up_bias, down_weight, down_bias, encode_weight, encode_bias, decode_weight, prior_means, prior_logits, out_grad):
    groups = slide_lengths.shape[0]
    cells = cell_states.shape[0] // groups
    weights = tuple((item.astype(jnp.float32) for item in (attn_gain, attn_shift, query_weight, key_weight, value_weight, out_weight, ffn_gain, ffn_shift, up_weight, up_bias, down_weight, down_bias, encode_weight, encode_bias, decode_weight, prior_means, prior_logits)))
    x_groups = cell_states.astype(jnp.float32).reshape(groups, cells, D)
    noise_groups = latent_noise.astype(jnp.float32).reshape(groups, cells, LAT)
    mask_groups = cell_mask.reshape(groups, cells)
    grad_groups = out_grad.astype(jnp.float32).reshape(groups, cells, D)
    beta = jnp.minimum(1.0, (train_step[0].astype(jnp.float32) + 1.0) / WARM)

    def total_loss(x_all, params):

        def one_group(carry, item):
            x_rows, noise_rows, mask_rows, lengths_row, grad_rows = item
            output, kl_sum, cat_sum, count = group_forward(params, x_rows, noise_rows, mask_rows, lengths_row)
            return (carry, (output, kl_sum, cat_sum, count, jnp.sum(output * grad_rows)))
        _, (outputs, kl_sums, cat_sums, counts, products) = lax.scan(jax.checkpoint(one_group), jnp.zeros((), jnp.float32), (x_all, noise_groups, mask_groups, slide_lengths, grad_groups))
        count = jnp.sum(counts)
        floored = jnp.sum(jnp.maximum(lax.optimization_barrier(jnp.sum(kl_sums, axis=0)) / count, free_floor))
        cat_mean = jnp.sum(cat_sums) / count
        kl_value = floored + cat_mean
        loss = jnp.sum(products) + beta * count * kl_value
        return (loss, (outputs, floored / LAT + cat_mean))
    loss, pullback, (outputs, kl_report) = jax.vjp(total_loss, x_groups, weights, has_aux=True)
    states_grad, weight_grads = pullback(jnp.ones((), jnp.float32))
    layer_out = outputs.reshape(groups * cells, D).astype(jnp.bfloat16)
    kl_out = kl_report.reshape(1)
    return (layer_out, states_grad.reshape(groups * cells, D), kl_out, weight_grads[0], weight_grads[1], weight_grads[2], weight_grads[3], weight_grads[4], weight_grads[5], weight_grads[6], weight_grads[7], weight_grads[8], weight_grads[9], weight_grads[10], weight_grads[11], weight_grads[12], weight_grads[13], weight_grads[14], weight_grads[15], weight_grads[16])
```

```python
from functools import partial

import jax
import jax.numpy as jnp
from jax import lax
from jax.sharding import PartitionSpec as P

D = 1024
H = 16
HD = 64
LAT = 512
K = 16
WARM = 2000


ln_eps = 1e-05
free_floor = 1.3
neg_fill = -1e30


def shortened(array):

    def short(part):
        return part.astype(jnp.bfloat16) if part.dtype == jnp.float32 else part

    return jax.tree.map(short, array)


def passed_along(value, axis, steps):
    count = lax.axis_size(axis)
    pairs = [(source, (source + steps) % count) for source in range(count)]
    return lax.ppermute(value, axis, pairs)


def layer_norm(values, gain, shift):
    center = values - jnp.mean(values, axis=-1, keepdims=True)
    spread = jnp.mean(center * center, axis=-1, keepdims=True)
    return center * lax.rsqrt(spread + ln_eps) * gain + shift


def slide_index(position, lengths_row):
    ends = jnp.cumsum(lengths_row)
    return jnp.sum((position[:, None] >= ends[None, :]).astype(jnp.int32), axis=1)


def exact_dot(left, right):
    return jnp.dot(left, right, precision=lax.Precision.HIGHEST, preferred_element_type=jnp.float32)


def kl_terms(latent_mean, latent_logvar, prior_means, prior_logits):
    log_prior = jax.nn.log_softmax(prior_logits)
    logits = exact_dot(latent_mean, prior_means.T) * LAT ** (-0.5) + log_prior[None, :]
    resp = jax.nn.softmax(logits, axis=-1)
    log_resp = jax.nn.log_softmax(logits, axis=-1)
    mixed_mean = exact_dot(resp, prior_means)
    mixed_square = exact_dot(resp, prior_means * prior_means)
    kl_dim = 0.5 * (
        jnp.exp(latent_logvar)
        + latent_mean * latent_mean
        - 2.0 * latent_mean * mixed_mean
        + mixed_square
        - 1.0
        - latent_logvar
    )
    categorical = jnp.sum(resp * (log_resp - log_prior[None, :]), axis=-1)
    return (kl_dim, categorical)


def plain_dot(left, right):
    return jnp.dot(left, right, preferred_element_type=jnp.float32)


def rows_dot(left, right):
    return lax.dot_general(
        left, right, (((0,), (0,)), ((), ())), preferred_element_type=jnp.float32
    )


def cols_dot(left, right):
    return lax.dot_general(
        left, right, (((1,), (1,)), ((), ())), preferred_element_type=jnp.float32
    )


def pair_mask(query_slide, query_pos, key_slide, key_pos, key_live):
    same = query_slide[:, None] == key_slide[None, :]
    open_key = (key_live[None, :] > 0.5) | (query_pos[:, None] == key_pos[None, :])
    return (same & open_key)[None]


def forward_update(
    state, heads_q, query_slide, query_pos, heads_k, heads_v, key_live, key_pos, key_slide
):
    peak, total, running = state
    allowed = pair_mask(query_slide, query_pos, key_slide, key_pos, key_live)
    scores = jnp.einsum(
        "qhd,khd->hqk", heads_q, heads_k, preferred_element_type=jnp.float32
    ) * HD ** (-0.5)
    scores = jnp.where(allowed, scores, neg_fill)
    new_peak = jnp.maximum(peak, jnp.max(scores, axis=-1))
    weights = jnp.where(allowed, jnp.exp(scores - new_peak[:, :, None]), 0.0)
    rescale = jnp.exp(peak - new_peak)
    total = total * rescale + jnp.sum(weights, axis=-1)
    running = running * rescale.T[:, :, None] + jnp.einsum(
        "hqk,khd->qhd", weights.astype(jnp.bfloat16), heads_v, preferred_element_type=jnp.float32
    )
    return (new_peak, total, running)


def forward_visit(
    state, heads_q, query_slide, query_pos, heads_k, heads_v, key_live, key_pos, lengths_row
):
    key_slide = slide_index(key_pos, lengths_row)
    return forward_update(
        state, heads_q, query_slide, query_pos, heads_k, heads_v, key_live, key_pos, key_slide
    )


def backward_update(
    heads_q,
    heads_o,
    log_total,
    delta,
    query_slide,
    query_pos,
    heads_k,
    heads_v,
    key_live,
    key_pos,
    key_slide,
):
    allowed = pair_mask(query_slide, query_pos, key_slide, key_pos, key_live)
    scores = jnp.einsum(
        "qhd,khd->hqk", heads_q, heads_k, preferred_element_type=jnp.float32
    ) * HD ** (-0.5)
    probs = jnp.where(allowed, jnp.exp(scores - log_total[:, :, None]), 0.0)
    dprobs = jnp.einsum("qhd,khd->hqk", heads_o, heads_v, preferred_element_type=jnp.float32)
    dscores = (probs * (dprobs - delta[:, :, None])).astype(jnp.bfloat16)
    grad_q = jnp.einsum(
        "hqk,khd->qhd", dscores, heads_k, preferred_element_type=jnp.float32
    ) * HD ** (-0.5)
    grad_k = jnp.einsum(
        "hqk,qhd->khd", dscores, heads_q, preferred_element_type=jnp.float32
    ) * HD ** (-0.5)
    grad_v = jnp.einsum(
        "hqk,qhd->khd", probs.astype(jnp.bfloat16), heads_o, preferred_element_type=jnp.float32
    )
    return (grad_q, grad_k, grad_v)


def backward_visit(
    heads_q,
    heads_o,
    log_total,
    delta,
    query_slide,
    query_pos,
    heads_k,
    heads_v,
    key_live,
    key_pos,
    key_slide,
):
    return backward_update(
        heads_q,
        heads_o,
        log_total,
        delta,
        query_slide,
        query_pos,
        heads_k,
        heads_v,
        key_live,
        key_pos,
        key_slide,
    )


MESH_AXES = ("dp", "blk")


def swapped(value, dp_mask, blk_mask):
    groups, blocks = lax.axis_size("dp"), lax.axis_size("blk")
    pairs = [
        (g * blocks + b, (g ^ dp_mask) * blocks + (b ^ blk_mask))
        for g in range(groups)
        for b in range(blocks)
    ]
    return lax.ppermute(value, MESH_AXES, pairs)


def bits_of(count):
    return count.bit_length() - 1


def dp_masks():
    return [1 << t for t in range(bits_of(lax.axis_size("dp")))]


def blk_masks():
    return [(2 << t) - 1 for t in range(bits_of(lax.axis_size("blk")))]


def blk_sides(index):
    count = bits_of(lax.axis_size("blk"))
    return [((index >> t) ^ (index >> (t + 1))) & 1 for t in range(count)]


def blk_leaf_order():
    blocks = lax.axis_size("blk")
    order = [0] * blocks
    for index in range(blocks):
        leaf = 0
        for side in blk_sides(index):
            leaf = 2 * leaf + side
        order[leaf] = index
    return order


def summed_everywhere(value):
    for mask in dp_masks():
        value = value + swapped(value, mask, 0)
    for mask in blk_masks():
        value = value + swapped(value, 0, mask)
    return value


def halves(value, side, axis):
    size = value.shape[axis] // 2
    keep = lax.dynamic_slice_in_dim(value, side * size, size, axis)
    send = lax.dynamic_slice_in_dim(value, (1 - side) * size, size, axis)
    return keep, send


def added(left, right):
    return (left.astype(jnp.float32) + right.astype(jnp.float32)).astype(jnp.bfloat16)


def joined(mine, other, side, axis):
    first = jnp.where(side == 0, mine, other)
    second = jnp.where(side == 0, other, mine)
    return jnp.concatenate([first, second], axis=axis)


def reduced(grad, flipped):
    blocks = lax.axis_size("blk")
    group, block = lax.axis_index("dp"), lax.axis_index("blk")
    rows, cols = grad.shape
    value = grad.astype(jnp.bfloat16).reshape(blocks, rows // blocks, cols)
    steps = dp_masks()
    if flipped:
        steps = steps[:1] + steps[1:][::-1]
    sides = [(group // mask) % 2 for mask in steps]
    for mask, side in zip(steps, sides):
        keep, send = halves(value, side, 1)
        value = added(keep, swapped(send, mask, 0))
    value = jnp.stack([value[index] for index in blk_leaf_order()])
    for mask, side in zip(blk_masks(), blk_sides(block)):
        keep, send = halves(value, side, 0)
        value = added(keep, swapped(send, 0, mask))
    value = value[0]
    for mask, side in reversed(list(zip(steps, sides))):
        value = joined(value, swapped(value, mask, 0), side, 0)
    return value.astype(jnp.float32)


def reduced_small(parts):
    block = lax.axis_index("blk")
    sizes = [part.shape[1] for part in parts]
    total = sum(sizes)
    padded = -(-total // 1024) * 1024
    value = jnp.concatenate(parts, axis=1)
    value = jnp.pad(value, ((0, 0), (0, padded - total)))
    value = jnp.stack([value[index] for index in blk_leaf_order()])
    for mask, side in zip(blk_masks(), blk_sides(block)):
        keep, send = halves(value, side, 0)
        value = keep + swapped(send, 0, mask)
    value = value[0]
    for mask in dp_masks():
        value = value + swapped(value, mask, 0)
    pieces, start = [], 0
    for size in sizes:
        pieces.append(value[start : start + size])
        start += size
    return pieces


def local(
    cell_states,
    slide_lengths,
    cell_mask,
    latent_noise,
    train_step,
    attn_gain,
    attn_shift,
    query_weight,
    key_weight,
    value_weight,
    out_weight,
    ffn_gain,
    ffn_shift,
    up_weight,
    up_bias,
    down_weight,
    down_bias,
    encode_weight,
    encode_bias,
    decode_weight,
    prior_means,
    prior_logits,
    out_grad,
):
    rows_here = cell_states.shape[0]
    blocks = lax.axis_size("blk")
    my_index = lax.axis_index("blk")
    lengths_row = slide_lengths[0]
    local_range = jnp.arange(rows_here, dtype=jnp.int32)
    local_pos = my_index * rows_here + local_range
    local_slide = slide_index(local_pos, lengths_row)
    live = cell_mask.astype(jnp.bfloat16)
    x_float = cell_states.astype(jnp.float32)
    normed, norm_back = jax.vjp(layer_norm, x_float, attn_gain, attn_shift)
    normed_b = normed.astype(jnp.bfloat16)
    queries = plain_dot(normed_b, query_weight).astype(jnp.bfloat16)
    keys = plain_dot(normed_b, key_weight).astype(jnp.bfloat16)
    values = plain_dot(normed_b, value_weight).astype(jnp.bfloat16)
    heads_q = queries.reshape(rows_here, H, HD)
    start_state = (
        jnp.full((H, rows_here), neg_fill, jnp.float32),
        jnp.zeros((H, rows_here), jnp.float32),
        jnp.zeros((rows_here, H, HD), jnp.float32),
    )
    state = start_state
    piece_keys = lax.all_gather(keys, "blk", axis=0, tiled=True)
    piece_values = lax.all_gather(values, "blk", axis=0, tiled=True)
    piece_live = lax.all_gather(live, "blk", axis=0, tiled=True)
    rows = piece_keys.shape[0]
    width = min(rows, rows_here)

    def one_block(carry, index):
        offset = index * width
        block_keys = lax.dynamic_slice_in_dim(piece_keys, offset, width, 0).reshape(width, H, HD)
        block_values = lax.dynamic_slice_in_dim(piece_values, offset, width, 0).reshape(
            width, H, HD
        )
        block_live = lax.dynamic_slice_in_dim(piece_live, offset, width, 0)
        key_pos = offset + jnp.arange(width, dtype=jnp.int32)
        return (
            forward_visit(
                carry,
                heads_q,
                local_slide,
                local_pos,
                block_keys,
                block_values,
                block_live,
                key_pos,
                lengths_row,
            ),
            None,
        )

    state, _ = lax.scan(one_block, state, jnp.arange(rows // width, dtype=jnp.int32))
    peak, total, running = state
    context = running / total.T[:, :, None]
    log_total = peak + jnp.log(total)
    context_b = context.reshape(rows_here, D).astype(jnp.bfloat16)
    hidden = x_float + plain_dot(context_b, out_weight)
    normed_two, norm_two_back = jax.vjp(layer_norm, hidden, ffn_gain, ffn_shift)
    normed_two_b = normed_two.astype(jnp.bfloat16)
    inner = plain_dot(normed_two_b, up_weight) + up_bias
    activated, gelu_back = jax.vjp(partial(jax.nn.gelu, approximate=False), inner)
    activated_b = activated.astype(jnp.bfloat16)
    hidden_two = hidden + plain_dot(activated_b, down_weight) + down_bias
    hidden_two_b = hidden_two.astype(jnp.bfloat16)
    encoded = plain_dot(hidden_two_b, encode_weight) + encode_bias
    latent_mean = encoded[:, :LAT]
    latent_logvar = encoded[:, LAT:]
    spread = jnp.exp(0.5 * latent_logvar)
    noise_float = latent_noise.astype(jnp.float32)
    latent_b = (latent_mean + spread * noise_float).astype(jnp.bfloat16)
    output = hidden_two + plain_dot(latent_b, decode_weight)
    (kl_dim, categorical), kl_back = jax.vjp(
        kl_terms, latent_mean, latent_logvar, prior_means, prior_logits
    )
    real = cell_mask.astype(jnp.float32)
    sums = jnp.concatenate(
        [
            jnp.sum(kl_dim * real[:, None], axis=0),
            jnp.sum(categorical * real)[None],
            jnp.sum(real)[None],
            jnp.zeros((126,), jnp.float32),
        ]
    )
    sums = summed_everywhere(sums)
    kl_sum, cat_sum, count = sums[:LAT], sums[LAT], sums[LAT + 1]
    kbar = kl_sum / count
    floored = jnp.sum(jnp.maximum(kbar, free_floor))
    cat_mean = cat_sum / count
    beta = jnp.minimum(1.0, (train_step[0].astype(jnp.float32) + 1.0) / WARM)
    active = (kbar > free_floor).astype(jnp.float32)
    grad_decode = rows_dot(latent_b, out_grad)
    grad_latent = cols_dot(out_grad, decode_weight)
    grad_mean, grad_logvar, grad_means, grad_prior = kl_back(
        (beta * real[:, None] * active[None, :], beta * real)
    )
    grad_mean = grad_mean + grad_latent
    grad_logvar = grad_logvar + grad_latent * 0.5 * spread * noise_float
    grad_encoded_b = jnp.concatenate([grad_mean, grad_logvar], axis=1).astype(jnp.bfloat16)
    grad_encode = rows_dot(hidden_two_b, grad_encoded_b)
    grad_encode_bias = jnp.sum(grad_encoded_b.astype(jnp.float32), axis=0)
    grad_two = out_grad.astype(jnp.float32) + cols_dot(grad_encoded_b, encode_weight)
    grad_down_bias = jnp.sum(grad_two, axis=0)
    grad_branch_b = grad_two.astype(jnp.bfloat16)
    grad_down = rows_dot(activated_b, grad_branch_b)
    (grad_inner,) = gelu_back(cols_dot(grad_branch_b, down_weight))
    grad_inner_b = grad_inner.astype(jnp.bfloat16)
    grad_up_bias = jnp.sum(grad_inner_b.astype(jnp.float32), axis=0)
    grad_up = rows_dot(normed_two_b, grad_inner_b)
    grad_hidden, grad_ffn_gain, grad_ffn_shift = norm_two_back(cols_dot(grad_inner_b, up_weight))
    grad_hidden = grad_hidden + grad_two
    grad_attn_b = grad_hidden.astype(jnp.bfloat16)
    grad_out = rows_dot(context_b, grad_attn_b)
    grad_context_b = cols_dot(grad_attn_b, out_weight).astype(jnp.bfloat16)
    heads_o = grad_context_b.reshape(rows_here, H, HD)
    delta = jnp.sum(heads_o.astype(jnp.float32) * context, axis=-1).T
    zero_heads = jnp.zeros((rows_here, H, HD), jnp.float32)

    def key_turn(turn, carry):
        travel, grads_travel, grad_q = carry
        held_keys, held_values, held_live = travel
        anchor = (my_index + turn) % blocks
        key_pos = anchor * rows_here + local_range
        key_slide = slide_index(key_pos, lengths_row)
        part_q, part_k, part_v = backward_visit(
            heads_q,
            heads_o,
            log_total,
            delta,
            local_slide,
            local_pos,
            held_keys.reshape(rows_here, H, HD),
            held_values.reshape(rows_here, H, HD),
            held_live,
            key_pos,
            key_slide,
        )
        grads_travel = (grads_travel[0] + part_k, grads_travel[1] + part_v)
        travel = jax.tree.map(
            lambda part, own: part.astype(own.dtype),
            passed_along(shortened(travel), "blk", -1),
            travel,
        )
        grads_travel = (
            passed_along(grads_travel[0].astype(jnp.bfloat16), "blk", -1).astype(jnp.float32),
            passed_along(grads_travel[1].astype(jnp.bfloat16), "blk", -1).astype(jnp.float32),
        )
        return (travel, grads_travel, grad_q + part_q)

    _, (grad_k, grad_v), grad_q = lax.fori_loop(
        0, blocks, key_turn, ((keys, values, live), (zero_heads, zero_heads), zero_heads)
    )
    grad_q_b = grad_q.reshape(rows_here, D).astype(jnp.bfloat16)
    grad_k_b = grad_k.reshape(rows_here, D).astype(jnp.bfloat16)
    grad_v_b = grad_v.reshape(rows_here, D).astype(jnp.bfloat16)
    grad_query = rows_dot(normed_b, grad_q_b)
    grad_key = rows_dot(normed_b, grad_k_b)
    grad_value = rows_dot(normed_b, grad_v_b)
    grad_normed = (
        cols_dot(grad_q_b, query_weight)
        + cols_dot(grad_k_b, key_weight)
        + cols_dot(grad_v_b, value_weight)
    )
    grad_from_norm, grad_attn_gain, grad_attn_shift = norm_back(grad_normed)
    states_grad = grad_hidden + grad_from_norm
    by_block = lambda part: part.reshape(blocks, -1)
    means_block = jnp.moveaxis(grad_means.reshape(K, blocks, LAT // blocks), 1, 0)
    small = reduced_small(
        [
            by_block(grad_attn_gain),
            by_block(grad_attn_shift),
            by_block(grad_ffn_gain),
            by_block(grad_ffn_shift),
            by_block(grad_up_bias),
            by_block(grad_down_bias),
            by_block(grad_encode_bias),
            by_block(means_block),
            by_block(grad_prior),
        ]
    )
    totals = (
        small[0],
        small[1],
        reduced(grad_query, False),
        reduced(grad_key, True),
        reduced(grad_value, False),
        reduced(grad_out, True),
        small[2],
        small[3],
        reduced(grad_up, True),
        small[4],
        reduced(grad_down, False),
        small[5],
        reduced(grad_encode, True),
        small[6],
        reduced(grad_decode, False),
        small[7].reshape(K, LAT // blocks),
        small[8],
    )
    kl_out = (floored / LAT + cat_mean).reshape(1)
    return (output.astype(jnp.bfloat16), states_grad, kl_out) + tuple(totals)


def solution(mesh):
    in_specs = (
        P(("dp", "blk"), None),
        P("dp", None),
        P(("dp", "blk")),
        P(("dp", "blk"), None),
        P(),
        P(),
        P(),
        P(),
        P(),
        P(),
        P(),
        P(),
        P(),
        P(),
        P(),
        P(),
        P(),
        P(),
        P(),
        P(),
        P(),
        P(),
        P(("dp", "blk"), None),
    )
    out_specs = (
        P(("dp", "blk"), None),
        P(("dp", "blk"), None),
        P(),
        P("blk"),
        P("blk"),
        P("blk", None),
        P("blk", None),
        P("blk", None),
        P("blk", None),
        P("blk"),
        P("blk"),
        P("blk", None),
        P("blk"),
        P("blk", None),
        P("blk"),
        P("blk", None),
        P("blk"),
        P("blk", None),
        P(None, "blk"),
        P("blk"),
    )
    return jax.shard_map(local, mesh=mesh, in_specs=in_specs, out_specs=out_specs, check_vma=False)
```

```python
import math
from functools import partial

import jax
import jax.numpy as jnp
from jax import lax
from jax.experimental import pallas as pl
from jax.experimental.pallas import tpu as pltpu
from jax.sharding import PartitionSpec as P

D = 1024
H = 16
HD = 64
LAT = 512
K = 16
WARM = 2000


ln_eps = 1e-05
free_floor = 1.3
neg_fill = -1e30

QUERY_TILE = 512
KEY_TILE = 512
KEY_UNIT = 128


def layer_norm(values, gain, shift):
    center = values - jnp.mean(values, axis=-1, keepdims=True)
    spread = jnp.mean(center * center, axis=-1, keepdims=True)
    return center * lax.rsqrt(spread + ln_eps) * gain + shift


def slide_index(position, lengths_row):
    ends = jnp.cumsum(lengths_row)
    return jnp.sum((position[:, None] >= ends[None, :]).astype(jnp.int32), axis=1)


def exact_dot(left, right):
    return jnp.dot(left, right, precision=lax.Precision.HIGHEST, preferred_element_type=jnp.float32)


def kl_terms(latent_mean, latent_logvar, prior_means, prior_logits):
    log_prior = jax.nn.log_softmax(prior_logits)
    logits = exact_dot(latent_mean, prior_means.T) * LAT ** (-0.5) + log_prior[None, :]
    resp = jax.nn.softmax(logits, axis=-1)
    log_resp = jax.nn.log_softmax(logits, axis=-1)
    mixed_mean = exact_dot(resp, prior_means)
    mixed_square = exact_dot(resp, prior_means * prior_means)
    kl_dim = 0.5 * (
        jnp.exp(latent_logvar)
        + latent_mean * latent_mean
        - 2.0 * latent_mean * mixed_mean
        + mixed_square
        - 1.0
        - latent_logvar
    )
    categorical = jnp.sum(resp * (log_resp - log_prior[None, :]), axis=-1)
    return (kl_dim, categorical)


def plain_dot(left, right):
    return jnp.dot(left, right, preferred_element_type=jnp.float32)


def rows_dot(left, right):
    return lax.dot_general(
        left, right, (((0,), (0,)), ((), ())), preferred_element_type=jnp.float32
    )


def cols_dot(left, right):
    return lax.dot_general(
        left, right, (((1,), (1,)), ((), ())), preferred_element_type=jnp.float32
    )


MESH_AXES = ("dp", "blk")


def swapped(value, dp_mask, blk_mask):
    groups, blocks = lax.axis_size("dp"), lax.axis_size("blk")
    pairs = [
        (g * blocks + b, (g ^ dp_mask) * blocks + (b ^ blk_mask))
        for g in range(groups)
        for b in range(blocks)
    ]
    return lax.ppermute(value, MESH_AXES, pairs)


def bits_of(count):
    return count.bit_length() - 1


def dp_masks():
    return [1 << t for t in range(bits_of(lax.axis_size("dp")))]


def blk_masks():
    return [(2 << t) - 1 for t in range(bits_of(lax.axis_size("blk")))]


def blk_sides(index):
    count = bits_of(lax.axis_size("blk"))
    return [((index >> t) ^ (index >> (t + 1))) & 1 for t in range(count)]


def blk_leaf_order():
    blocks = lax.axis_size("blk")
    order = [0] * blocks
    for index in range(blocks):
        leaf = 0
        for side in blk_sides(index):
            leaf = 2 * leaf + side
        order[leaf] = index
    return order


def summed_everywhere(value):
    for mask in dp_masks():
        value = value + swapped(value, mask, 0)
    for mask in blk_masks():
        value = value + swapped(value, 0, mask)
    return value


def halves(value, side, axis):
    size = value.shape[axis] // 2
    keep = lax.dynamic_slice_in_dim(value, side * size, size, axis)
    send = lax.dynamic_slice_in_dim(value, (1 - side) * size, size, axis)
    return keep, send


def added(left, right):
    return (left.astype(jnp.float32) + right.astype(jnp.float32)).astype(jnp.bfloat16)


def joined(mine, other, side, axis):
    first = jnp.where(side == 0, mine, other)
    second = jnp.where(side == 0, other, mine)
    return jnp.concatenate([first, second], axis=axis)


def reduced(grad, flipped):
    blocks = lax.axis_size("blk")
    group, block = lax.axis_index("dp"), lax.axis_index("blk")
    rows, cols = grad.shape
    value = grad.astype(jnp.bfloat16).reshape(blocks, rows // blocks, cols)
    steps = dp_masks()
    if flipped:
        steps = steps[:1] + steps[1:][::-1]
    sides = [(group // mask) % 2 for mask in steps]
    for mask, side in zip(steps, sides):
        keep, send = halves(value, side, 1)
        value = added(keep, swapped(send, mask, 0))
    value = jnp.stack([value[index] for index in blk_leaf_order()])
    for mask, side in zip(blk_masks(), blk_sides(block)):
        keep, send = halves(value, side, 0)
        value = added(keep, swapped(send, 0, mask))
    value = value[0]
    for mask, side in reversed(list(zip(steps, sides))):
        value = joined(value, swapped(value, mask, 0), side, 0)
    return value.astype(jnp.float32)


def reduced_small(parts):
    block = lax.axis_index("blk")
    sizes = [part.shape[1] for part in parts]
    total = sum(sizes)
    padded = -(-total // 1024) * 1024
    value = jnp.concatenate(parts, axis=1)
    value = jnp.pad(value, ((0, 0), (0, padded - total)))
    value = jnp.stack([value[index] for index in blk_leaf_order()])
    for mask, side in zip(blk_masks(), blk_sides(block)):
        keep, send = halves(value, side, 0)
        value = keep + swapped(send, 0, mask)
    value = value[0]
    for mask in dp_masks():
        value = value + swapped(value, mask, 0)
    pieces, start = [], 0
    for size in sizes:
        pieces.append(value[start : start + size])
        start += size
    return pieces


def head_lanes(value, head):
    lane = lax.broadcasted_iota(jnp.int32, value.shape, 1) // HD
    return jnp.where(lane == head, value, jnp.zeros_like(value))

def nt_dot(left, right):
    return lax.dot_general(left, right, (((1,),(1,)),((),())), preferred_element_type=jnp.float32)

def nn_dot(left, right):
    return lax.dot_general(left, right, (((1,),(0,)),((),())), preferred_element_type=jnp.float32)

def allowed_pairs(code_k, code_q, block_k, tile):
    key_pos = block_k + lax.broadcasted_iota(jnp.int32, tile, 0)
    query_pos = pl.program_id(0) * QUERY_TILE + lax.broadcasted_iota(jnp.int32, tile, 1)
    return (code_k == code_q) | (key_pos == query_pos)

def forward_kernel(range_ref, q_ref, k_ref, vt_ref, cq_ref, ck_ref, ctx_ref, lse_ref, m_ref, l_ref, acc_ref):
    nh = q_ref.shape[1] // HD
    step = pl.program_id(0)
    m_ref[...] = jnp.full(m_ref.shape, neg_fill, jnp.float32)
    l_ref[...] = jnp.zeros(l_ref.shape, jnp.float32)
    acc_ref[...] = jnp.zeros(acc_ref.shape, jnp.float32)
    code_q = cq_ref[...]
    scaled = (q_ref[...].astype(jnp.float32) * HD ** (-0.5)).astype(jnp.bfloat16)
    def body(kb, _):
        start = pl.multiple_of(range_ref[step, 0] * KEY_UNIT + kb * KEY_TILE, KEY_UNIT)
        keys = k_ref[pl.ds(start, KEY_TILE), :]
        open_pair = allowed_pairs(ck_ref[pl.ds(start, KEY_TILE), :], code_q, start, (KEY_TILE, QUERY_TILE))
        for h in range(nh):
            s = nt_dot(keys, head_lanes(scaled, h))
            s = jnp.where(open_pair, s, neg_fill)
            m_old = m_ref[h:h+1, :]
            m_new = jnp.maximum(m_old, jnp.max(s, axis=0, keepdims=True))
            p = jnp.exp(s - m_new)
            alpha = jnp.exp(m_old - m_new)
            l_ref[h:h+1, :] = l_ref[h:h+1, :] * alpha + jnp.sum(p, axis=0, keepdims=True)
            m_ref[h:h+1, :] = m_new
            rows = slice(h*HD, (h+1)*HD)
            acc_ref[rows, :] = acc_ref[rows, :] * alpha + nn_dot(vt_ref[rows, pl.ds(start, KEY_TILE)], p.astype(jnp.bfloat16))
        return 0
    lax.fori_loop(0, range_ref[step, 1], body, 0)
    for h in range(nh):
        rows = slice(h*HD, (h+1)*HD)
        acc_ref[rows, :] = acc_ref[rows, :] / l_ref[h:h+1, :]
    ctx_ref[...] = acc_ref[...].T.astype(jnp.bfloat16)
    lse_ref[...] = m_ref[...] + jnp.log(l_ref[...])

def attention_forward(ranges, q, k, vt, code_q, code_k):
    N, W = q.shape
    nh = W // HD
    full = lambda shape: pl.BlockSpec(shape, lambda i, r: (0,)*len(shape))
    return pl.pallas_call(
        forward_kernel,
        out_shape=(jax.ShapeDtypeStruct((N, W), jnp.bfloat16), jax.ShapeDtypeStruct((nh, N), jnp.float32)),
        grid_spec=pltpu.PrefetchScalarGridSpec(
            num_scalar_prefetch=1, grid=(N//QUERY_TILE,),
            in_specs=[pl.BlockSpec((QUERY_TILE, W), lambda i, r: (i, 0)), full((N, W)), full((W, N)),
                      pl.BlockSpec((1, QUERY_TILE), lambda i, r: (0, i)), full((N, 1))],
            out_specs=[pl.BlockSpec((QUERY_TILE, W), lambda i, r: (i, 0)), pl.BlockSpec((nh, QUERY_TILE), lambda i, r: (0, i))],
            scratch_shapes=[pltpu.VMEM((nh, QUERY_TILE), jnp.float32), pltpu.VMEM((nh, QUERY_TILE), jnp.float32), pltpu.VMEM((W, QUERY_TILE), jnp.float32)]),
        name="attention_forward",
    )(ranges, q, k, vt, code_q, code_k)

def backward_kernel(range_ref, q_ref, do_ref, ctx_ref, lse_ref, k_ref, v_ref, kt_ref, cq_ref, ck_ref,
                    dq_ref, dk_ref, dv_ref, dqt_ref, dk_acc, dv_acc):
    nh = q_ref.shape[1] // HD
    step = pl.program_id(0)
    @pl.when(step == 0)
    def _():
        dk_acc[...] = jnp.zeros(dk_acc.shape, jnp.float32)
        dv_acc[...] = jnp.zeros(dv_acc.shape, jnp.float32)
    dqt_ref[...] = jnp.zeros(dqt_ref.shape, jnp.float32)
    code_q = cq_ref[...]
    scaled = (q_ref[...].astype(jnp.float32) * HD ** (-0.5)).astype(jnp.bfloat16)
    grads = do_ref[...]
    product = (grads.astype(jnp.float32) * ctx_ref[...].astype(jnp.float32)).T
    deltas = [jnp.sum(product[h*HD:(h+1)*HD, :], axis=0, keepdims=True) for h in range(nh)]
    q_all = jnp.concatenate([head_lanes(scaled, h) for h in range(nh)], axis=0)
    do_all = jnp.concatenate([head_lanes(grads, h) for h in range(nh)], axis=0)
    def body(kb, _):
        start = pl.multiple_of(range_ref[step, 0] * KEY_UNIT + kb * KEY_TILE, KEY_UNIT)
        keys = k_ref[pl.ds(start, KEY_TILE), :]
        values = v_ref[pl.ds(start, KEY_TILE), :]
        open_pair = allowed_pairs(ck_ref[pl.ds(start, KEY_TILE), :], code_q, start, (KEY_TILE, QUERY_TILE))
        ps, dss = [], []
        for h in range(nh):
            cols = slice(h*QUERY_TILE, (h+1)*QUERY_TILE)
            rows = slice(h*HD, (h+1)*HD)
            s = nt_dot(keys, q_all[cols, :])
            p = jnp.where(open_pair, jnp.exp(s - lse_ref[h:h+1, :]), 0.0)
            dp = nt_dot(values, do_all[cols, :])
            ds = (p * (dp - deltas[h])).astype(jnp.bfloat16)
            ps.append(p.astype(jnp.bfloat16))
            dss.append(ds)
            dqt_ref[rows, :] += nn_dot(kt_ref[rows, pl.ds(start, KEY_TILE)], ds)
        dv_acc[pl.ds(start, KEY_TILE), :] += nn_dot(jnp.concatenate(ps, axis=1), do_all)
        dk_acc[pl.ds(start, KEY_TILE), :] += nn_dot(jnp.concatenate(dss, axis=1), q_all)
        return 0
    lax.fori_loop(0, range_ref[step, 1], body, 0)
    dq_ref[...] = (dqt_ref[...] * HD ** (-0.5)).T.astype(jnp.bfloat16)
    @pl.when(step == pl.num_programs(0) - 1)
    def _():
        dk_ref[...] = dk_acc[...].astype(jnp.bfloat16)
        dv_ref[...] = dv_acc[...].astype(jnp.bfloat16)

def attention_backward(ranges, q, do, ctx, lse, k, v, kt, code_q, code_k):
    N, W = q.shape
    nh = W // HD
    full = lambda shape: pl.BlockSpec(shape, lambda i, r: (0,)*len(shape))
    row = lambda: pl.BlockSpec((QUERY_TILE, W), lambda i, r: (i, 0))
    out = jax.ShapeDtypeStruct((N, W), jnp.bfloat16)
    return pl.pallas_call(
        backward_kernel,
        out_shape=(out, out, out),
        grid_spec=pltpu.PrefetchScalarGridSpec(
            num_scalar_prefetch=1, grid=(N//QUERY_TILE,),
            in_specs=[row(), row(), row(), pl.BlockSpec((nh, QUERY_TILE), lambda i, r: (0, i)), full((N, W)), full((N, W)), full((W, N)),
                      pl.BlockSpec((1, QUERY_TILE), lambda i, r: (0, i)), full((N, 1))],
            out_specs=[row(), full((N, W)), full((N, W))],
            scratch_shapes=[pltpu.VMEM((W, QUERY_TILE), jnp.float32), pltpu.VMEM((N, W), jnp.float32), pltpu.VMEM((N, W), jnp.float32)]),
        name="attention_backward",
    )(ranges, q, do, ctx, lse, k, v, kt, code_q, code_k)

def slide_tables(lengths_row, mask_all):
    cells = mask_all.shape[0]
    ends = jnp.cumsum(lengths_row)
    starts = ends - lengths_row
    slide = slide_index(jnp.arange(cells, dtype=jnp.int32), lengths_row)
    first = jnp.arange(cells // QUERY_TILE, dtype=jnp.int32) * QUERY_TILE
    first_slide = slide_index(first, lengths_row)
    last_slide = slide_index(first + (QUERY_TILE - 1), lengths_row)
    order = jnp.arange(lengths_row.shape[0], dtype=jnp.int32)

    def picked(table, index):
        return jnp.sum(jnp.where(index[:, None] == order[None, :], table[None, :], 0), axis=1)

    low = picked(starts, first_slide) // KEY_UNIT
    high = picked(ends, last_slide)
    tiles = (high - low * KEY_UNIT + KEY_TILE - 1) // KEY_TILE
    low = jnp.minimum(low, (cells - tiles * KEY_TILE) // KEY_UNIT)
    ranges = jnp.stack([low, tiles], axis=1).astype(jnp.int32)
    open_code = jnp.where(mask_all == 1, slide, -1)
    return ranges, slide[None, :], open_code[:, None]


def moved(value, target):
    groups, blocks = lax.axis_size("dp"), lax.axis_size("blk")
    pairs = []
    for g in range(groups):
        for b in range(blocks):
            there = target(g, b)
            if there is not None:
                pairs.append((g * blocks + b, there[0] * blocks + there[1]))
    return lax.ppermute(value, MESH_AXES, pairs)


def at_home(g, b):
    return g % 2 == b // (lax.axis_size("blk") // 2)


def head_block(g, b):
    return (b % (lax.axis_size("blk") // 2)) * 2 + g % 2


def worker_of(g, block_of_heads):
    half = lax.axis_size("blk") // 2
    return (g - g % 2) + block_of_heads % 2, (g % 2) * half + block_of_heads // 2


def owner_of(g, b, index):
    return (g - g % 2) + b // (lax.axis_size("blk") // 2), index


def pair_masks():
    return [1 << t for t in range(bits_of(lax.axis_size("blk")) - 1)]


def group_meta(meta):
    blocks = lax.axis_size("blk")
    group, block = lax.axis_index("dp"), lax.axis_index("blk")
    other = swapped(meta, 1, 0)
    both = jnp.where(group % 2 == 0, jnp.stack([meta, other]), jnp.stack([other, meta]))
    pieces = jnp.stack([both] + [swapped(both, 0, mask) for mask in range(1, blocks)])
    half = block // (blocks // 2)
    mine = jnp.where(half == 0, pieces[:, 0], pieces[:, 1])
    order = jnp.arange(blocks, dtype=jnp.int32) ^ block
    chosen = order[:, None] == jnp.arange(blocks, dtype=jnp.int32)[None, :]
    return jnp.sum(jnp.where(chosen[:, :, None], mine[None], 0), axis=1)


def group_rows(own):
    blocks = lax.axis_size("blk")
    group, block = lax.axis_index("dp"), lax.axis_index("blk")
    home = at_home(group, block)
    rows, cols = own.shape
    mirror = moved(own, lambda g, b: None if at_home(g, b) else (g, blocks - 1 - b))
    pieces = [(own, lambda b: b), (mirror, lambda b: blocks - 1 - b)]
    for mask in pair_masks():
        more = []
        for value, place in pieces:
            value = moved(value, lambda g, b: (g, b ^ mask) if at_home(g, b) else None)
            more.append((value, lambda b, place=place, mask=mask: place(b ^ mask)))
        pieces = pieces + more
    whole = jnp.zeros((blocks * rows, cols), own.dtype)
    for value, place in pieces:
        other = moved(value, lambda g, b: (g ^ 1, b) if at_home(g, b) else None)
        value = jnp.where(home, value, other)
        whole = lax.dynamic_update_slice_in_dim(whole, value, place(block) * rows, 0)
    return whole


def rows_to_owners(context):
    blocks = lax.axis_size("blk")
    group, block = lax.axis_index("dp"), lax.axis_index("blk")
    mine = head_block(group, block)
    cells, width = context.shape
    rows = cells // blocks
    whole = jnp.zeros((rows, blocks * width), context.dtype)
    for k in range(blocks):
        piece = lax.dynamic_slice_in_dim(context, (mine + k) % blocks * rows, rows, 0)
        piece = moved(piece, lambda g, b: owner_of(g, b, (head_block(g, b) + k) % blocks))
        whole = lax.dynamic_update_slice_in_dim(whole, piece, (block - k) % blocks * width, 1)
    return whole


def heads_to_workers(value):
    blocks = lax.axis_size("blk")
    group, block = lax.axis_index("dp"), lax.axis_index("blk")
    mine = head_block(group, block)
    rows, cols = value.shape
    width = cols // blocks
    whole = jnp.zeros((blocks * rows, width), value.dtype)
    for k in range(blocks):
        piece = lax.dynamic_slice_in_dim(value, (block - k) % blocks * width, width, 1)
        piece = moved(piece, lambda g, b: worker_of(g, (b - k) % blocks))
        whole = lax.dynamic_update_slice_in_dim(whole, piece, (mine + k) % blocks * rows, 0)
    return whole


def rows_summed(partial_rows):
    blocks = lax.axis_size("blk")
    group, block = lax.axis_index("dp"), lax.axis_index("blk")
    rows = partial_rows.shape[0] // blocks
    home = at_home(group, block)
    other = moved(partial_rows, lambda g, b: None if at_home(g, b) else (g ^ 1, b))
    total = added(partial_rows, other)

    def taken(place):
        return lax.dynamic_slice_in_dim(total, place * rows, rows, 0)

    mine = {r: [taken(block ^ r), taken(blocks - 1 - (block ^ r))] for r in range(blocks // 2)}
    for mask in reversed(pair_masks()):
        kept = {r: mine[r] for r in range(mask)}
        for r in range(mask):
            came = [
                moved(part, lambda g, b: (g, b ^ mask) if at_home(g, b) else None)
                for part in mine[r + mask]
            ]
            kept[r] = [added(here, there) for here, there in zip(kept[r], came)]
        mine = kept
    own, mirror = mine[0]
    far = moved(mirror, lambda g, b: (g, blocks - 1 - b) if at_home(g, b) else None)
    return jnp.where(home, own, far)


def reduced_heads(grad):
    blocks = lax.axis_size("blk")
    group, block = lax.axis_index("dp"), lax.axis_index("blk")
    half = blocks // 2
    rows, cols = grad.shape
    width = cols // 3
    value = grad.astype(jnp.bfloat16).reshape(blocks, rows // blocks, cols)
    steps = dp_masks()[1:]
    sides = [(group // mask) % 2 for mask in steps]
    for mask, side in zip(steps, sides):
        keep, send = halves(value, side, 1)
        value = added(keep, swapped(send, mask, 0))
    keep, send = halves(value, block // half, 0)
    value = added(keep, swapped(send, 0, half))
    place = block % half
    pieces = [
        (
            lax.dynamic_index_in_dim(value, place ^ k, 0, keepdims=False)
            if k == 0
            else swapped(
                lax.dynamic_index_in_dim(value, place ^ k, 0, keepdims=False), 0, k
            )
        )
        for k in range(half)
    ]
    order = [place ^ k for k in range(half)]
    value = jnp.zeros((half,) + pieces[0].shape, pieces[0].dtype)
    for piece, index in zip(pieces, order):
        value = lax.dynamic_update_slice_in_dim(value, piece[None], index, 0)
    for mask, side in reversed(list(zip(steps, sides))):
        value = joined(value, swapped(value, mask, 0), side, 1)
    core = group % 2
    other = swapped(value, 1, 0)
    both = jnp.stack([jnp.where(core == 0, value, other), jnp.where(core == 0, other, value)])
    both = both.reshape(2, half, rows // blocks, 3, width)
    both = jnp.transpose(both, (3, 2, 1, 0, 4)).reshape(3, rows // blocks, blocks * width)
    both = both.astype(jnp.float32)
    return both[0], both[1], both[2]


def local(
    cell_states,
    slide_lengths,
    cell_mask,
    latent_noise,
    train_step,
    attn_gain,
    attn_shift,
    query_weight,
    key_weight,
    value_weight,
    out_weight,
    ffn_gain,
    ffn_shift,
    up_weight,
    up_bias,
    down_weight,
    down_bias,
    encode_weight,
    encode_bias,
    decode_weight,
    prior_means,
    prior_logits,
    out_grad,
):
    rows_here = cell_states.shape[0]
    blocks = lax.axis_size("blk")
    group, block = lax.axis_index("dp"), lax.axis_index("blk")
    width = D // blocks
    my_heads = head_block(group, block) * width
    meta = group_meta(jnp.concatenate([cell_mask, slide_lengths[0]]))
    mask_all = meta[:, :rows_here].reshape(-1)
    ranges, query_code, key_code = slide_tables(meta[0, rows_here:], mask_all)
    x_float = cell_states.astype(jnp.float32)
    _, norm_back = jax.vjp(layer_norm, x_float, attn_gain, attn_shift)
    x_all = group_rows(cell_states)
    normed_b = layer_norm(x_all.astype(jnp.float32), attn_gain, attn_shift).astype(jnp.bfloat16)
    weight_here = jnp.concatenate(
        [
            lax.dynamic_slice_in_dim(weight, my_heads, width, 1)
            for weight in (query_weight, key_weight, value_weight)
        ],
        axis=1,
    )
    projected = plain_dot(normed_b, weight_here).astype(jnp.bfloat16)
    queries = projected[:, :width]
    keys = projected[:, width : 2 * width]
    values = projected[:, 2 * width :]
    context_here, log_total = attention_forward(
        ranges, queries, keys, values.T, query_code, key_code
    )
    context_b = rows_to_owners(context_here)
    hidden = x_float + plain_dot(context_b, out_weight)
    normed_two, norm_two_back = jax.vjp(layer_norm, hidden, ffn_gain, ffn_shift)
    normed_two_b = normed_two.astype(jnp.bfloat16)
    inner = plain_dot(normed_two_b, up_weight) + up_bias
    activated, gelu_back = jax.vjp(partial(jax.nn.gelu, approximate=False), inner)
    activated_b = activated.astype(jnp.bfloat16)
    hidden_two = hidden + plain_dot(activated_b, down_weight) + down_bias
    hidden_two_b = hidden_two.astype(jnp.bfloat16)
    encoded = plain_dot(hidden_two_b, encode_weight) + encode_bias
    latent_mean = encoded[:, :LAT]
    latent_logvar = encoded[:, LAT:]
    spread = jnp.exp(0.5 * latent_logvar)
    noise_float = latent_noise.astype(jnp.float32)
    latent_b = (latent_mean + spread * noise_float).astype(jnp.bfloat16)
    output = hidden_two + plain_dot(latent_b, decode_weight)
    (kl_dim, categorical), kl_back = jax.vjp(
        kl_terms, latent_mean, latent_logvar, prior_means, prior_logits
    )
    real = cell_mask.astype(jnp.float32)
    sums = jnp.concatenate(
        [
            jnp.sum(kl_dim * real[:, None], axis=0),
            jnp.sum(categorical * real)[None],
            jnp.sum(real)[None],
            jnp.zeros((126,), jnp.float32),
        ]
    )
    sums = summed_everywhere(sums)
    kl_sum, cat_sum, count = sums[:LAT], sums[LAT], sums[LAT + 1]
    kbar = kl_sum / count
    floored = jnp.sum(jnp.maximum(kbar, free_floor))
    cat_mean = cat_sum / count
    beta = jnp.minimum(1.0, (train_step[0].astype(jnp.float32) + 1.0) / WARM)
    active = (kbar > free_floor).astype(jnp.float32)
    grad_decode = rows_dot(latent_b, out_grad)
    grad_latent = cols_dot(out_grad, decode_weight)
    grad_mean, grad_logvar, grad_means, grad_prior = kl_back(
        (beta * real[:, None] * active[None, :], beta * real)
    )
    grad_mean = grad_mean + grad_latent
    grad_logvar = grad_logvar + grad_latent * 0.5 * spread * noise_float
    grad_encoded_b = jnp.concatenate([grad_mean, grad_logvar], axis=1).astype(jnp.bfloat16)
    grad_encode = rows_dot(hidden_two_b, grad_encoded_b)
    grad_encode_bias = jnp.sum(grad_encoded_b.astype(jnp.float32), axis=0)
    grad_two = out_grad.astype(jnp.float32) + cols_dot(grad_encoded_b, encode_weight)
    grad_down_bias = jnp.sum(grad_two, axis=0)
    grad_branch_b = grad_two.astype(jnp.bfloat16)
    grad_down = rows_dot(activated_b, grad_branch_b)
    (grad_inner,) = gelu_back(cols_dot(grad_branch_b, down_weight))
    grad_inner_b = grad_inner.astype(jnp.bfloat16)
    grad_up_bias = jnp.sum(grad_inner_b.astype(jnp.float32), axis=0)
    grad_up = rows_dot(normed_two_b, grad_inner_b)
    grad_hidden, grad_ffn_gain, grad_ffn_shift = norm_two_back(cols_dot(grad_inner_b, up_weight))
    grad_hidden = grad_hidden + grad_two
    grad_attn_b = grad_hidden.astype(jnp.bfloat16)
    grad_out = rows_dot(context_b, grad_attn_b)
    grad_context_b = cols_dot(grad_attn_b, out_weight).astype(jnp.bfloat16)
    grad_here = heads_to_workers(grad_context_b)
    grad_q, grad_k, grad_v = attention_backward(
        ranges, queries, grad_here, context_here, log_total, keys, values, keys.T, query_code, key_code
    )
    grad_projected = jnp.concatenate([grad_q, grad_k, grad_v], axis=1)
    grad_query, grad_key, grad_value = reduced_heads(rows_dot(normed_b, grad_projected))
    grad_normed = rows_summed(cols_dot(grad_projected, weight_here).astype(jnp.bfloat16))
    grad_normed = grad_normed.astype(jnp.float32)
    grad_from_norm, grad_attn_gain, grad_attn_shift = norm_back(grad_normed)
    states_grad = grad_hidden + grad_from_norm
    by_block = lambda part: part.reshape(blocks, -1)
    means_block = jnp.moveaxis(grad_means.reshape(K, blocks, LAT // blocks), 1, 0)
    small = reduced_small(
        [
            by_block(grad_attn_gain),
            by_block(grad_attn_shift),
            by_block(grad_ffn_gain),
            by_block(grad_ffn_shift),
            by_block(grad_up_bias),
            by_block(grad_down_bias),
            by_block(grad_encode_bias),
            by_block(means_block),
            by_block(grad_prior),
        ]
    )
    totals = (
        small[0],
        small[1],
        grad_query,
        grad_key,
        grad_value,
        reduced(grad_out, True),
        small[2],
        small[3],
        reduced(grad_up, True),
        small[4],
        reduced(grad_down, False),
        small[5],
        reduced(grad_encode, True),
        small[6],
        reduced(grad_decode, False),
        small[7].reshape(K, LAT // blocks),
        small[8],
    )
    kl_out = (floored / LAT + cat_mean).reshape(1)
    return (output.astype(jnp.bfloat16), states_grad, kl_out) + tuple(totals)


def solution(mesh):
    in_specs = (
        P(("dp", "blk"), None),
        P("dp", None),
        P(("dp", "blk")),
        P(("dp", "blk"), None),
        P(),
        P(),
        P(),
        P(),
        P(),
        P(),
        P(),
        P(),
        P(),
        P(),
        P(),
        P(),
        P(),
        P(),
        P(),
        P(),
        P(),
        P(),
        P(("dp", "blk"), None),
    )
    out_specs = (
        P(("dp", "blk"), None),
        P(("dp", "blk"), None),
        P(),
        P("blk"),
        P("blk"),
        P("blk", None),
        P("blk", None),
        P("blk", None),
        P("blk", None),
        P("blk"),
        P("blk"),
        P("blk", None),
        P("blk"),
        P("blk", None),
        P("blk"),
        P("blk", None),
        P("blk"),
        P("blk", None),
        P(None, "blk"),
        P("blk"),
    )
    return jax.shard_map(local, mesh=mesh, in_specs=in_specs, out_specs=out_specs, check_vma=False)
```

```python
import math
from functools import partial

import jax
import jax.numpy as jnp
from jax import lax
from jax.experimental import pallas as pl
from jax.experimental.pallas import tpu as pltpu
from jax.sharding import PartitionSpec as P

D = 1024
H = 16
HD = 64
LAT = 512
K = 16
WARM = 2000


ln_eps = 1e-05
free_floor = 1.3
neg_fill = -1e30

QUERY_TILE = 512
KEY_TILE = 512
KEY_UNIT = 128
FEED_TILE = 512


def layer_norm(values, gain, shift):
    center = values - jnp.mean(values, axis=-1, keepdims=True)
    spread = jnp.mean(center * center, axis=-1, keepdims=True)
    return center * lax.rsqrt(spread + ln_eps) * gain + shift


def slide_index(position, lengths_row):
    ends = jnp.cumsum(lengths_row)
    return jnp.sum((position[:, None] >= ends[None, :]).astype(jnp.int32), axis=1)


def exact_dot(left, right):
    return jnp.dot(left, right, precision=lax.Precision.HIGHEST, preferred_element_type=jnp.float32)


def kl_terms(latent_mean, latent_logvar, prior_means, prior_logits):
    log_prior = jax.nn.log_softmax(prior_logits)
    logits = exact_dot(latent_mean, prior_means.T) * LAT ** (-0.5) + log_prior[None, :]
    resp = jax.nn.softmax(logits, axis=-1)
    log_resp = jax.nn.log_softmax(logits, axis=-1)
    mixed_mean = exact_dot(resp, prior_means)
    mixed_square = exact_dot(resp, prior_means * prior_means)
    kl_dim = 0.5 * (
        jnp.exp(latent_logvar)
        + latent_mean * latent_mean
        - 2.0 * latent_mean * mixed_mean
        + mixed_square
        - 1.0
        - latent_logvar
    )
    categorical = jnp.sum(resp * (log_resp - log_prior[None, :]), axis=-1)
    return (kl_dim, categorical)


def plain_dot(left, right):
    return jnp.dot(left, right, preferred_element_type=jnp.float32)


def rows_dot(left, right):
    return lax.dot_general(
        left, right, (((0,), (0,)), ((), ())), preferred_element_type=jnp.float32
    )


def cols_dot(left, right):
    return lax.dot_general(
        left, right, (((1,), (1,)), ((), ())), preferred_element_type=jnp.float32
    )


MESH_AXES = ("dp", "blk")


def swapped(value, dp_mask, blk_mask):
    groups, blocks = lax.axis_size("dp"), lax.axis_size("blk")
    pairs = [
        (g * blocks + b, (g ^ dp_mask) * blocks + (b ^ blk_mask))
        for g in range(groups)
        for b in range(blocks)
    ]
    return lax.ppermute(value, MESH_AXES, pairs)


def bits_of(count):
    return count.bit_length() - 1


def dp_masks():
    return [1 << t for t in range(bits_of(lax.axis_size("dp")))]


def blk_masks():
    return [(2 << t) - 1 for t in range(bits_of(lax.axis_size("blk")))]


def summed_everywhere(value):
    for mask in dp_masks():
        value = value + swapped(value, mask, 0)
    for mask in blk_masks():
        value = value + swapped(value, 0, mask)
    return value


def added(left, right):
    return (left.astype(jnp.float32) + right.astype(jnp.float32)).astype(jnp.bfloat16)


def summed(terms):
    total = terms[0].astype(jnp.float32)
    for term in terms[1:]:
        total = total + term.astype(jnp.float32)
    return total.astype(jnp.bfloat16)


def chunk(value, start, size, axis):
    return lax.dynamic_slice_in_dim(value, start, size, axis)


def tied(value, other):
    return lax.optimization_barrier((value, other))[0]


class Exchange:
    def __init__(self, steps):
        self.steps = steps
        self.result = None
        self.last = None
        self.flight = None
        self._take(lambda: next(self.steps))

    def _take(self, step):
        try:
            values, permute = step()
            self.last = values
            self.flight = [permute(value) for value in values]
        except StopIteration as end:
            self.result = end.value
            self.last = end.value
            self.flight = None

    def advance(self, token):
        came = tied(self.flight, token)
        self._take(lambda: self.steps.send(came))
        return self.last


def by_mask(dp_mask, blk_mask):
    return lambda value: swapped(value, dp_mask, blk_mask)


def dp_order(flipped):
    masks = dp_masks()
    return masks[:1] + masks[1:][::-1] if flipped else masks


def relative_masks(steps):
    places = [0]
    for step in steps[::-1]:
        places = places + [place ^ step for place in places]
    return places


def relative_table(steps, mine):
    masks = relative_masks(steps)
    inverse = [masks.index(place) for place in range(len(masks))]
    order = jnp.arange(len(masks), dtype=jnp.int32)
    wanted = order ^ mine
    return sum(jnp.where(wanted == place, inverse[place], 0) for place in range(len(masks)))


def spread_kernel(parts, table_ref, mine_ref, other_ref, *out_refs):
    held, _, width = mine_ref.shape
    cols = 2 * held * width
    for place in range(2 * held):
        index = table_ref[place]
        piece = jnp.where(index < held, mine_ref[index & (held - 1)], other_ref[index & (held - 1)])
        piece = piece.astype(jnp.float32)
        for out_ref, (begin, count, times) in zip(out_refs, parts):
            for time in range(times):
                row, column = begin + time * count, time * cols + place * width
                out_ref[:, column : column + width] = piece[row : row + count]


def spread_columns(mine, other, table, parts):
    held, rows, width = mine.shape
    cols = 2 * held * width
    begin, placed, shapes = 0, [], []
    for count, times in parts:
        placed.append((begin, count, times))
        shapes.append(jax.ShapeDtypeStruct((count, times * cols), jnp.float32))
        begin += count * times
    return pl.pallas_call(
        partial(spread_kernel, placed),
        out_shape=shapes,
        grid_spec=pltpu.PrefetchScalarGridSpec(
            num_scalar_prefetch=1,
            grid=(1,),
            in_specs=[resident((held, rows, width))] * 2,
            out_specs=[resident(shape.shape) for shape in shapes],
        ),
        cost_estimate=nothing(),
        name="spread_columns",
    )(table, mine, other)


def head_steps(value):
    blocks = lax.axis_size("blk")
    group, block = lax.axis_index("dp"), lax.axis_index("blk")
    half = blocks // 2
    steps = dp_masks()[1:]
    masks = relative_masks([step >> 1 for step in steps])
    taken = [[chunk(value, (group >> 1) ^ mask, 1, 1)] for mask in masks]
    size = len(masks)
    for step in steps:
        size = size // 2
        send = jnp.concatenate([summed(taken[place]) for place in range(size, 2 * size)], axis=1)
        (came,) = yield [send], by_mask(step, 0)
        taken = [taken[place] + [came[:, place : place + 1]] for place in range(size)]
    side = block >> (bits_of(blocks) - 1)
    away = [chunk(term, (1 - side) * half, half, 0) for term in taken[0]]
    (came,) = yield [summed(away)], by_mask(0, half)
    terms = [chunk(term, side * half, half, 0) for term in taken[0]] + [came]
    place = block & (half - 1)
    pieces = [summed([chunk(term, place, 1, 0) for term in terms])]
    for k in range(1, half):
        send = summed([chunk(term, place ^ k, 1, 0) for term in terms])
        (came,) = yield [send], by_mask(0, k)
        pieces.append(came)
    value = jnp.concatenate(pieces, axis=1)
    for step in steps[::-1]:
        (came,) = yield [value], by_mask(step, 0)
        value = jnp.concatenate([value, came], axis=0)
    (other,) = yield [value], by_mask(1, 0)
    return value, other


def heads_kernel(table_ref, mine_ref, other_ref, *out_refs):
    pieces = pl.num_programs(0)
    place, core = table_ref[pieces], table_ref[pieces + 1]
    half = mine_ref.shape[1]
    rows = out_refs[0].shape[0]
    width = mine_ref.shape[3] // 3
    for chip in range(half):
        mine = mine_ref[0, chip ^ place].astype(jnp.float32)
        other = other_ref[0, chip ^ place].astype(jnp.float32)
        for c in range(2):
            value = jnp.where(core == c, mine, other)
            column = (2 * chip + c) * width
            for kind in range(3):
                out_refs[kind][:, column : column + width] = value[:rows, kind * width : (kind + 1) * width]


def spread_heads(mine, other, rows):
    blocks = lax.axis_size("blk")
    group, block = lax.axis_index("dp"), lax.axis_index("blk")
    pieces, half, held_rows, width = mine.shape
    table = relative_table([step >> 1 for step in dp_masks()[1:]], group >> 1)
    table = jnp.concatenate([table, jnp.stack([block & (half - 1), group & 1])])
    held = pl.BlockSpec((1, half, held_rows, width), lambda i, table: (table[i], 0, 0, 0))
    cols = 2 * half * width // 3
    return pl.pallas_call(
        heads_kernel,
        out_shape=(jax.ShapeDtypeStruct((pieces * rows, cols), jnp.float32),) * 3,
        grid_spec=pltpu.PrefetchScalarGridSpec(
            num_scalar_prefetch=1,
            grid=(pieces,),
            in_specs=[held, held],
            out_specs=[pl.BlockSpec((rows, cols), lambda i, table: (i, 0))] * 3,
        ),
        cost_estimate=nothing(),
        name="spread_heads",
    )(table, mine, other)


def head_lanes(value, head):
    lane = lax.broadcasted_iota(jnp.int32, value.shape, 1) // HD
    return jnp.where(lane == head, value, jnp.zeros_like(value))

def nt_dot(left, right):
    return lax.dot_general(left, right, (((1,),(1,)),((),())), preferred_element_type=jnp.float32)

def nn_dot(left, right):
    return lax.dot_general(left, right, (((1,),(0,)),((),())), preferred_element_type=jnp.float32)

def allowed_pairs(code_k, code_q, block_k, tile):
    key_pos = block_k + lax.broadcasted_iota(jnp.int32, tile, 0)
    query_pos = pl.program_id(0) * QUERY_TILE + lax.broadcasted_iota(jnp.int32, tile, 1)
    return (code_k == code_q) | (key_pos == query_pos)

def forward_kernel(range_ref, q_ref, k_ref, v_ref, cq_ref, ck_ref, ctx_ref, lse_ref, m_ref, l_ref, acc_ref, vt_ref):
    nh = q_ref.shape[1] // HD
    step = pl.program_id(0)

    @pl.when(step == 0)
    def _():
        vt_ref[...] = v_ref[...].T

    m_ref[...] = jnp.full(m_ref.shape, neg_fill, jnp.float32)
    l_ref[...] = jnp.zeros(l_ref.shape, jnp.float32)
    acc_ref[...] = jnp.zeros(acc_ref.shape, jnp.float32)
    code_q = cq_ref[...]
    scaled = (q_ref[...].astype(jnp.float32) * HD ** (-0.5)).astype(jnp.bfloat16)
    def body(kb, _):
        start = pl.multiple_of(range_ref[step, 0] * KEY_UNIT + kb * KEY_TILE, KEY_UNIT)
        keys = k_ref[pl.ds(start, KEY_TILE), :]
        open_pair = allowed_pairs(ck_ref[pl.ds(start, KEY_TILE), :], code_q, start, (KEY_TILE, QUERY_TILE))
        for h in range(nh):
            s = nt_dot(keys, head_lanes(scaled, h))
            s = jnp.where(open_pair, s, neg_fill)
            m_old = m_ref[h:h+1, :]
            m_new = jnp.maximum(m_old, jnp.max(s, axis=0, keepdims=True))
            p = jnp.exp(s - m_new)
            alpha = jnp.exp(m_old - m_new)
            l_ref[h:h+1, :] = l_ref[h:h+1, :] * alpha + jnp.sum(p, axis=0, keepdims=True)
            m_ref[h:h+1, :] = m_new
            rows = slice(h*HD, (h+1)*HD)
            acc_ref[rows, :] = acc_ref[rows, :] * alpha + nn_dot(vt_ref[rows, pl.ds(start, KEY_TILE)], p.astype(jnp.bfloat16))
        return 0
    lax.fori_loop(0, range_ref[step, 1], body, 0)
    for h in range(nh):
        rows = slice(h*HD, (h+1)*HD)
        acc_ref[rows, :] = acc_ref[rows, :] / l_ref[h:h+1, :]
    ctx_ref[...] = acc_ref[...].T.astype(jnp.bfloat16)
    lse_ref[...] = m_ref[...] + jnp.log(l_ref[...])

def attention_forward(ranges, q, k, v, code_q, code_k):
    N, W = q.shape
    nh = W // HD
    full = lambda shape: pl.BlockSpec(shape, lambda i, r: (0,)*len(shape))
    return pl.pallas_call(
        forward_kernel,
        out_shape=(jax.ShapeDtypeStruct((N, W), jnp.bfloat16), jax.ShapeDtypeStruct((nh, N), jnp.float32)),
        grid_spec=pltpu.PrefetchScalarGridSpec(
            num_scalar_prefetch=1, grid=(N//QUERY_TILE,),
            in_specs=[pl.BlockSpec((QUERY_TILE, W), lambda i, r: (i, 0)), full((N, W)), full((N, W)),
                      pl.BlockSpec((1, QUERY_TILE), lambda i, r: (0, i)), full((N, 1))],
            out_specs=[pl.BlockSpec((QUERY_TILE, W), lambda i, r: (i, 0)), pl.BlockSpec((nh, QUERY_TILE), lambda i, r: (0, i))],
            scratch_shapes=[pltpu.VMEM((nh, QUERY_TILE), jnp.float32), pltpu.VMEM((nh, QUERY_TILE), jnp.float32), pltpu.VMEM((W, QUERY_TILE), jnp.float32), pltpu.VMEM((W, N), jnp.bfloat16)]),
        cost_estimate=nothing(),
        name="attention_forward",
    )(ranges, q, k, v, code_q, code_k)

def backward_kernel(range_ref, row_ref, q_ref, ctx_ref, lse_ref, k_ref, v_ref, cq_ref, ck_ref,
                    *refs):
    pieces = row_ref.shape[0]
    do_refs, (dq_ref, dk_ref, dv_ref, dqt_ref, dk_acc, dv_acc, kt_ref, do_ref) = refs[:pieces], refs[pieces:]
    nh = q_ref.shape[1] // HD
    step = pl.program_id(0)
    @pl.when(step == 0)
    def _():
        dk_acc[...] = jnp.zeros(dk_acc.shape, jnp.float32)
        dv_acc[...] = jnp.zeros(dv_acc.shape, jnp.float32)
        kt_ref[...] = k_ref[...].T
        for k, piece_ref in enumerate(do_refs):
            rows = piece_ref.shape[0]
            do_ref[pl.ds(pl.multiple_of(row_ref[k] * rows, rows), rows), :] = piece_ref[...]

    dqt_ref[...] = jnp.zeros(dqt_ref.shape, jnp.float32)
    code_q = cq_ref[...]
    scaled = (q_ref[...].astype(jnp.float32) * HD ** (-0.5)).astype(jnp.bfloat16)
    grads = do_ref[pl.ds(pl.multiple_of(step * QUERY_TILE, QUERY_TILE), QUERY_TILE), :]
    product = (grads.astype(jnp.float32) * ctx_ref[...].astype(jnp.float32)).T
    deltas = [jnp.sum(product[h*HD:(h+1)*HD, :], axis=0, keepdims=True) for h in range(nh)]
    q_all = jnp.concatenate([head_lanes(scaled, h) for h in range(nh)], axis=0)
    do_all = jnp.concatenate([head_lanes(grads, h) for h in range(nh)], axis=0)
    def body(kb, _):
        start = pl.multiple_of(range_ref[step, 0] * KEY_UNIT + kb * KEY_TILE, KEY_UNIT)
        keys = k_ref[pl.ds(start, KEY_TILE), :]
        values = v_ref[pl.ds(start, KEY_TILE), :]
        open_pair = allowed_pairs(ck_ref[pl.ds(start, KEY_TILE), :], code_q, start, (KEY_TILE, QUERY_TILE))
        ps, dss = [], []
        for h in range(nh):
            cols = slice(h*QUERY_TILE, (h+1)*QUERY_TILE)
            rows = slice(h*HD, (h+1)*HD)
            s = nt_dot(keys, q_all[cols, :])
            p = jnp.where(open_pair, jnp.exp(s - lse_ref[h:h+1, :]), 0.0)
            dp = nt_dot(values, do_all[cols, :])
            ds = (p * (dp - deltas[h])).astype(jnp.bfloat16)
            ps.append(p.astype(jnp.bfloat16))
            dss.append(ds)
            dqt_ref[rows, :] += nn_dot(kt_ref[rows, pl.ds(start, KEY_TILE)], ds)
        dv_acc[pl.ds(start, KEY_TILE), :] += nn_dot(jnp.concatenate(ps, axis=1), do_all)
        dk_acc[pl.ds(start, KEY_TILE), :] += nn_dot(jnp.concatenate(dss, axis=1), q_all)
        return 0
    lax.fori_loop(0, range_ref[step, 1], body, 0)
    dq_ref[...] = (dqt_ref[...] * HD ** (-0.5)).T.astype(jnp.bfloat16)
    @pl.when(step == pl.num_programs(0) - 1)
    def _():
        dk_ref[...] = dk_acc[...].astype(jnp.bfloat16)
        dv_ref[...] = dv_acc[...].astype(jnp.bfloat16)

def attention_backward(ranges, places, q, pieces, ctx, lse, k, v, code_q, code_k):
    cells, width = q.shape
    heads = width // HD

    def row():
        return pl.BlockSpec((QUERY_TILE, width), lambda i, *_: (i, 0))

    out = jax.ShapeDtypeStruct((cells, width), jnp.bfloat16)
    return pl.pallas_call(
        backward_kernel,
        out_shape=(out, out, out),
        grid_spec=pltpu.PrefetchScalarGridSpec(
            num_scalar_prefetch=2,
            grid=(cells // QUERY_TILE,),
            in_specs=[
                row(),
                row(),
                pl.BlockSpec((heads, QUERY_TILE), lambda i, *_: (0, i)),
                resident((cells, width)),
                resident((cells, width)),
                pl.BlockSpec((1, QUERY_TILE), lambda i, *_: (0, i)),
                resident((cells, 1)),
            ]
            + [resident(piece.shape) for piece in pieces],
            out_specs=[row(), resident((cells, width)), resident((cells, width))],
            scratch_shapes=[
                pltpu.VMEM((width, QUERY_TILE), jnp.float32),
                pltpu.VMEM((cells, width), jnp.float32),
                pltpu.VMEM((cells, width), jnp.float32),
                pltpu.VMEM((width, cells), jnp.bfloat16),
                pltpu.VMEM((cells, width), jnp.bfloat16),
            ],
        ),
        cost_estimate=nothing(),
        name="attention_backward",
    )(ranges, places, q, ctx, lse, k, v, code_q, code_k, *pieces)


def slide_tables(lengths_row, mask_all):
    cells = mask_all.shape[0]
    ends = jnp.cumsum(lengths_row)
    starts = ends - lengths_row
    slide = slide_index(jnp.arange(cells, dtype=jnp.int32), lengths_row)
    first = jnp.arange(cells // QUERY_TILE, dtype=jnp.int32) * QUERY_TILE
    first_slide = slide_index(first, lengths_row)
    last_slide = slide_index(first + (QUERY_TILE - 1), lengths_row)
    order = jnp.arange(lengths_row.shape[0], dtype=jnp.int32)

    def picked(table, index):
        return jnp.sum(jnp.where(index[:, None] == order[None, :], table[None, :], 0), axis=1)

    low = picked(starts, first_slide) // KEY_UNIT
    high = picked(ends, last_slide)
    tiles = (high - low * KEY_UNIT + KEY_TILE - 1) // KEY_TILE
    low = jnp.minimum(low, (cells - tiles * KEY_TILE) // KEY_UNIT)
    ranges = jnp.stack([low, tiles], axis=1).astype(jnp.int32)
    open_code = jnp.where(mask_all == 1, slide, -1)
    return ranges, slide[None, :], open_code[:, None]


def moved(value, target):
    groups, blocks = lax.axis_size("dp"), lax.axis_size("blk")
    pairs = []
    for g in range(groups):
        for b in range(blocks):
            there = target(g, b)
            if there is not None:
                pairs.append((g * blocks + b, there[0] * blocks + there[1]))
    return lax.ppermute(value, MESH_AXES, pairs)


def at_home(g, b):
    return (g & 1) == b >> (bits_of(lax.axis_size("blk")) - 1)


def head_block(g, b):
    return (b & (lax.axis_size("blk") // 2 - 1)) * 2 + (g & 1)


def worker_of(g, block_of_heads):
    half = lax.axis_size("blk") // 2
    return (g - g % 2) + block_of_heads % 2, (g % 2) * half + block_of_heads // 2


def owner_of(g, b, index):
    return (g - g % 2) + b // (lax.axis_size("blk") // 2), index


def pair_masks():
    return [1 << t for t in range(bits_of(lax.axis_size("blk")) - 1)]


def with_meta(cells, mask, lengths):
    count = lengths.shape[0]
    meta = jnp.concatenate([mask, lengths >> 7, lengths & 127]).astype(cells.dtype)
    meta = jnp.pad(meta, (0, cells.shape[1] - mask.shape[0] - 2 * count))
    return jnp.concatenate([cells, jnp.pad(meta[None], ((0, 7), (0, 0)))], axis=0)


def from_meta(meta, rows, count):
    meta = meta.astype(jnp.int32)
    high = meta[0, rows : rows + count]
    return meta[:, :rows].reshape(-1), high * 128 + meta[0, rows + count : rows + 2 * count]


def from_home(value):
    return moved(value, lambda g, b: (g ^ 1, b) if at_home(g, b) else None)


def paired(value, mask):
    return moved(value, lambda g, b: (g, b ^ mask) if at_home(g, b) else None)


def group_rows(own, use):
    blocks = lax.axis_size("blk")
    block = lax.axis_index("blk")
    mirror = moved(own, lambda g, b: None if at_home(g, b) else (g, blocks - 1 - b))
    held, rows = None, []
    for mirrored in (False, True):
        pieces = [(mirror if mirrored else own, 0)]
        for mask in pair_masks():
            pieces += [(paired(piece, mask), place ^ mask) for piece, place in pieces]
        pieces = [
            (piece, from_home(tied(piece, held) if mirrored else piece), blocks - 1 - (block ^ place) if mirrored else block ^ place)
            for piece, place in pieces
        ]
        held = use(pieces, held)
        rows += pieces
    return held, rows


def entry_kernel(count, place_ref, *refs):
    pieces, refs = refs[: 2 * count], refs[2 * count :]
    gain_ref, shift_ref = refs[:2]
    weights = refs[2:5]
    normed_ref, *out_refs = refs[-4:]
    step, home = pl.program_id(0), place_ref[count]
    rows = normed_ref.shape[0]
    for k in range(count):

        @pl.when(step == k)
        def _(k=k):
            value = jnp.where(home == 1, pieces[2 * k][:rows], pieces[2 * k + 1][:rows])
            unit, _ = norm_parts(value.astype(jnp.float32))
            normed_ref[...] = (unit * gain_ref[...] + shift_ref[...]).astype(jnp.bfloat16)

    for weight_ref, out_ref in zip(weights, out_refs):
        out_ref[...] = nn_dot(normed_ref[...], weight_ref[...]).astype(jnp.bfloat16)


def head_columns(weight):
    width = weight.shape[1] // lax.axis_size("blk")
    if width % 128 == 0:
        return weight, pl.BlockSpec((weight.shape[0], width), lambda i, place: (0, place[place.shape[0] - 1]))
    mine = head_block(lax.axis_index("dp"), lax.axis_index("blk")) * width
    return lax.dynamic_slice_in_dim(weight, mine, width, 1), resident((weight.shape[0], width))


def entry(pieces, gain, shift, weights, held):
    blocks, count = lax.axis_size("blk"), len(pieces)
    group, block = lax.axis_index("dp"), lax.axis_index("blk")
    rows, model = pieces[0][0].shape[0] - 8, pieces[0][0].shape[1]
    width = model // blocks
    home = at_home(group, block).astype(jnp.int32)
    table = jnp.stack([place for _, _, place in pieces] + [home, head_block(group, block)])
    narrow = pl.BlockSpec((rows, width), lambda i, place: (place[i], 0))
    shapes = [jax.ShapeDtypeStruct((blocks * rows, cols), jnp.bfloat16) for cols in (model,) + (width,) * 3]
    operands = [value for mine, other, _ in pieces for value in (mine, other)]
    specs = [resident(value.shape) for value in operands] + [resident((1, model))] * 2
    operands += [gain[None], shift[None]]
    for weight in weights:
        weight, spec = head_columns(weight)
        operands.append(weight)
        specs.append(spec)
    aliases = {}
    if held is not None:
        aliases = {1 + len(operands) + i: i for i in range(4)}
        operands += list(held)
        specs += [pl.BlockSpec(memory_space=pl.ANY)] * 4
    return pl.pallas_call(
        partial(entry_kernel, count),
        grid_spec=pltpu.PrefetchScalarGridSpec(
            num_scalar_prefetch=1,
            grid=(count,),
            in_specs=specs,
            out_specs=[pl.BlockSpec((rows, model), lambda i, place: (place[i], 0)), narrow, narrow, narrow],
        ),
        out_shape=shapes,
        input_output_aliases=aliases,
        cost_estimate=nothing(),
        name="entry",
    )(table, *operands)


def project_back_kernel(place_ref, normed_ref, dq_ref, dk_ref, dv_ref, wq_ref, wk_ref, wv_ref,
                        rows_ref, grad_ref, gain_ref, shift_ref, acc_ref, sum_ref):
    step = pl.program_id(0)
    width = dq_ref.shape[1]

    @pl.when(step == 0)
    def _():
        acc_ref[...] = jnp.zeros(acc_ref.shape, jnp.float32)
        sum_ref[...] = jnp.zeros(sum_ref.shape, jnp.float32)

    total = jnp.zeros(rows_ref.shape, jnp.float32)
    for kind, (grad, weight_ref) in enumerate(((dq_ref, wq_ref), (dk_ref, wk_ref), (dv_ref, wv_ref))):
        cols = slice(kind * width, (kind + 1) * width)
        total += nt_dot(grad[...], weight_ref[...])
        acc_ref[:, cols] += tn_dot(normed_ref[...], grad[...])
        sum_ref[:1, cols] += jnp.sum(grad[...].astype(jnp.float32), axis=0, keepdims=True)
    rows_ref[...] = total.astype(jnp.bfloat16)

    @pl.when(step == pl.num_programs(0) - 1)
    def _():
        grad_ref[...] = acc_ref[...].astype(jnp.bfloat16)
        ones = jnp.ones((8, width), jnp.float32)
        gain = jnp.zeros(gain_ref.shape, jnp.float32)
        shift = jnp.zeros(shift_ref.shape, jnp.float32)
        for kind, weight_ref in enumerate((wq_ref, wk_ref, wv_ref)):
            cols = slice(kind * width, (kind + 1) * width)
            weight = weight_ref[...].astype(jnp.float32)
            gain += exact_nt_dot(ones, weight * acc_ref[:, cols])
            shift += exact_nt_dot(sum_ref[:, cols], weight)
        gain_ref[...] = gain
        shift_ref[...] = shift


def exact_nt_dot(left, right):
    return lax.dot_general(
        left,
        right,
        (((1,), (1,)), ((), ())),
        precision=lax.Precision.HIGHEST,
        preferred_element_type=jnp.float32,
    )


def project_back(normed, grads, weights):
    cells, width = grads[0].shape
    model = weights[0].shape[0]
    columns = [head_columns(weight) for weight in weights]
    table = head_block(lax.axis_index("dp"), lax.axis_index("blk"))[None]
    wide = pl.BlockSpec((QUERY_TILE, model), lambda i, place: (i, 0))
    return pl.pallas_call(
        project_back_kernel,
        grid_spec=pltpu.PrefetchScalarGridSpec(
            num_scalar_prefetch=1,
            grid=(cells // QUERY_TILE,),
            in_specs=[wide]
            + [pl.BlockSpec((QUERY_TILE, width), lambda i, place: (i, 0))] * 3
            + [spec for _, spec in columns],
            out_specs=[wide, resident((model, 3 * width)), resident((8, model)), resident((8, model))],
            scratch_shapes=[pltpu.VMEM((model, 3 * width), jnp.float32), pltpu.VMEM((8, 3 * width), jnp.float32)],
        ),
        out_shape=[
            jax.ShapeDtypeStruct((cells, model), jnp.bfloat16),
            jax.ShapeDtypeStruct((model, 3 * width), jnp.bfloat16),
            jax.ShapeDtypeStruct((8, model), jnp.float32),
            jax.ShapeDtypeStruct((8, model), jnp.float32),
        ],
        cost_estimate=nothing(),
        name="project_back",
    )(table, normed, *grads, *[weight for weight, _ in columns])


def heads_at_owner():
    blocks, block = lax.axis_size("blk"), lax.axis_index("blk")
    return jnp.stack([(block - k) & (blocks - 1) for k in range(blocks)])


def rows_at_worker():
    blocks = lax.axis_size("blk")
    mine = head_block(lax.axis_index("dp"), lax.axis_index("blk"))
    return jnp.stack([(mine + k) & (blocks - 1) for k in range(blocks)])


def rows_to_owners(context):
    blocks = lax.axis_size("blk")
    places = rows_at_worker()
    rows = context.shape[0] // blocks
    return [
        moved(
            chunk(context, places[k] * rows, rows, 0),
            lambda g, b: owner_of(g, b, (head_block(g, b) + k) % blocks),
        )
        for k in range(blocks)
    ]


def heads_to_workers(pieces):
    blocks = lax.axis_size("blk")
    return [
        moved(piece, lambda g, b: worker_of(g, (b - k) % blocks)) for k, piece in enumerate(pieces)
    ]


def row_steps(partial_rows):
    blocks = lax.axis_size("blk")
    group, block = lax.axis_index("dp"), lax.axis_index("blk")
    rows = partial_rows.shape[0] // blocks
    home = at_home(group, block)
    (other,) = yield [partial_rows], lambda value: moved(
        value, lambda g, b: None if at_home(g, b) else (g ^ 1, b)
    )

    def taken(place):
        return [chunk(part, place * rows, rows, 0)[None] for part in (partial_rows, other)]

    mine = {r: (taken(block ^ r), taken(blocks - 1 - (block ^ r))) for r in range(blocks // 2)}
    for mask in reversed(pair_masks()):
        send = jnp.concatenate([summed(part) for r in range(mask) for part in mine[r + mask]], axis=0)
        (came,) = yield [send], lambda value, mask=mask: moved(
            value, lambda g, b: (g, b ^ mask) if at_home(g, b) else None
        )
        mine = {
            r: tuple(mine[r][k] + [came[2 * r + k : 2 * r + k + 1]] for k in range(2))
            for r in range(mask)
        }
    own, mirror = mine[0]
    (far,) = yield [summed(mirror)], lambda value: moved(
        value, lambda g, b: (g, blocks - 1 - b) if at_home(g, b) else None
    )
    return jnp.where(home, summed(own), far)[0]


def norm_parts(values):
    center = values - jnp.mean(values, axis=-1, keepdims=True)
    spread = jnp.mean(center * center, axis=-1, keepdims=True)
    scale = lax.rsqrt(spread + ln_eps)
    return center * scale, scale


def nothing():
    return pl.CostEstimate(flops=0, bytes_accessed=0, transcendentals=0)


def resident(shape):
    return pl.BlockSpec(shape, lambda *_: (0,) * len(shape))


def feed_kernel(head_ref, *refs):
    pieces = head_ref.shape[0]
    context_refs, (cell_ref, weight_ref), refs = refs[:pieces], refs[pieces : pieces + 2], refs[pieces + 2 :]
    context_ref, hidden_ref, refs = refs[6], refs[7], refs[:6] + refs[8:]

    @pl.when(pl.program_id(0) == 0)
    def _():
        width = weight_ref.shape[0] // pieces
        total = cell_ref[...].astype(jnp.float32)
        for k in range(pieces):
            begin = head_ref[k] * width
            piece = context_refs[k][...]
            total += nn_dot(piece, weight_ref[pl.ds(pl.multiple_of(begin, width), width), :])
            if width % 128 == 0:
                context_ref[:, pl.ds(pl.multiple_of(begin, width), width)] = piece
        hidden_ref[...] = total

    feed_body(hidden_ref, *refs)


def feed_body(hidden_ref, gain_ref, shift_ref, up_ref, up_bias_ref, down_ref, down_bias_ref,
                normed_ref, active_ref, slope_ref, two_ref, two_b_ref, acc_ref):
    step = pl.program_id(0)

    @pl.when(step == 0)
    def _():
        unit, _ = norm_parts(hidden_ref[...])
        normed_ref[...] = (unit * gain_ref[...] + shift_ref[...]).astype(jnp.bfloat16)
        acc_ref[...] = hidden_ref[...] + down_bias_ref[...]

    inner = nn_dot(normed_ref[...], up_ref[...]) + up_bias_ref[...]
    chance = 0.5 + 0.5 * lax.erf(inner * 2.0**-0.5)
    active = (inner * chance).astype(jnp.bfloat16)
    active_ref[...] = active
    slope = chance + inner * jnp.exp(-0.5 * inner * inner) * (2.0 * math.pi) ** -0.5
    slope_ref[...] = slope.astype(jnp.bfloat16)
    acc_ref[...] += nn_dot(active, down_ref[...])

    @pl.when(step == pl.num_programs(0) - 1)
    def _():
        two_ref[...] = acc_ref[...]
        two_b_ref[...] = acc_ref[...].astype(jnp.bfloat16)


def feed_forward(heads, contexts, cells, out_weight, gain, shift, up_weight, up_bias, down_weight, down_bias):
    rows, model = cells.shape
    inner = up_weight.shape[1]
    tile = FEED_TILE
    across = pl.BlockSpec((rows, tile), lambda j, heads: (0, j))
    return pl.pallas_call(
        feed_kernel,
        grid_spec=pltpu.PrefetchScalarGridSpec(
            num_scalar_prefetch=1,
            grid=(inner // tile,),
            in_specs=[resident(part.shape) for part in contexts]
            + [
                resident((rows, model)),
                resident((model, model)),
                resident((1, model)),
                resident((1, model)),
                pl.BlockSpec((model, tile), lambda j, heads: (0, j)),
                pl.BlockSpec((1, tile), lambda j, heads: (0, j)),
                pl.BlockSpec((tile, model), lambda j, heads: (j, 0)),
                resident((1, model)),
            ],
            out_specs=[
                resident((rows, model)),
                resident((rows, model)),
                resident((rows, model)),
                across,
                across,
                resident((rows, model)),
                resident((rows, model)),
            ],
            scratch_shapes=[pltpu.VMEM((rows, model), jnp.float32)],
        ),
        out_shape=[
            jax.ShapeDtypeStruct((rows, model), jnp.bfloat16),
            jax.ShapeDtypeStruct((rows, model), jnp.float32),
            jax.ShapeDtypeStruct((rows, model), jnp.bfloat16),
            jax.ShapeDtypeStruct((rows, inner), jnp.bfloat16),
            jax.ShapeDtypeStruct((rows, inner), jnp.bfloat16),
            jax.ShapeDtypeStruct((rows, model), jnp.float32),
            jax.ShapeDtypeStruct((rows, model), jnp.bfloat16),
        ],
        cost_estimate=nothing(),
        name="feed_forward",
    )(
        heads, *contexts, cells, out_weight, gain[None], shift[None], up_weight, up_bias[None], down_weight,
        down_bias[None],
    )


def feed_back_kernel(head_ref, two_ref, branch_ref, slope_ref, down_ref, up_ref, hidden_ref, gain_ref, weight_ref,
                     inner_ref, bias_ref, hidden_grad_ref, hidden_grad_b_ref, gain_grad_ref, shift_grad_ref,
                     *rest):
    piece_refs, acc_ref = rest[:-1], rest[-1]
    step = pl.program_id(0)

    @pl.when(step == 0)
    def _():
        acc_ref[...] = jnp.zeros(acc_ref.shape, jnp.float32)

    inner = (nt_dot(branch_ref[...], down_ref[...]) * slope_ref[...].astype(jnp.float32)).astype(jnp.bfloat16)
    inner_ref[...] = inner
    bias_ref[...] = jnp.sum(inner.astype(jnp.float32), axis=0, keepdims=True)
    acc_ref[...] += nt_dot(inner, up_ref[...])

    @pl.when(step == pl.num_programs(0) - 1)
    def _():
        unit, scale = norm_parts(hidden_ref[...])
        grad = acc_ref[...]
        gain_grad_ref[...] = jnp.sum(grad * unit, axis=0, keepdims=True)
        shift_grad_ref[...] = jnp.sum(grad, axis=0, keepdims=True)
        grad = grad * gain_ref[...]
        mean = jnp.mean(grad, axis=-1, keepdims=True)
        slant = jnp.mean(grad * unit, axis=-1, keepdims=True)
        total = two_ref[...] + scale * (grad - mean - unit * slant)
        hidden_grad_ref[...] = total
        total = total.astype(jnp.bfloat16)
        hidden_grad_b_ref[...] = total
        for k, piece_ref in enumerate(piece_refs):
            width = piece_ref.shape[1]
            begin = pl.multiple_of(head_ref[k] * width, width)
            piece_ref[...] = nt_dot(total, weight_ref[pl.ds(begin, width), :]).astype(jnp.bfloat16)


def feed_back(heads, grad_two, grad_branch, slope, down_weight, up_weight, hidden, gain, out_weight):
    rows, model = hidden.shape
    inner = up_weight.shape[1]
    tile = FEED_TILE
    count = heads.shape[0]
    return pl.pallas_call(
        feed_back_kernel,
        grid_spec=pltpu.PrefetchScalarGridSpec(
            num_scalar_prefetch=1,
            grid=(inner // tile,),
            in_specs=[
                resident((rows, model)),
                resident((rows, model)),
                pl.BlockSpec((rows, tile), lambda j, heads: (0, j)),
                pl.BlockSpec((tile, model), lambda j, heads: (j, 0)),
                pl.BlockSpec((model, tile), lambda j, heads: (0, j)),
                resident((rows, model)),
                resident((1, model)),
                resident((model, model)),
            ],
            out_specs=[
                pl.BlockSpec((rows, tile), lambda j, heads: (0, j)),
                pl.BlockSpec((1, tile), lambda j, heads: (0, j)),
                resident((rows, model)),
                resident((rows, model)),
                resident((1, model)),
                resident((1, model)),
            ]
            + [resident((rows, model // count))] * count,
            scratch_shapes=[pltpu.VMEM((rows, model), jnp.float32)],
        ),
        out_shape=[
            jax.ShapeDtypeStruct((rows, inner), jnp.bfloat16),
            jax.ShapeDtypeStruct((1, inner), jnp.float32),
            jax.ShapeDtypeStruct((rows, model), jnp.float32),
            jax.ShapeDtypeStruct((rows, model), jnp.bfloat16),
            jax.ShapeDtypeStruct((1, model), jnp.float32),
            jax.ShapeDtypeStruct((1, model), jnp.float32),
        ]
        + [jax.ShapeDtypeStruct((rows, model // count), jnp.bfloat16)] * count,
        cost_estimate=nothing(),
        name="feed_back",
    )(heads, grad_two, grad_branch, slope, down_weight, up_weight, hidden, gain[None], out_weight)


def tn_dot(left, right):
    return lax.dot_general(left, right, (((0,), (0,)), ((), ())), preferred_element_type=jnp.float32)


def weights_kernel(lefts_at, ready, place_ref, column_ref, *refs):
    count = len(lefts_at)
    scratch = 0 if ready else count
    lefts = refs[: max(lefts_at) + 1]
    rights = refs[len(lefts) : len(lefts) + count]
    refs, ordered = refs[len(lefts) + count : len(refs) - scratch], refs[len(refs) - scratch :]
    vector_ref, (keep_ref, send_ref) = refs[:-2], refs[-2:]
    held, grouped, _, width = keep_ref.shape
    if ready:
        ordered = rights
    else:

        @pl.when(pl.program_id(0) == 0)
        def _():
            for right_ref, ordered_ref in zip(rights, ordered):
                for piece in range(2 * held):
                    begin = pl.multiple_of(column_ref[piece] * width, width)
                    ordered_ref[:, piece * width : (piece + 1) * width] = right_ref[:, pl.ds(begin, width)]

    begin = 0
    for at, ordered_ref in zip(lefts_at, ordered):
        total = lefts[at].shape[1]
        tile = min(total, 256)
        rows = min(tile, total // grouped)
        for first in range(0, total, tile):
            value = tn_dot(lefts[at][:, first : first + tile], ordered_ref[...]).astype(jnp.bfloat16)
            for inside in range(0, tile, rows):
                z, row = divmod(first + inside, total // grouped)
                part = value[inside : inside + rows]
                place = slice(begin + row, begin + row + rows)
                for piece in range(held):
                    keep_ref[piece, z, place, :] = part[:, piece * width : (piece + 1) * width]
                    other = held + piece
                    send_ref[piece, z, place, :] = part[:, other * width : (other + 1) * width]
        begin += total // grouped

    if vector_ref:
        keep_ref[:, :, begin:, :] = vector_ref[0][0]
        send_ref[:, :, begin:, :] = vector_ref[0][1]


def relative_columns(value, steps):
    group = lax.axis_index("dp")
    masks = relative_masks(steps)
    size = value.shape[1] // len(masks)
    return jnp.concatenate([chunk(value, (group ^ mask) * size, size, 1) for mask in masks], axis=1)


def weight_pieces(pairs, steps, vector=None):
    blocks, block = lax.axis_size("blk"), lax.axis_index("blk")
    pieces, group = lax.axis_size("dp"), lax.axis_index("dp")
    width = D // pieces
    masks = relative_masks(blk_masks())
    sizes = [left.shape[1] // blocks for left, _, _ in pairs]
    places = jnp.stack([block ^ mask for mask in masks])
    columns = jnp.stack([group ^ mask for mask in relative_masks(steps)])
    cells = pairs[0][1].shape[0]
    lefts, lefts_at = [], []
    for left, _, _ in pairs:
        if not any(left is seen for seen in lefts):
            lefts.append(left)
        lefts_at.append(next(i for i, seen in enumerate(lefts) if left is seen))
    rights = [right for _, right, _ in pairs]
    parts = [part for _, _, part in pairs]
    grouped = max(1, 128 // min(sizes))
    ready = grouped > 1 or width % 128 != 0
    if ready:
        rights = [
            relative_columns(right[:, part * D : (part + 1) * D], steps) for right, part in zip(rights, parts)
        ]
        parts = [0] * len(parts)
        lefts = [
            jnp.concatenate(
                [chunk(left, (block ^ mask) * (left.shape[1] // blocks), left.shape[1] // blocks, 1) for mask in masks],
                axis=1,
            )
            for left in lefts
        ]
        places = jnp.arange(blocks, dtype=jnp.int32)
    rows = sum(sizes) + (0 if vector is None else vector.shape[3])
    out = pl.BlockSpec((pieces // 2, grouped, rows, width), lambda z, place, column: (0, z, 0, 0))
    specs = [
        pl.BlockSpec((cells, left.shape[1] // blocks * grouped), lambda z, place, column: (0, place[z]))
        for left in lefts
    ]
    specs += [pl.BlockSpec((cells, D), lambda z, place, column, part=part: (0, part)) for part in parts]
    operands = lefts + rights
    if vector is not None:
        specs.append(
            pl.BlockSpec(
                (2, pieces // 2, grouped, vector.shape[3], width), lambda z, place, column: (0, 0, z, 0, 0)
            )
        )
        operands.append(vector)
    shape = jax.ShapeDtypeStruct((pieces // 2, blocks, rows, width), jnp.bfloat16)
    return pl.pallas_call(
        partial(weights_kernel, lefts_at, ready),
        grid_spec=pltpu.PrefetchScalarGridSpec(
            num_scalar_prefetch=2,
            grid=(blocks // grouped,),
            in_specs=specs,
            out_specs=[out, out],
            scratch_shapes=[pltpu.VMEM((cells, D), jnp.bfloat16) for _ in pairs if not ready],
        ),
        out_shape=[shape, shape],
        cost_estimate=nothing(),
        name="weight_pieces",
    )(places, columns, *operands)


def weight_steps(keep, send, flipped, parts):
    steps = dp_order(flipped)
    (came,) = yield [send], by_mask(steps[0], 0)
    size = keep.shape[0]
    terms = [[keep[place], came[place]] for place in range(size)]
    for mask in steps[1:]:
        size = size // 2
        came = yield [summed(terms[place]) for place in range(size, 2 * size)], by_mask(mask, 0)
        terms = [terms[place] + [came[place]] for place in range(size)]
    terms = terms[0]
    size = keep.shape[1]
    for mask in blk_masks():
        size = size // 2
        (came,) = yield [summed([term[size : 2 * size] for term in terms])], by_mask(0, mask)
        terms = [term[:size] for term in terms] + [came]
    value = summed(terms)
    for mask in steps[:0:-1]:
        (came,) = yield [value], by_mask(mask, 0)
        value = jnp.concatenate([value, came], axis=0)
    (came,) = yield [value], by_mask(steps[0], 0)
    return spread_columns(value, came, relative_table(steps, lax.axis_index("dp")), parts)


def local(
    cell_states,
    slide_lengths,
    cell_mask,
    latent_noise,
    train_step,
    attn_gain,
    attn_shift,
    query_weight,
    key_weight,
    value_weight,
    out_weight,
    ffn_gain,
    ffn_shift,
    up_weight,
    up_bias,
    down_weight,
    down_bias,
    encode_weight,
    encode_bias,
    decode_weight,
    prior_means,
    prior_logits,
    out_grad,
):
    rows_here = cell_states.shape[0]
    blocks = lax.axis_size("blk")
    group, block = lax.axis_index("dp"), lax.axis_index("blk")
    width = D // blocks
    x_float = cell_states.astype(jnp.float32)
    _, norm_back = jax.vjp(layer_norm, x_float, attn_gain, attn_shift)
    weights = (query_weight, key_weight, value_weight)
    held, pieces = group_rows(
        with_meta(cell_states, cell_mask, slide_lengths[0]),
        lambda pieces, held: entry(pieces, attn_gain, attn_shift, weights, held),
    )
    normed_b, queries, keys, values = held
    meta = jnp.zeros((blocks, D), jnp.bfloat16)
    order = jnp.arange(blocks, dtype=jnp.int32)
    for mine, other, place in pieces:
        row = jnp.where(at_home(group, block), mine[rows_here], other[rows_here])
        meta = jnp.where(order[:, None] == place, row[None], meta)
    mask_all, lengths_row = from_meta(meta, rows_here, slide_lengths.shape[1])
    ranges, query_code, key_code = slide_tables(lengths_row, mask_all)
    context_here, log_total = attention_forward(ranges, queries, keys, values, query_code, key_code)
    contexts = rows_to_owners(context_here)
    owner_heads = heads_at_owner()
    context_b, hidden, normed_two_b, activated_b, slope_b, hidden_two, hidden_two_b = feed_forward(
        owner_heads, contexts, cell_states, out_weight, ffn_gain, ffn_shift, up_weight, up_bias, down_weight,
        down_bias,
    )
    if width % 128:
        context_b = jnp.zeros((rows_here, D), jnp.bfloat16)
        for k in range(blocks):
            context_b = lax.dynamic_update_slice_in_dim(context_b, contexts[k], owner_heads[k] * width, 1)
    encoded = plain_dot(hidden_two_b, encode_weight) + encode_bias
    latent_mean = encoded[:, :LAT]
    latent_logvar = encoded[:, LAT:]
    spread = jnp.exp(0.5 * latent_logvar)
    noise_float = latent_noise.astype(jnp.float32)
    latent_b = (latent_mean + spread * noise_float).astype(jnp.bfloat16)
    output = hidden_two + plain_dot(latent_b, decode_weight)
    (kl_dim, categorical), kl_back = jax.vjp(
        kl_terms, latent_mean, latent_logvar, prior_means, prior_logits
    )
    real = cell_mask.astype(jnp.float32)
    sums = jnp.concatenate(
        [
            jnp.sum(kl_dim * real[:, None], axis=0),
            jnp.sum(categorical * real)[None],
            jnp.sum(real)[None],
            jnp.zeros((126,), jnp.float32),
        ]
    )
    sums = summed_everywhere(sums)
    kl_sum, cat_sum, count = sums[:LAT], sums[LAT], sums[LAT + 1]
    kbar = kl_sum / count
    floored = jnp.sum(jnp.maximum(kbar, free_floor))
    cat_mean = cat_sum / count
    beta = jnp.minimum(1.0, (train_step[0].astype(jnp.float32) + 1.0) / WARM)
    active = (kbar > free_floor).astype(jnp.float32)
    grad_latent = cols_dot(out_grad, decode_weight)
    grad_mean, grad_logvar, grad_means, grad_prior = kl_back(
        (beta * real[:, None] * active[None, :], beta * real)
    )
    grad_mean = grad_mean + grad_latent
    grad_logvar = grad_logvar + grad_latent * 0.5 * spread * noise_float
    grad_encoded_b = jnp.concatenate([grad_mean, grad_logvar], axis=1).astype(jnp.bfloat16)
    grad_encode_bias = jnp.sum(grad_encoded_b.astype(jnp.float32), axis=0)
    grad_two = out_grad.astype(jnp.float32) + cols_dot(grad_encoded_b, encode_weight)
    grad_down_bias = jnp.sum(grad_two, axis=0)
    grad_branch_b = grad_two.astype(jnp.bfloat16)

    straight, flipped = dp_order(False), dp_order(True)
    block_rows = D // blocks
    down = Exchange(
        weight_steps(
            *weight_pieces(
                [(activated_b, grad_branch_b, 0), (hidden_two_b, grad_encoded_b, 0), (latent_b, out_grad, 0)],
                straight,
            ),
            False,
            [(4 * block_rows, 1), (block_rows, 1), (block_rows // 2, 1)],
        )
    )
    back = feed_back(
        owner_heads, grad_two, tied(grad_branch_b, down.last), slope_b, down_weight, up_weight, hidden, ffn_gain,
        out_weight,
    )
    grad_inner_b, grad_up_bias, grad_hidden, grad_attn_b, grad_ffn_gain, grad_ffn_shift = back[:6]
    grads_here = heads_to_workers(back[6:])
    token = grads_here
    by_block = lambda part: part.reshape(blocks, -1)
    means_block = jnp.moveaxis(grad_means.reshape(K, blocks, LAT // blocks), 1, 0)
    vectors = [
        by_block(grad_ffn_gain),
        by_block(grad_ffn_shift),
        by_block(grad_up_bias),
        by_block(grad_down_bias),
        by_block(grad_encode_bias),
        by_block(means_block),
        by_block(grad_prior),
    ]
    sizes = [part.shape[1] for part in vectors]
    vector = jnp.concatenate([part.astype(jnp.bfloat16) for part in vectors], axis=1)
    vector_rows = -(-sum(sizes) // (8 * D)) * 8
    vector = jnp.pad(vector, ((0, 0), (0, vector_rows * D - sum(sizes))))
    vector = relative_columns(vector.reshape(blocks * vector_rows, D), flipped)
    devices_along = lax.axis_size("dp")
    vector = vector.reshape(blocks, vector_rows, 2, devices_along // 2, D // devices_along)
    vector = jnp.transpose(vector, (2, 3, 0, 1, 4))
    vector = jnp.concatenate([chunk(vector, block ^ mask, 1, 2) for mask in relative_masks(blk_masks())], axis=2)
    up = Exchange(
        weight_steps(
            *weight_pieces(
                [(normed_two_b, tied(grad_inner_b, token), part) for part in range(4)]
                + [(context_b, grad_attn_b, 0)],
                flipped,
                vector,
            ),
            True,
            [(block_rows, 4), (block_rows, 1), (vector_rows, 1)],
        )
    )
    token = down.advance(up.last)
    token = up.advance(token)
    grads = attention_backward(
        ranges, rows_at_worker(), tied(queries, token), grads_here, context_here, log_total, keys, values, query_code,
        key_code,
    )
    grads = tied(grads, (down.flight[0], up.flight[0]))
    partial_rows, grad_heads, part_gain, part_shift = project_back(normed_b, grads, weights)
    partial_rows, grad_heads = tied((partial_rows, grad_heads), (down.flight, up.flight))
    row_sum = Exchange(row_steps(partial_rows))
    part_shift = part_shift[0]
    part_gain = (part_gain[0] - attn_shift * part_shift) / attn_gain
    token = down.advance(grad_heads)
    token = up.advance(token)
    extra = jnp.concatenate([by_block(part_gain), by_block(part_shift)], axis=1)
    extra_size = extra.shape[1]
    extra = jnp.pad(extra, ((0, 0), (0, 3 * width - extra_size))).astype(jnp.bfloat16)
    pieces = lax.axis_size("dp") // 2
    piece_rows = block_rows // pieces
    grad_heads = grad_heads.reshape(blocks, pieces, piece_rows, 3 * width)
    extra = jnp.broadcast_to(extra[:, None, None, :], (blocks, pieces, 8, 3 * width))
    attn = Exchange(head_steps(jnp.concatenate([grad_heads, extra], axis=2)))
    token = attn.last
    order = [row_sum, attn, down, up, row_sum, attn]
    live = [down, row_sum, up, attn]
    for bundle in order:
        token = bundle.advance(token)
    while any(bundle.result is None for bundle in live):
        for bundle in live:
            if bundle.result is None:
                token = bundle.advance(token)
    grad_normed = row_sum.result.astype(jnp.float32)
    grad_from_norm, _, _ = norm_back(grad_normed)
    states_grad = grad_hidden + grad_from_norm
    mine, other = attn.result
    attn_vector = jnp.sum((mine[0].astype(jnp.float32) + other[0].astype(jnp.float32)), axis=0)[piece_rows]
    main = spread_heads(mine, other, piece_rows)
    down_sum, encode_sum, decode_sum = down.result
    up_sum, out_sum, vector_sum = up.result
    flat = vector_sum.reshape(-1)
    small, begin = [], 0
    for size in sizes:
        small.append(flat[begin : begin + size])
        begin += size
    totals = (
        attn_vector[: extra_size // 2],
        attn_vector[extra_size // 2 : extra_size],
        main[0],
        main[1],
        main[2],
        out_sum,
        small[0],
        small[1],
        up_sum,
        small[2],
        down_sum,
        small[3],
        encode_sum,
        small[4],
        decode_sum,
        small[5].reshape(K, LAT // blocks),
        small[6],
    )
    kl_out = (floored / LAT + cat_mean).reshape(1)
    return (output.astype(jnp.bfloat16), states_grad, kl_out) + tuple(totals)


def solution(mesh):
    in_specs = (
        P(("dp", "blk"), None),
        P("dp", None),
        P(("dp", "blk")),
        P(("dp", "blk"), None),
        P(),
        P(),
        P(),
        P(),
        P(),
        P(),
        P(),
        P(),
        P(),
        P(),
        P(),
        P(),
        P(),
        P(),
        P(),
        P(),
        P(),
        P(),
        P(("dp", "blk"), None),
    )
    out_specs = (
        P(("dp", "blk"), None),
        P(("dp", "blk"), None),
        P(),
        P("blk"),
        P("blk"),
        P("blk", None),
        P("blk", None),
        P("blk", None),
        P("blk", None),
        P("blk"),
        P("blk"),
        P("blk", None),
        P("blk"),
        P("blk", None),
        P("blk"),
        P("blk", None),
        P("blk"),
        P("blk", None),
        P(None, "blk"),
        P("blk"),
    )
    return jax.shard_map(local, mesh=mesh, in_specs=in_specs, out_specs=out_specs, check_vma=False)
```

```python
import math
from functools import partial

import jax
import jax.numpy as jnp
from jax import lax
from jax.experimental import pallas as pl
from jax.experimental.pallas import tpu as pltpu
from jax.sharding import PartitionSpec as P

D = 1024
H = 16
HD = 64
LAT = 512
K = 16
WARM = 2000


ln_eps = 1e-05
free_floor = 1.3
neg_fill = -1e30

QUERY_TILE = 256
KEY_TILE = 384
ROW_TILE = 512
KEY_UNIT = 128
FEED_TILE = 512


def layer_norm(values, gain, shift):
    center = values - jnp.mean(values, axis=-1, keepdims=True)
    spread = jnp.mean(center * center, axis=-1, keepdims=True)
    return center * lax.rsqrt(spread + ln_eps) * gain + shift


def slide_index(position, lengths_row):
    ends = jnp.cumsum(lengths_row)
    return jnp.sum((position[:, None] >= ends[None, :]).astype(jnp.int32), axis=1)


def exact_dot(left, right):
    return jnp.dot(left, right, precision=lax.Precision.HIGHEST, preferred_element_type=jnp.float32)


def kl_terms(latent_mean, latent_logvar, prior_means, prior_logits):
    log_prior = jax.nn.log_softmax(prior_logits)
    logits = exact_dot(latent_mean, prior_means.T) * LAT ** (-0.5) + log_prior[None, :]
    resp = jax.nn.softmax(logits, axis=-1)
    log_resp = jax.nn.log_softmax(logits, axis=-1)
    mixed_mean = exact_dot(resp, prior_means)
    mixed_square = exact_dot(resp, prior_means * prior_means)
    kl_dim = 0.5 * (
        jnp.exp(latent_logvar)
        + latent_mean * latent_mean
        - 2.0 * latent_mean * mixed_mean
        + mixed_square
        - 1.0
        - latent_logvar
    )
    categorical = jnp.sum(resp * (log_resp - log_prior[None, :]), axis=-1)
    return (kl_dim, categorical)


def plain_dot(left, right):
    return jnp.dot(left, right, preferred_element_type=jnp.float32)


def rows_dot(left, right):
    return lax.dot_general(
        left, right, (((0,), (0,)), ((), ())), preferred_element_type=jnp.float32
    )


def cols_dot(left, right):
    return lax.dot_general(
        left, right, (((1,), (1,)), ((), ())), preferred_element_type=jnp.float32
    )


MESH_AXES = ("dp", "blk")


def swapped(value, dp_mask, blk_mask):
    groups, blocks = lax.axis_size("dp"), lax.axis_size("blk")
    pairs = [
        (g * blocks + b, (g ^ dp_mask) * blocks + (b ^ blk_mask))
        for g in range(groups)
        for b in range(blocks)
    ]
    return lax.ppermute(value, MESH_AXES, pairs)


def bits_of(count):
    return count.bit_length() - 1


def dp_masks():
    return [1 << t for t in range(bits_of(lax.axis_size("dp")))]


def blk_masks():
    return [(2 << t) - 1 for t in range(bits_of(lax.axis_size("blk")))]


def tree_sum(value, masks):
    places = [(0, 0)]
    for dp_mask, blk_mask in masks:
        places = places + [(dp ^ dp_mask, blk ^ blk_mask) for dp, blk in places]
    terms = [value] + [swapped(value, dp, blk) for dp, blk in places[1:]]
    while len(terms) > 1:
        terms = [terms[i] + terms[i + 1] for i in range(0, len(terms), 2)]
    return terms[0]


def summed_everywhere(value):
    value = tree_sum(value, [(1, 0)])
    value = tree_sum(value, [(mask, 0) for mask in dp_masks()[1:]])
    return tree_sum(value, [(0, mask) for mask in blk_masks()])


def added(left, right):
    return (left.astype(jnp.float32) + right.astype(jnp.float32)).astype(jnp.bfloat16)


def summed(terms):
    total = terms[0].astype(jnp.float32)
    for term in terms[1:]:
        total = total + term.astype(jnp.float32)
    return total.astype(jnp.bfloat16)


def chunk(value, start, size, axis):
    return lax.dynamic_slice_in_dim(value, start, size, axis)


def tied(value, other):
    return lax.optimization_barrier((value, other))[0]


class Exchange:
    def __init__(self, steps):
        self.steps = steps
        self.result = None
        self.last = None
        self.flight = None
        self._take(lambda: next(self.steps))

    def _take(self, step, hold=False):
        try:
            values, permute = step()
            first = len(values) // 2 if hold else len(values)
            self.last = values
            self.flight = [permute(value) for value in values[:first]]
            self.held = (values[first:], permute)
        except StopIteration as end:
            self.result = end.value
            self.last = end.value
            self.flight = None

    def advance(self, token, hold=False):
        came = tied(self.flight, token)
        self._take(lambda: self.steps.send(came), hold)
        return self.last

    def release(self, token):
        values, permute = self.held
        self.flight = self.flight + [permute(tied(value, token)) for value in values]


def by_mask(dp_mask, blk_mask):
    return lambda value: swapped(value, dp_mask, blk_mask)


def dp_order(flipped):
    masks = dp_masks()
    return masks[:1] + masks[1:][::-1] if flipped else masks


def relative_masks(steps):
    places = [0]
    for step in steps[::-1]:
        places = places + [place ^ step for place in places]
    return places


def relative_table(steps, mine):
    masks = relative_masks(steps)
    inverse = [masks.index(place) for place in range(len(masks))]
    order = jnp.arange(len(masks), dtype=jnp.int32)
    wanted = order ^ mine
    return sum(jnp.where(wanted == place, inverse[place], 0) for place in range(len(masks)))


def spread_kernel(parts, table_ref, mine_ref, other_ref, *out_refs):
    held, _, width = mine_ref.shape
    cols = 2 * held * width
    for place in range(2 * held):
        index = table_ref[place]
        piece = jnp.where(index < held, mine_ref[index & (held - 1)], other_ref[index & (held - 1)])
        piece = piece.astype(jnp.float32)
        for out_ref, (begin, count, times) in zip(out_refs, parts):
            for time in range(times):
                row, column = begin + time * count, time * cols + place * width
                out_ref[:, column : column + width] = piece[row : row + count]


def spread_columns(mine, other, table, parts):
    held, rows, width = mine.shape
    cols = 2 * held * width
    begin, placed, shapes = 0, [], []
    for count, times in parts:
        placed.append((begin, count, times))
        shapes.append(jax.ShapeDtypeStruct((count, times * cols), jnp.float32))
        begin += count * times
    return pl.pallas_call(
        partial(spread_kernel, placed),
        out_shape=shapes,
        grid_spec=pltpu.PrefetchScalarGridSpec(
            num_scalar_prefetch=1,
            grid=(1,),
            in_specs=[resident((held, rows, width))] * 2,
            out_specs=[resident(shape.shape) for shape in shapes],
        ),
        cost_estimate=nothing(),
        name="spread_columns",
    )(table, mine, other)


def head_steps(value):
    blocks = lax.axis_size("blk")
    group, block = lax.axis_index("dp"), lax.axis_index("blk")
    half = blocks // 2
    steps = dp_masks()[1:]
    masks = relative_masks([step >> 1 for step in steps])
    taken = [[chunk(value, (group >> 1) ^ mask, 1, 1)] for mask in masks]
    size = len(masks)
    for step in steps:
        size = size // 2
        send = jnp.concatenate([summed(taken[place]) for place in range(size, 2 * size)], axis=1)
        (came,) = yield [send], by_mask(step, 0)
        taken = [taken[place] + [came[:, place : place + 1]] for place in range(size)]
    side = block >> (bits_of(blocks) - 1)
    away = [chunk(term, (1 - side) * half, half, 0) for term in taken[0]]
    (came,) = yield [summed(away)], by_mask(0, half)
    terms = [chunk(term, side * half, half, 0) for term in taken[0]] + [came]
    place = block & (half - 1)
    pieces = [summed([chunk(term, place, 1, 0) for term in terms])]
    for k in range(1, half):
        send = summed([chunk(term, place ^ k, 1, 0) for term in terms])
        (came,) = yield [send], by_mask(0, k)
        pieces.append(came)
    value = jnp.concatenate(pieces, axis=1)
    for step in steps[::-1]:
        (came,) = yield [value], by_mask(step, 0)
        value = jnp.concatenate([value, came], axis=0)
    (other,) = yield [value], by_mask(1, 0)
    return value, other


def heads_kernel(table_ref, mine_ref, other_ref, *out_refs):
    pieces = pl.num_programs(0)
    place, core = table_ref[pieces], table_ref[pieces + 1]
    half = mine_ref.shape[1]
    rows = out_refs[0].shape[0]
    width = mine_ref.shape[3] // 3
    for chip in range(half):
        mine = mine_ref[0, chip ^ place].astype(jnp.float32)
        other = other_ref[0, chip ^ place].astype(jnp.float32)
        for c in range(2):
            value = jnp.where(core == c, mine, other)
            column = (2 * chip + c) * width
            for kind in range(3):
                out_refs[kind][:, column : column + width] = value[:rows, kind * width : (kind + 1) * width]


def spread_heads(mine, other, rows):
    blocks = lax.axis_size("blk")
    group, block = lax.axis_index("dp"), lax.axis_index("blk")
    pieces, half, held_rows, width = mine.shape
    table = relative_table([step >> 1 for step in dp_masks()[1:]], group >> 1)
    table = jnp.concatenate([table, jnp.stack([block & (half - 1), group & 1])])
    held = pl.BlockSpec((1, half, held_rows, width), lambda i, table: (table[i], 0, 0, 0))
    cols = 2 * half * width // 3
    return pl.pallas_call(
        heads_kernel,
        out_shape=(jax.ShapeDtypeStruct((pieces * rows, cols), jnp.float32),) * 3,
        grid_spec=pltpu.PrefetchScalarGridSpec(
            num_scalar_prefetch=1,
            grid=(pieces,),
            in_specs=[held, held],
            out_specs=[pl.BlockSpec((rows, cols), lambda i, table: (i, 0))] * 3,
        ),
        cost_estimate=nothing(),
        name="spread_heads",
    )(table, mine, other)


def head_lanes(value, head):
    lane = lax.broadcasted_iota(jnp.int32, value.shape, 1) // HD
    return jnp.where(lane == head, value, jnp.zeros_like(value))

def nt_dot(left, right):
    return lax.dot_general(left, right, (((1,),(1,)),((),())), preferred_element_type=jnp.float32)

def nn_dot(left, right):
    return lax.dot_general(left, right, (((1,),(0,)),((),())), preferred_element_type=jnp.float32)

def allowed_pairs(code_k, code_q, block_k, tile):
    key_pos = block_k + lax.broadcasted_iota(jnp.int32, tile, 0)
    query_pos = pl.program_id(0) * QUERY_TILE + lax.broadcasted_iota(jnp.int32, tile, 1)
    return (code_k == code_q) | (key_pos == query_pos)

def forward_kernel(range_ref, q_ref, k_ref, v_ref, cq_ref, ck_ref, ctx_ref, lse_ref, m_ref, l_ref, acc_ref, vt_ref):
    nh = q_ref.shape[1] // HD
    step = pl.program_id(0)

    @pl.when(step == 0)
    def _():
        vt_ref[...] = v_ref[...].T

    m_ref[...] = jnp.full(m_ref.shape, neg_fill, jnp.float32)
    l_ref[...] = jnp.zeros(l_ref.shape, jnp.float32)
    acc_ref[...] = jnp.zeros(acc_ref.shape, jnp.float32)
    code_q = cq_ref[...]
    scaled = (q_ref[...].astype(jnp.float32) * HD ** (-0.5)).astype(jnp.bfloat16)
    def body(kb, _):
        start = pl.multiple_of(range_ref[step, 0] * KEY_UNIT + kb * KEY_TILE, KEY_UNIT)
        keys = k_ref[pl.ds(start, KEY_TILE), :]
        open_pair = allowed_pairs(ck_ref[pl.ds(start, KEY_TILE), :], code_q, start, (KEY_TILE, QUERY_TILE))
        bias = jnp.where(open_pair, 0.0, neg_fill)
        rows = [slice(h * HD, (h + 1) * HD) for h in range(nh)]
        scores = [nt_dot(keys[:, rows[h]], scaled[:, rows[h]]) + bias for h in range(nh)]
        probs, scales = [], []
        for h in range(nh):
            m_old = m_ref[h : h + 1, :]
            m_new = jnp.maximum(m_old, jnp.max(scores[h], axis=0, keepdims=True))
            p = jnp.exp(scores[h] - m_new)
            alpha = jnp.exp(m_old - m_new)
            l_ref[h : h + 1, :] = l_ref[h : h + 1, :] * alpha + jnp.sum(p, axis=0, keepdims=True)
            m_ref[h : h + 1, :] = m_new
            probs.append(p.astype(jnp.bfloat16))
            scales.append(alpha)
        for h in range(nh):
            part = nn_dot(vt_ref[rows[h], pl.ds(start, KEY_TILE)], probs[h])
            acc_ref[rows[h], :] = acc_ref[rows[h], :] * scales[h] + part
        return 0
    lax.fori_loop(0, range_ref[step, 1], body, 0)
    for h in range(nh):
        rows = slice(h*HD, (h+1)*HD)
        acc_ref[rows, :] = acc_ref[rows, :] / l_ref[h:h+1, :]
    ctx_ref[...] = acc_ref[...].T.astype(jnp.bfloat16)
    lse_ref[...] = m_ref[...] + jnp.log(l_ref[...])

def attention_forward(ranges, q, k, v, code_q, code_k):
    N, W = q.shape
    nh = W // HD
    full = lambda shape: pl.BlockSpec(shape, lambda i, r: (0,)*len(shape))
    return pl.pallas_call(
        forward_kernel,
        out_shape=(jax.ShapeDtypeStruct((N, W), jnp.bfloat16), jax.ShapeDtypeStruct((nh, N), jnp.float32)),
        grid_spec=pltpu.PrefetchScalarGridSpec(
            num_scalar_prefetch=1, grid=(N//QUERY_TILE,),
            in_specs=[pl.BlockSpec((QUERY_TILE, W), lambda i, r: (i, 0)), full((N, W)), full((N, W)),
                      pl.BlockSpec((1, QUERY_TILE), lambda i, r: (0, i)), full((N, 1))],
            out_specs=[pl.BlockSpec((QUERY_TILE, W), lambda i, r: (i, 0)), pl.BlockSpec((nh, QUERY_TILE), lambda i, r: (0, i))],
            scratch_shapes=[pltpu.VMEM((nh, QUERY_TILE), jnp.float32), pltpu.VMEM((nh, QUERY_TILE), jnp.float32), pltpu.VMEM((W, QUERY_TILE), jnp.float32), pltpu.VMEM((W, N), jnp.bfloat16)]),
        cost_estimate=nothing(),
        name="attention_forward",
    )(ranges, q, k, v, code_q, code_k)

def backward_kernel(range_ref, row_ref, q_ref, ctx_ref, lse_ref, k_ref, v_ref, cq_ref, ck_ref,
                    *refs):
    pieces = row_ref.shape[0]
    do_refs, (dq_ref, dk_ref, dv_ref, dqt_ref, dk_acc, dv_acc, kt_ref, do_ref) = refs[:pieces], refs[pieces:]
    nh = q_ref.shape[1] // HD
    step = pl.program_id(0)
    @pl.when(step == 0)
    def _():
        dk_acc[...] = jnp.zeros(dk_acc.shape, jnp.float32)
        dv_acc[...] = jnp.zeros(dv_acc.shape, jnp.float32)
        kt_ref[...] = k_ref[...].T
        for k, piece_ref in enumerate(do_refs):
            rows = piece_ref.shape[0]
            do_ref[pl.ds(pl.multiple_of(row_ref[k] * rows, rows), rows), :] = piece_ref[...]

    dqt_ref[...] = jnp.zeros(dqt_ref.shape, jnp.float32)
    code_q = cq_ref[...]
    scaled = (q_ref[...].astype(jnp.float32) * HD ** (-0.5)).astype(jnp.bfloat16)
    grads = do_ref[pl.ds(pl.multiple_of(step * QUERY_TILE, QUERY_TILE), QUERY_TILE), :]
    product = (grads.astype(jnp.float32) * ctx_ref[...].astype(jnp.float32)).T
    deltas = [jnp.sum(product[h*HD:(h+1)*HD, :], axis=0, keepdims=True) for h in range(nh)]
    q_all = jnp.concatenate([head_lanes(scaled, h) for h in range(nh)], axis=0)
    do_all = jnp.concatenate([head_lanes(grads, h) for h in range(nh)], axis=0)
    def body(kb, _):
        start = pl.multiple_of(range_ref[step, 0] * KEY_UNIT + kb * KEY_TILE, KEY_UNIT)
        keys = k_ref[pl.ds(start, KEY_TILE), :]
        values = v_ref[pl.ds(start, KEY_TILE), :]
        open_pair = allowed_pairs(ck_ref[pl.ds(start, KEY_TILE), :], code_q, start, (KEY_TILE, QUERY_TILE))
        bias = jnp.where(open_pair, 0.0, neg_fill)
        cols = [slice(h * QUERY_TILE, (h + 1) * QUERY_TILE) for h in range(nh)]
        scores = [nt_dot(keys, q_all[cols[h], :]) + bias for h in range(nh)]
        dps = [nt_dot(values, do_all[cols[h], :]) for h in range(nh)]
        ps = [jnp.exp(scores[h] - lse_ref[h : h + 1, :]) for h in range(nh)]
        dss = [(ps[h] * (dps[h] - deltas[h])).astype(jnp.bfloat16) for h in range(nh)]
        ps = [p.astype(jnp.bfloat16) for p in ps]
        for h in range(nh):
            rows = slice(h * HD, (h + 1) * HD)
            dqt_ref[rows, :] += nn_dot(kt_ref[rows, pl.ds(start, KEY_TILE)], dss[h])
        dv_acc[pl.ds(start, KEY_TILE), :] += nn_dot(jnp.concatenate(ps, axis=1), do_all)
        dk_acc[pl.ds(start, KEY_TILE), :] += nn_dot(jnp.concatenate(dss, axis=1), q_all)
        return 0
    lax.fori_loop(0, range_ref[step, 1], body, 0)
    dq_ref[...] = (dqt_ref[...] * HD ** (-0.5)).T.astype(jnp.bfloat16)
    @pl.when(step == pl.num_programs(0) - 1)
    def _():
        dk_ref[...] = dk_acc[...].astype(jnp.bfloat16)
        dv_ref[...] = dv_acc[...].astype(jnp.bfloat16)

def attention_backward(ranges, places, q, pieces, ctx, lse, k, v, code_q, code_k):
    cells, width = q.shape
    heads = width // HD

    def row():
        return pl.BlockSpec((QUERY_TILE, width), lambda i, *_: (i, 0))

    out = jax.ShapeDtypeStruct((cells, width), jnp.bfloat16)
    return pl.pallas_call(
        backward_kernel,
        out_shape=(out, out, out),
        grid_spec=pltpu.PrefetchScalarGridSpec(
            num_scalar_prefetch=2,
            grid=(cells // QUERY_TILE,),
            in_specs=[
                row(),
                row(),
                pl.BlockSpec((heads, QUERY_TILE), lambda i, *_: (0, i)),
                resident((cells, width)),
                resident((cells, width)),
                pl.BlockSpec((1, QUERY_TILE), lambda i, *_: (0, i)),
                resident((cells, 1)),
            ]
            + [resident(piece.shape) for piece in pieces],
            out_specs=[row(), resident((cells, width)), resident((cells, width))],
            scratch_shapes=[
                pltpu.VMEM((width, QUERY_TILE), jnp.float32),
                pltpu.VMEM((cells, width), jnp.float32),
                pltpu.VMEM((cells, width), jnp.float32),
                pltpu.VMEM((width, cells), jnp.bfloat16),
                pltpu.VMEM((cells, width), jnp.bfloat16),
            ],
        ),
        cost_estimate=nothing(),
        name="attention_backward",
    )(ranges, places, q, ctx, lse, k, v, code_q, code_k, *pieces)


def slide_tables(lengths_row, mask_all):
    cells = mask_all.shape[0]
    ends = jnp.cumsum(lengths_row)
    starts = ends - lengths_row
    slide = slide_index(jnp.arange(cells, dtype=jnp.int32), lengths_row)
    first = jnp.arange(cells // QUERY_TILE, dtype=jnp.int32) * QUERY_TILE
    first_slide = slide_index(first, lengths_row)
    last_slide = slide_index(first + (QUERY_TILE - 1), lengths_row)
    order = jnp.arange(lengths_row.shape[0], dtype=jnp.int32)

    def picked(table, index):
        return jnp.sum(jnp.where(index[:, None] == order[None, :], table[None, :], 0), axis=1)

    low = picked(starts, first_slide) // KEY_UNIT
    high = picked(ends, last_slide)
    tiles = (high - low * KEY_UNIT + KEY_TILE - 1) // KEY_TILE
    low = jnp.minimum(low, (cells - tiles * KEY_TILE) // KEY_UNIT)
    ranges = jnp.stack([low, tiles], axis=1).astype(jnp.int32)
    open_code = jnp.where(mask_all == 1, slide, -1)
    return ranges, slide[None, :], open_code[:, None]


def moved(value, target):
    groups, blocks = lax.axis_size("dp"), lax.axis_size("blk")
    pairs = []
    for g in range(groups):
        for b in range(blocks):
            there = target(g, b)
            if there is not None:
                pairs.append((g * blocks + b, there[0] * blocks + there[1]))
    return lax.ppermute(value, MESH_AXES, pairs)


def at_home(g, b):
    return (g & 1) == b >> (bits_of(lax.axis_size("blk")) - 1)


def head_block(g, b):
    return (b & (lax.axis_size("blk") // 2 - 1)) * 2 + (g & 1)


def worker_of(g, block_of_heads):
    half = lax.axis_size("blk") // 2
    return (g - g % 2) + block_of_heads % 2, (g % 2) * half + block_of_heads // 2


def owner_of(g, b, index):
    return (g - g % 2) + b // (lax.axis_size("blk") // 2), index


def pair_masks():
    return [1 << t for t in range(bits_of(lax.axis_size("blk")) - 1)]


def with_meta(cells, mask, lengths):
    count = lengths.shape[0]
    meta = jnp.concatenate([mask, lengths >> 7, lengths & 127]).astype(cells.dtype)
    meta = jnp.pad(meta, (0, cells.shape[1] - mask.shape[0] - 2 * count))
    return jnp.concatenate([cells, jnp.pad(meta[None], ((0, 7), (0, 0)))], axis=0)


def from_meta(meta, rows, count):
    meta = meta.astype(jnp.int32)
    high = meta[0, rows : rows + count]
    return meta[:, :rows].reshape(-1), high * 128 + meta[0, rows + count : rows + 2 * count]


def from_home(value):
    return moved(value, lambda g, b: (g ^ 1, b) if at_home(g, b) else None)


def paired(value, mask):
    return moved(value, lambda g, b: (g, b ^ mask) if at_home(g, b) else None)


def group_rows(own, use):
    blocks = lax.axis_size("blk")
    block = lax.axis_index("blk")
    mirror = moved(own, lambda g, b: None if at_home(g, b) else (g, blocks - 1 - b))
    held, rows = None, []
    for mirrored in (False, True):
        pieces = [(mirror if mirrored else own, 0)]
        for mask in pair_masks():
            pieces += [(paired(piece, mask), place ^ mask) for piece, place in pieces]
        pieces = [
            (piece, from_home(tied(piece, held) if mirrored else piece), blocks - 1 - (block ^ place) if mirrored else block ^ place)
            for piece, place in pieces
        ]
        held = use(pieces, held)
        rows += pieces
    return held, rows


def entry_kernel(count, place_ref, *refs):
    pieces, refs = refs[: 2 * count], refs[2 * count :]
    gain_ref, shift_ref = refs[:2]
    weights = refs[2:5]
    normed_ref, *out_refs = refs[-4:]
    step, home = pl.program_id(0), place_ref[count]
    rows = normed_ref.shape[0]
    for k in range(count):

        @pl.when(step == k)
        def _(k=k):
            value = jnp.where(home == 1, pieces[2 * k][:rows], pieces[2 * k + 1][:rows])
            unit, _ = norm_parts(value.astype(jnp.float32))
            normed_ref[...] = (unit * gain_ref[...] + shift_ref[...]).astype(jnp.bfloat16)

    for weight_ref, out_ref in zip(weights, out_refs):
        out_ref[...] = nn_dot(normed_ref[...], weight_ref[...]).astype(jnp.bfloat16)


def head_columns(weight):
    width = weight.shape[1] // lax.axis_size("blk")
    if width % 128 == 0:
        return weight, pl.BlockSpec((weight.shape[0], width), lambda i, place: (0, place[place.shape[0] - 1]))
    mine = head_block(lax.axis_index("dp"), lax.axis_index("blk")) * width
    return lax.dynamic_slice_in_dim(weight, mine, width, 1), resident((weight.shape[0], width))


def entry(pieces, gain, shift, weights, held):
    blocks, count = lax.axis_size("blk"), len(pieces)
    group, block = lax.axis_index("dp"), lax.axis_index("blk")
    rows, model = pieces[0][0].shape[0] - 8, pieces[0][0].shape[1]
    width = model // blocks
    home = at_home(group, block).astype(jnp.int32)
    table = jnp.stack([place for _, _, place in pieces] + [home, head_block(group, block)])
    narrow = pl.BlockSpec((rows, width), lambda i, place: (place[i], 0))
    shapes = [jax.ShapeDtypeStruct((blocks * rows, cols), jnp.bfloat16) for cols in (model,) + (width,) * 3]
    operands = [value for mine, other, _ in pieces for value in (mine, other)]
    specs = [resident(value.shape) for value in operands] + [resident((1, model))] * 2
    operands += [gain[None], shift[None]]
    for weight in weights:
        weight, spec = head_columns(weight)
        operands.append(weight)
        specs.append(spec)
    aliases = {}
    if held is not None:
        aliases = {1 + len(operands) + i: i for i in range(4)}
        operands += list(held)
        specs += [pl.BlockSpec(memory_space=pl.ANY)] * 4
    return pl.pallas_call(
        partial(entry_kernel, count),
        grid_spec=pltpu.PrefetchScalarGridSpec(
            num_scalar_prefetch=1,
            grid=(count,),
            in_specs=specs,
            out_specs=[pl.BlockSpec((rows, model), lambda i, place: (place[i], 0)), narrow, narrow, narrow],
        ),
        out_shape=shapes,
        input_output_aliases=aliases,
        cost_estimate=nothing(),
        name="entry",
    )(table, *operands)


def project_back_kernel(place_ref, normed_ref, dq_ref, dk_ref, dv_ref, wq_ref, wk_ref, wv_ref,
                        rows_ref, grad_ref, gain_ref, shift_ref, acc_ref, sum_ref):
    step = pl.program_id(0)
    width = dq_ref.shape[1]

    @pl.when(step == 0)
    def _():
        acc_ref[...] = jnp.zeros(acc_ref.shape, jnp.float32)
        sum_ref[...] = jnp.zeros(sum_ref.shape, jnp.float32)

    total = jnp.zeros(rows_ref.shape, jnp.float32)
    for kind, (grad, weight_ref) in enumerate(((dq_ref, wq_ref), (dk_ref, wk_ref), (dv_ref, wv_ref))):
        cols = slice(kind * width, (kind + 1) * width)
        total += nt_dot(grad[...], weight_ref[...])
        acc_ref[:, cols] += tn_dot(normed_ref[...], grad[...])
        sum_ref[:1, cols] += jnp.sum(grad[...].astype(jnp.float32), axis=0, keepdims=True)
    rows_ref[...] = total.astype(jnp.bfloat16)

    @pl.when(step == pl.num_programs(0) - 1)
    def _():
        grad_ref[...] = acc_ref[...].astype(jnp.bfloat16)
        ones = jnp.ones((8, width), jnp.float32)
        gain = jnp.zeros(gain_ref.shape, jnp.float32)
        shift = jnp.zeros(shift_ref.shape, jnp.float32)
        for kind, weight_ref in enumerate((wq_ref, wk_ref, wv_ref)):
            cols = slice(kind * width, (kind + 1) * width)
            weight = weight_ref[...].astype(jnp.float32)
            gain += exact_nt_dot(ones, weight * acc_ref[:, cols])
            shift += exact_nt_dot(sum_ref[:, cols], weight)
        gain_ref[...] = gain
        shift_ref[...] = shift


def exact_nt_dot(left, right):
    return lax.dot_general(
        left,
        right,
        (((1,), (1,)), ((), ())),
        precision=lax.Precision.HIGHEST,
        preferred_element_type=jnp.float32,
    )


def project_back(normed, grads, weights):
    cells, width = grads[0].shape
    model = weights[0].shape[0]
    columns = [head_columns(weight) for weight in weights]
    table = head_block(lax.axis_index("dp"), lax.axis_index("blk"))[None]
    wide = pl.BlockSpec((ROW_TILE, model), lambda i, place: (i, 0))
    return pl.pallas_call(
        project_back_kernel,
        grid_spec=pltpu.PrefetchScalarGridSpec(
            num_scalar_prefetch=1,
            grid=(cells // ROW_TILE,),
            in_specs=[wide]
            + [pl.BlockSpec((ROW_TILE, width), lambda i, place: (i, 0))] * 3
            + [spec for _, spec in columns],
            out_specs=[wide, resident((model, 3 * width)), resident((8, model)), resident((8, model))],
            scratch_shapes=[pltpu.VMEM((model, 3 * width), jnp.float32), pltpu.VMEM((8, 3 * width), jnp.float32)],
        ),
        out_shape=[
            jax.ShapeDtypeStruct((cells, model), jnp.bfloat16),
            jax.ShapeDtypeStruct((model, 3 * width), jnp.bfloat16),
            jax.ShapeDtypeStruct((8, model), jnp.float32),
            jax.ShapeDtypeStruct((8, model), jnp.float32),
        ],
        cost_estimate=nothing(),
        name="project_back",
    )(table, normed, *grads, *[weight for weight, _ in columns])


def heads_at_owner():
    blocks, block = lax.axis_size("blk"), lax.axis_index("blk")
    return jnp.stack([(block - k) & (blocks - 1) for k in range(blocks)])


def rows_at_worker():
    blocks = lax.axis_size("blk")
    mine = head_block(lax.axis_index("dp"), lax.axis_index("blk"))
    return jnp.stack([(mine + k) & (blocks - 1) for k in range(blocks)])


def rows_to_owners(context):
    blocks = lax.axis_size("blk")
    places = rows_at_worker()
    rows = context.shape[0] // blocks
    return [
        moved(
            chunk(context, places[k] * rows, rows, 0),
            lambda g, b: owner_of(g, b, (head_block(g, b) + k) % blocks),
        )
        for k in range(blocks)
    ]


def heads_to_workers(pieces):
    blocks = lax.axis_size("blk")
    return [
        moved(piece, lambda g, b: worker_of(g, (b - k) % blocks)) for k, piece in enumerate(pieces)
    ]


def row_steps(partial_rows):
    blocks = lax.axis_size("blk")
    group, block = lax.axis_index("dp"), lax.axis_index("blk")
    rows = partial_rows.shape[0] // blocks
    home = at_home(group, block)
    (other,) = yield [partial_rows], lambda value: moved(
        value, lambda g, b: None if at_home(g, b) else (g ^ 1, b)
    )

    def taken(place):
        return [chunk(part, place * rows, rows, 0)[None] for part in (partial_rows, other)]

    mine = {r: (taken(block ^ r), taken(blocks - 1 - (block ^ r))) for r in range(blocks // 2)}
    for mask in reversed(pair_masks()):
        send = jnp.concatenate([summed(part) for r in range(mask) for part in mine[r + mask]], axis=0)
        (came,) = yield [send], lambda value, mask=mask: moved(
            value, lambda g, b: (g, b ^ mask) if at_home(g, b) else None
        )
        mine = {
            r: tuple(mine[r][k] + [came[2 * r + k : 2 * r + k + 1]] for k in range(2))
            for r in range(mask)
        }
    own, mirror = mine[0]
    (far,) = yield [summed(mirror)], lambda value: moved(
        value, lambda g, b: (g, blocks - 1 - b) if at_home(g, b) else None
    )
    return jnp.where(home, summed(own), far)[0]


def norm_parts(values):
    center = values - jnp.mean(values, axis=-1, keepdims=True)
    spread = jnp.mean(center * center, axis=-1, keepdims=True)
    scale = lax.rsqrt(spread + ln_eps)
    return center * scale, scale


def nothing():
    return pl.CostEstimate(flops=0, bytes_accessed=0, transcendentals=0)


def resident(shape):
    return pl.BlockSpec(shape, lambda *_: (0,) * len(shape))


def feed_kernel(head_ref, *refs):
    pieces = head_ref.shape[0]
    context_refs, (cell_ref, weight_ref), refs = refs[:pieces], refs[pieces : pieces + 2], refs[pieces + 2 :]
    context_ref, hidden_ref, refs = refs[6], refs[7], refs[:6] + refs[8:]

    @pl.when(pl.program_id(0) == 0)
    def _():
        width = weight_ref.shape[0] // pieces
        total = cell_ref[...].astype(jnp.float32)
        for k in range(pieces):
            begin = head_ref[k] * width
            piece = context_refs[k][...]
            total += nn_dot(piece, weight_ref[pl.ds(pl.multiple_of(begin, width), width), :])
            if width % 128 == 0:
                context_ref[:, pl.ds(pl.multiple_of(begin, width), width)] = piece
        hidden_ref[...] = total

    feed_body(hidden_ref, *refs)


def feed_body(hidden_ref, gain_ref, shift_ref, up_ref, up_bias_ref, down_ref, down_bias_ref,
                normed_ref, active_ref, slope_ref, two_ref, two_b_ref, acc_ref):
    step = pl.program_id(0)

    @pl.when(step == 0)
    def _():
        unit, _ = norm_parts(hidden_ref[...])
        normed_ref[...] = (unit * gain_ref[...] + shift_ref[...]).astype(jnp.bfloat16)
        acc_ref[...] = hidden_ref[...] + down_bias_ref[...]

    inner = nn_dot(normed_ref[...], up_ref[...]) + up_bias_ref[...]
    chance = 0.5 + 0.5 * lax.erf(inner * 2.0**-0.5)
    active = (inner * chance).astype(jnp.bfloat16)
    active_ref[...] = active
    slope = chance + inner * jnp.exp(-0.5 * inner * inner) * (2.0 * math.pi) ** -0.5
    slope_ref[...] = slope.astype(jnp.bfloat16)
    acc_ref[...] += nn_dot(active, down_ref[...])

    @pl.when(step == pl.num_programs(0) - 1)
    def _():
        two_ref[...] = acc_ref[...]
        two_b_ref[...] = acc_ref[...].astype(jnp.bfloat16)


def feed_forward(heads, contexts, cells, out_weight, gain, shift, up_weight, up_bias, down_weight, down_bias):
    rows, model = cells.shape
    inner = up_weight.shape[1]
    tile = FEED_TILE
    across = pl.BlockSpec((rows, tile), lambda j, heads: (0, j))
    return pl.pallas_call(
        feed_kernel,
        grid_spec=pltpu.PrefetchScalarGridSpec(
            num_scalar_prefetch=1,
            grid=(inner // tile,),
            in_specs=[resident(part.shape) for part in contexts]
            + [
                resident((rows, model)),
                resident((model, model)),
                resident((1, model)),
                resident((1, model)),
                pl.BlockSpec((model, tile), lambda j, heads: (0, j)),
                pl.BlockSpec((1, tile), lambda j, heads: (0, j)),
                pl.BlockSpec((tile, model), lambda j, heads: (j, 0)),
                resident((1, model)),
            ],
            out_specs=[
                resident((rows, model)),
                resident((rows, model)),
                resident((rows, model)),
                across,
                across,
                resident((rows, model)),
                resident((rows, model)),
            ],
            scratch_shapes=[pltpu.VMEM((rows, model), jnp.float32)],
        ),
        out_shape=[
            jax.ShapeDtypeStruct((rows, model), jnp.bfloat16),
            jax.ShapeDtypeStruct((rows, model), jnp.float32),
            jax.ShapeDtypeStruct((rows, model), jnp.bfloat16),
            jax.ShapeDtypeStruct((rows, inner), jnp.bfloat16),
            jax.ShapeDtypeStruct((rows, inner), jnp.bfloat16),
            jax.ShapeDtypeStruct((rows, model), jnp.float32),
            jax.ShapeDtypeStruct((rows, model), jnp.bfloat16),
        ],
        cost_estimate=nothing(),
        name="feed_forward",
    )(
        heads, *contexts, cells, out_weight, gain[None], shift[None], up_weight, up_bias[None], down_weight,
        down_bias[None],
    )


def feed_back_kernel(head_ref, two_ref, branch_ref, slope_ref, down_ref, up_ref, hidden_ref, gain_ref, weight_ref,
                     inner_ref, bias_ref, hidden_grad_ref, hidden_grad_b_ref, gain_grad_ref, shift_grad_ref,
                     *rest):
    piece_refs, acc_ref = rest[:-1], rest[-1]
    step = pl.program_id(0)

    @pl.when(step == 0)
    def _():
        acc_ref[...] = jnp.zeros(acc_ref.shape, jnp.float32)

    inner = (nt_dot(branch_ref[...], down_ref[...]) * slope_ref[...].astype(jnp.float32)).astype(jnp.bfloat16)
    inner_ref[...] = inner
    bias_ref[...] = jnp.sum(inner.astype(jnp.float32), axis=0, keepdims=True)
    acc_ref[...] += nt_dot(inner, up_ref[...])

    @pl.when(step == pl.num_programs(0) - 1)
    def _():
        unit, scale = norm_parts(hidden_ref[...])
        grad = acc_ref[...]
        gain_grad_ref[...] = jnp.sum(grad * unit, axis=0, keepdims=True)
        shift_grad_ref[...] = jnp.sum(grad, axis=0, keepdims=True)
        grad = grad * gain_ref[...]
        mean = jnp.mean(grad, axis=-1, keepdims=True)
        slant = jnp.mean(grad * unit, axis=-1, keepdims=True)
        total = two_ref[...] + scale * (grad - mean - unit * slant)
        hidden_grad_ref[...] = total
        total = total.astype(jnp.bfloat16)
        hidden_grad_b_ref[...] = total
        for k, piece_ref in enumerate(piece_refs):
            width = piece_ref.shape[1]
            begin = pl.multiple_of(head_ref[k] * width, width)
            piece_ref[...] = nt_dot(total, weight_ref[pl.ds(begin, width), :]).astype(jnp.bfloat16)


def feed_back(heads, grad_two, grad_branch, slope, down_weight, up_weight, hidden, gain, out_weight):
    rows, model = hidden.shape
    inner = up_weight.shape[1]
    tile = FEED_TILE
    count = heads.shape[0]
    return pl.pallas_call(
        feed_back_kernel,
        grid_spec=pltpu.PrefetchScalarGridSpec(
            num_scalar_prefetch=1,
            grid=(inner // tile,),
            in_specs=[
                resident((rows, model)),
                resident((rows, model)),
                pl.BlockSpec((rows, tile), lambda j, heads: (0, j)),
                pl.BlockSpec((tile, model), lambda j, heads: (j, 0)),
                pl.BlockSpec((model, tile), lambda j, heads: (0, j)),
                resident((rows, model)),
                resident((1, model)),
                resident((model, model)),
            ],
            out_specs=[
                pl.BlockSpec((rows, tile), lambda j, heads: (0, j)),
                pl.BlockSpec((1, tile), lambda j, heads: (0, j)),
                resident((rows, model)),
                resident((rows, model)),
                resident((1, model)),
                resident((1, model)),
            ]
            + [resident((rows, model // count))] * count,
            scratch_shapes=[pltpu.VMEM((rows, model), jnp.float32)],
        ),
        out_shape=[
            jax.ShapeDtypeStruct((rows, inner), jnp.bfloat16),
            jax.ShapeDtypeStruct((1, inner), jnp.float32),
            jax.ShapeDtypeStruct((rows, model), jnp.float32),
            jax.ShapeDtypeStruct((rows, model), jnp.bfloat16),
            jax.ShapeDtypeStruct((1, model), jnp.float32),
            jax.ShapeDtypeStruct((1, model), jnp.float32),
        ]
        + [jax.ShapeDtypeStruct((rows, model // count), jnp.bfloat16)] * count,
        cost_estimate=nothing(),
        name="feed_back",
    )(heads, grad_two, grad_branch, slope, down_weight, up_weight, hidden, gain[None], out_weight)


def tn_dot(left, right):
    return lax.dot_general(left, right, (((0,), (0,)), ((), ())), preferred_element_type=jnp.float32)


def weights_kernel(lefts_at, ready, place_ref, column_ref, *refs):
    count = len(lefts_at)
    scratch = 0 if ready else count
    lefts = refs[: max(lefts_at) + 1]
    rights = refs[len(lefts) : len(lefts) + count]
    refs, ordered = refs[len(lefts) + count : len(refs) - scratch], refs[len(refs) - scratch :]
    vector_ref, (keep_ref, send_ref) = refs[:-2], refs[-2:]
    held, grouped, _, width = keep_ref.shape
    if ready:
        ordered = rights
    else:

        @pl.when(pl.program_id(0) == 0)
        def _():
            for right_ref, ordered_ref in zip(rights, ordered):
                for piece in range(2 * held):
                    begin = pl.multiple_of(column_ref[piece] * width, width)
                    ordered_ref[:, piece * width : (piece + 1) * width] = right_ref[:, pl.ds(begin, width)]

    begin = 0
    for at, ordered_ref in zip(lefts_at, ordered):
        total = lefts[at].shape[1]
        tile = min(total, 256)
        rows = min(tile, total // grouped)
        for first in range(0, total, tile):
            value = tn_dot(lefts[at][:, first : first + tile], ordered_ref[...]).astype(jnp.bfloat16)
            for inside in range(0, tile, rows):
                z, row = divmod(first + inside, total // grouped)
                part = value[inside : inside + rows]
                place = slice(begin + row, begin + row + rows)
                for piece in range(held):
                    keep_ref[piece, z, place, :] = part[:, piece * width : (piece + 1) * width]
                    other = held + piece
                    send_ref[piece, z, place, :] = part[:, other * width : (other + 1) * width]
        begin += total // grouped

    if vector_ref:
        keep_ref[:, :, begin:, :] = vector_ref[0][0]
        send_ref[:, :, begin:, :] = vector_ref[0][1]


def relative_columns(value, steps):
    group = lax.axis_index("dp")
    masks = relative_masks(steps)
    size = value.shape[1] // len(masks)
    return jnp.concatenate([chunk(value, (group ^ mask) * size, size, 1) for mask in masks], axis=1)


def weight_pieces(pairs, steps, vector=None):
    blocks, block = lax.axis_size("blk"), lax.axis_index("blk")
    pieces, group = lax.axis_size("dp"), lax.axis_index("dp")
    width = D // pieces
    masks = relative_masks(blk_masks())
    sizes = [left.shape[1] // blocks for left, _, _ in pairs]
    places = jnp.stack([block ^ mask for mask in masks])
    columns = jnp.stack([group ^ mask for mask in relative_masks(steps)])
    cells = pairs[0][1].shape[0]
    lefts, lefts_at = [], []
    for left, _, _ in pairs:
        if not any(left is seen for seen in lefts):
            lefts.append(left)
        lefts_at.append(next(i for i, seen in enumerate(lefts) if left is seen))
    rights = [right for _, right, _ in pairs]
    parts = [part for _, _, part in pairs]
    grouped = max(1, 128 // min(sizes))
    ready = grouped > 1 or width % 128 != 0
    if ready:
        rights = [
            relative_columns(right[:, part * D : (part + 1) * D], steps) for right, part in zip(rights, parts)
        ]
        parts = [0] * len(parts)
        lefts = [
            jnp.concatenate(
                [chunk(left, (block ^ mask) * (left.shape[1] // blocks), left.shape[1] // blocks, 1) for mask in masks],
                axis=1,
            )
            for left in lefts
        ]
        places = jnp.arange(blocks, dtype=jnp.int32)
    rows = sum(sizes) + (0 if vector is None else vector.shape[3])
    out = pl.BlockSpec((pieces // 2, grouped, rows, width), lambda z, place, column: (0, z, 0, 0))
    specs = [
        pl.BlockSpec((cells, left.shape[1] // blocks * grouped), lambda z, place, column: (0, place[z]))
        for left in lefts
    ]
    specs += [pl.BlockSpec((cells, D), lambda z, place, column, part=part: (0, part)) for part in parts]
    operands = lefts + rights
    if vector is not None:
        specs.append(
            pl.BlockSpec(
                (2, pieces // 2, grouped, vector.shape[3], width), lambda z, place, column: (0, 0, z, 0, 0)
            )
        )
        operands.append(vector)
    shape = jax.ShapeDtypeStruct((pieces // 2, blocks, rows, width), jnp.bfloat16)
    return pl.pallas_call(
        partial(weights_kernel, lefts_at, ready),
        grid_spec=pltpu.PrefetchScalarGridSpec(
            num_scalar_prefetch=2,
            grid=(blocks // grouped,),
            in_specs=specs,
            out_specs=[out, out],
            scratch_shapes=[pltpu.VMEM((cells, D), jnp.bfloat16) for _ in pairs if not ready],
        ),
        out_shape=[shape, shape],
        cost_estimate=nothing(),
        name="weight_pieces",
    )(places, columns, *operands)


def weight_steps(keep, send, flipped, parts):
    steps = dp_order(flipped)
    (came,) = yield [send], by_mask(steps[0], 0)
    size = keep.shape[0]
    terms = [[keep[place], came[place]] for place in range(size)]
    for mask in steps[1:]:
        size = size // 2
        came = yield [summed(terms[place]) for place in range(size, 2 * size)], by_mask(mask, 0)
        terms = [terms[place] + [came[place]] for place in range(size)]
    terms = terms[0]
    size = keep.shape[1]
    for mask in blk_masks():
        size = size // 2
        (came,) = yield [summed([term[size : 2 * size] for term in terms])], by_mask(0, mask)
        terms = [term[:size] for term in terms] + [came]
    value = summed(terms)
    for mask in steps[:0:-1]:
        (came,) = yield [value], by_mask(mask, 0)
        value = jnp.concatenate([value, came], axis=0)
    (came,) = yield [value], by_mask(steps[0], 0)
    return spread_columns(value, came, relative_table(steps, lax.axis_index("dp")), parts)


def local(
    cell_states,
    slide_lengths,
    cell_mask,
    latent_noise,
    train_step,
    attn_gain,
    attn_shift,
    query_weight,
    key_weight,
    value_weight,
    out_weight,
    ffn_gain,
    ffn_shift,
    up_weight,
    up_bias,
    down_weight,
    down_bias,
    encode_weight,
    encode_bias,
    decode_weight,
    prior_means,
    prior_logits,
    out_grad,
):
    rows_here = cell_states.shape[0]
    blocks = lax.axis_size("blk")
    group, block = lax.axis_index("dp"), lax.axis_index("blk")
    width = D // blocks
    x_float = cell_states.astype(jnp.float32)
    _, norm_back = jax.vjp(layer_norm, x_float, attn_gain, attn_shift)
    weights = (query_weight, key_weight, value_weight)
    held, pieces = group_rows(
        with_meta(cell_states, cell_mask, slide_lengths[0]),
        lambda pieces, held: entry(pieces, attn_gain, attn_shift, weights, held),
    )
    normed_b, queries, keys, values = held
    meta = jnp.zeros((blocks, D), jnp.bfloat16)
    order = jnp.arange(blocks, dtype=jnp.int32)
    for mine, other, place in pieces:
        row = jnp.where(at_home(group, block), mine[rows_here], other[rows_here])
        meta = jnp.where(order[:, None] == place, row[None], meta)
    mask_all, lengths_row = from_meta(meta, rows_here, slide_lengths.shape[1])
    ranges, query_code, key_code = slide_tables(lengths_row, mask_all)
    context_here, log_total = attention_forward(ranges, queries, keys, values, query_code, key_code)
    contexts = rows_to_owners(context_here)
    owner_heads = heads_at_owner()
    context_b, hidden, normed_two_b, activated_b, slope_b, hidden_two, hidden_two_b = feed_forward(
        owner_heads, contexts, cell_states, out_weight, ffn_gain, ffn_shift, up_weight, up_bias, down_weight,
        down_bias,
    )
    if width % 128:
        context_b = jnp.zeros((rows_here, D), jnp.bfloat16)
        for k in range(blocks):
            context_b = lax.dynamic_update_slice_in_dim(context_b, contexts[k], owner_heads[k] * width, 1)
    encoded = plain_dot(hidden_two_b, encode_weight) + encode_bias
    latent_mean = encoded[:, :LAT]
    latent_logvar = encoded[:, LAT:]
    spread = jnp.exp(0.5 * latent_logvar)
    noise_float = latent_noise.astype(jnp.float32)
    latent_b = (latent_mean + spread * noise_float).astype(jnp.bfloat16)
    output = hidden_two + plain_dot(latent_b, decode_weight)
    (kl_dim, categorical), kl_back = jax.vjp(
        kl_terms, latent_mean, latent_logvar, prior_means, prior_logits
    )
    real = cell_mask.astype(jnp.float32)
    sums = jnp.concatenate(
        [
            jnp.sum(kl_dim * real[:, None], axis=0),
            jnp.sum(categorical * real)[None],
            jnp.sum(real)[None],
            jnp.zeros((126,), jnp.float32),
        ]
    )
    sums = summed_everywhere(sums)
    kl_sum, cat_sum, count = sums[:LAT], sums[LAT], sums[LAT + 1]
    kbar = kl_sum / count
    floored = jnp.sum(jnp.maximum(kbar, free_floor))
    cat_mean = cat_sum / count
    beta = jnp.minimum(1.0, (train_step[0].astype(jnp.float32) + 1.0) / WARM)
    active = (kbar > free_floor).astype(jnp.float32)
    grad_latent = cols_dot(out_grad, decode_weight)
    grad_mean, grad_logvar, grad_means, grad_prior = kl_back(
        (beta * real[:, None] * active[None, :], beta * real)
    )
    grad_mean = grad_mean + grad_latent
    grad_logvar = grad_logvar + grad_latent * 0.5 * spread * noise_float
    grad_encoded_b = jnp.concatenate([grad_mean, grad_logvar], axis=1).astype(jnp.bfloat16)
    grad_encode_bias = jnp.sum(grad_encoded_b.astype(jnp.float32), axis=0)
    grad_two = out_grad.astype(jnp.float32) + cols_dot(grad_encoded_b, encode_weight)
    grad_down_bias = jnp.sum(grad_two, axis=0)
    grad_branch_b = grad_two.astype(jnp.bfloat16)

    straight, flipped = dp_order(False), dp_order(True)
    block_rows = D // blocks
    down = Exchange(
        weight_steps(
            *weight_pieces(
                [(activated_b, grad_branch_b, 0), (hidden_two_b, grad_encoded_b, 0), (latent_b, out_grad, 0)],
                straight,
            ),
            False,
            [(4 * block_rows, 1), (block_rows, 1), (block_rows // 2, 1)],
        )
    )
    back = feed_back(
        owner_heads, grad_two, tied(grad_branch_b, down.last), slope_b, down_weight, up_weight, hidden, ffn_gain,
        out_weight,
    )
    grad_inner_b, grad_up_bias, grad_hidden, grad_attn_b, grad_ffn_gain, grad_ffn_shift = back[:6]
    grads_here = heads_to_workers(back[6:])
    by_block = lambda part: part.reshape(blocks, -1)
    means_block = jnp.moveaxis(grad_means.reshape(K, blocks, LAT // blocks), 1, 0)
    vectors = [
        by_block(grad_ffn_gain),
        by_block(grad_ffn_shift),
        by_block(grad_up_bias),
        by_block(grad_down_bias),
        by_block(grad_encode_bias),
        by_block(means_block),
        by_block(grad_prior),
    ]
    sizes = [part.shape[1] for part in vectors]
    vector = jnp.concatenate([part.astype(jnp.bfloat16) for part in vectors], axis=1)
    vector_rows = -(-sum(sizes) // (8 * D)) * 8
    vector = jnp.pad(vector, ((0, 0), (0, vector_rows * D - sum(sizes))))
    vector = relative_columns(vector.reshape(blocks * vector_rows, D), flipped)
    devices_along = lax.axis_size("dp")
    vector = vector.reshape(blocks, vector_rows, 2, devices_along // 2, D // devices_along)
    vector = jnp.transpose(vector, (2, 3, 0, 1, 4))
    vector = jnp.concatenate([chunk(vector, block ^ mask, 1, 2) for mask in relative_masks(blk_masks())], axis=2)
    up_pieces = weight_pieces(
        [(normed_two_b, tied(grad_inner_b, back[6:]), part) for part in range(4)] + [(context_b, grad_attn_b, 0)],
        flipped,
        vector,
    )
    up = Exchange(
        weight_steps(
            *tied(up_pieces, grads_here), True, [(block_rows, 4), (block_rows, 1), (vector_rows, 1)]
        )
    )
    token = down.advance(up.last, hold=True)
    token = up.advance(token, hold=True)
    grads = attention_backward(
        ranges, rows_at_worker(), tied(queries, token), grads_here, context_here, log_total, keys, values, query_code,
        key_code,
    )
    grads = tied(grads, (down.flight, up.flight))
    down.release(grads[0])
    up.release(grads[0])
    partial_rows, grad_heads, part_gain, part_shift = project_back(normed_b, grads, weights)
    partial_rows, grad_heads = tied((partial_rows, grad_heads), (down.flight, up.flight))
    row_sum = Exchange(row_steps(partial_rows))
    part_shift = part_shift[0]
    part_gain = (part_gain[0] - attn_shift * part_shift) / attn_gain
    token = up.advance(grad_heads)
    token = down.advance(token)
    extra = jnp.concatenate([by_block(part_gain), by_block(part_shift)], axis=1)
    extra_size = extra.shape[1]
    extra = jnp.pad(extra, ((0, 0), (0, 3 * width - extra_size))).astype(jnp.bfloat16)
    pieces = lax.axis_size("dp") // 2
    piece_rows = block_rows // pieces
    grad_heads = grad_heads.reshape(blocks, pieces, piece_rows, 3 * width)
    extra = jnp.broadcast_to(extra[:, None, None, :], (blocks, pieces, 8, 3 * width))
    attn = Exchange(head_steps(jnp.concatenate([grad_heads, extra], axis=2)))
    token = attn.last
    order = [row_sum, attn, down, row_sum, up, attn]
    live = [down, row_sum, up, attn]
    for bundle in order:
        token = bundle.advance(token)
    while any(bundle.result is None for bundle in live):
        for bundle in live:
            if bundle.result is None:
                token = bundle.advance(token)
    grad_normed = row_sum.result.astype(jnp.float32)
    grad_from_norm, _, _ = norm_back(grad_normed)
    states_grad = grad_hidden + grad_from_norm
    mine, other = attn.result
    attn_vector = jnp.sum((mine[0].astype(jnp.float32) + other[0].astype(jnp.float32)), axis=0)[piece_rows]
    main = spread_heads(mine, other, piece_rows)
    down_sum, encode_sum, decode_sum = down.result
    up_sum, out_sum, vector_sum = up.result
    flat = vector_sum.reshape(-1)
    small, begin = [], 0
    for size in sizes:
        small.append(flat[begin : begin + size])
        begin += size
    totals = (
        attn_vector[: extra_size // 2],
        attn_vector[extra_size // 2 : extra_size],
        main[0],
        main[1],
        main[2],
        out_sum,
        small[0],
        small[1],
        up_sum,
        small[2],
        down_sum,
        small[3],
        encode_sum,
        small[4],
        decode_sum,
        small[5].reshape(K, LAT // blocks),
        small[6],
    )
    kl_out = (floored / LAT + cat_mean).reshape(1)
    return (output.astype(jnp.bfloat16), states_grad, kl_out) + tuple(totals)


def solution(mesh):
    in_specs = (
        P(("dp", "blk"), None),
        P("dp", None),
        P(("dp", "blk")),
        P(("dp", "blk"), None),
        P(),
        P(),
        P(),
        P(),
        P(),
        P(),
        P(),
        P(),
        P(),
        P(),
        P(),
        P(),
        P(),
        P(),
        P(),
        P(),
        P(),
        P(),
        P(("dp", "blk"), None),
    )
    out_specs = (
        P(("dp", "blk"), None),
        P(("dp", "blk"), None),
        P(),
        P("blk"),
        P("blk"),
        P("blk", None),
        P("blk", None),
        P("blk", None),
        P("blk", None),
        P("blk"),
        P("blk"),
        P("blk", None),
        P("blk"),
        P("blk", None),
        P("blk"),
        P("blk", None),
        P("blk"),
        P("blk", None),
        P(None, "blk"),
        P("blk"),
    )
    return jax.shard_map(local, mesh=mesh, in_specs=in_specs, out_specs=out_specs, check_vma=False)
```

```python
import math
from functools import partial

import jax
import jax.numpy as jnp
from jax import lax
from jax.experimental import pallas as pl
from jax.experimental.pallas import tpu as pltpu
from jax.sharding import PartitionSpec as P

D = 1024
H = 16
HD = 64
LAT = 512
K = 16
WARM = 2000


ln_eps = 1e-05
free_floor = 1.3
neg_fill = -1e30

QUERY_TILE = 256
KEY_TILE = 384
ROW_TILE = 512
KEY_UNIT = 128
FEED_TILE = 1024


def layer_norm(values, gain, shift):
    center = values - jnp.mean(values, axis=-1, keepdims=True)
    spread = jnp.mean(center * center, axis=-1, keepdims=True)
    return center * lax.rsqrt(spread + ln_eps) * gain + shift


def slide_index(position, lengths_row):
    ends = jnp.cumsum(lengths_row)
    return jnp.sum((position[:, None] >= ends[None, :]).astype(jnp.int32), axis=1)


def exact_dot(left, right):
    return jnp.dot(left, right, precision=lax.Precision.HIGHEST, preferred_element_type=jnp.float32)


def kl_terms(latent_mean, latent_logvar, prior_means, prior_logits):
    log_prior = jax.nn.log_softmax(prior_logits)
    logits = exact_dot(latent_mean, prior_means.T) * LAT ** (-0.5) + log_prior[None, :]
    resp = jax.nn.softmax(logits, axis=-1)
    log_resp = jax.nn.log_softmax(logits, axis=-1)
    mixed_mean = exact_dot(resp, prior_means)
    mixed_square = exact_dot(resp, prior_means * prior_means)
    kl_dim = 0.5 * (
        jnp.exp(latent_logvar)
        + latent_mean * latent_mean
        - 2.0 * latent_mean * mixed_mean
        + mixed_square
        - 1.0
        - latent_logvar
    )
    categorical = jnp.sum(resp * (log_resp - log_prior[None, :]), axis=-1)
    return (kl_dim, categorical)


def plain_dot(left, right):
    return jnp.dot(left, right, preferred_element_type=jnp.float32)


def rows_dot(left, right):
    return lax.dot_general(
        left, right, (((0,), (0,)), ((), ())), preferred_element_type=jnp.float32
    )


def cols_dot(left, right):
    return lax.dot_general(
        left, right, (((1,), (1,)), ((), ())), preferred_element_type=jnp.float32
    )


MESH_AXES = ("dp", "blk")


def swapped(value, dp_mask, blk_mask):
    groups, blocks = lax.axis_size("dp"), lax.axis_size("blk")
    pairs = [
        (g * blocks + b, (g ^ dp_mask) * blocks + (b ^ blk_mask))
        for g in range(groups)
        for b in range(blocks)
    ]
    return lax.ppermute(value, MESH_AXES, pairs)


def bits_of(count):
    return count.bit_length() - 1


def dp_masks():
    return [1 << t for t in range(bits_of(lax.axis_size("dp")))]


def blk_masks():
    return [(2 << t) - 1 for t in range(bits_of(lax.axis_size("blk")))]


def tree_sum(value, masks):
    places = [(0, 0)]
    for dp_mask, blk_mask in masks:
        places = places + [(dp ^ dp_mask, blk ^ blk_mask) for dp, blk in places]
    terms = [value] + [swapped(value, dp, blk) for dp, blk in places[1:]]
    while len(terms) > 1:
        terms = [terms[i] + terms[i + 1] for i in range(0, len(terms), 2)]
    return terms[0]


def summed_everywhere(value):
    value = tree_sum(value, [(1, 0)])
    value = tree_sum(value, [(mask, 0) for mask in dp_masks()[1:]])
    return tree_sum(value, [(0, mask) for mask in blk_masks()])


def added(left, right):
    return (left.astype(jnp.float32) + right.astype(jnp.float32)).astype(jnp.bfloat16)


def summed(terms):
    total = terms[0].astype(jnp.float32)
    for term in terms[1:]:
        total = total + term.astype(jnp.float32)
    return total.astype(jnp.bfloat16)


def chunk(value, start, size, axis):
    return lax.dynamic_slice_in_dim(value, start, size, axis)


def tied(value, other):
    return lax.optimization_barrier((value, other))[0]


class Exchange:
    def __init__(self, steps):
        self.steps = steps
        self.result = None
        self.last = None
        self.flight = None
        self._take(lambda: next(self.steps))

    def _take(self, step, hold=False):
        try:
            values, permute = step()
            first = len(values) // 2 if hold else len(values)
            self.last = values
            self.flight = [permute(value) for value in values[:first]]
            self.held = (values[first:], permute)
        except StopIteration as end:
            self.result = end.value
            self.last = end.value
            self.flight = None

    def advance(self, token, hold=False):
        came = tied(self.flight, token)
        self._take(lambda: self.steps.send(came), hold)
        return self.last

    def release(self, token):
        values, permute = self.held
        self.flight = self.flight + [permute(tied(value, token)) for value in values]


def by_mask(dp_mask, blk_mask):
    return lambda value: swapped(value, dp_mask, blk_mask)


def dp_order(flipped):
    masks = dp_masks()
    return masks[:1] + masks[1:][::-1] if flipped else masks


def relative_masks(steps):
    places = [0]
    for step in steps[::-1]:
        places = places + [place ^ step for place in places]
    return places


def relative_table(steps, mine):
    masks = relative_masks(steps)
    inverse = [masks.index(place) for place in range(len(masks))]
    order = jnp.arange(len(masks), dtype=jnp.int32)
    wanted = order ^ mine
    return sum(jnp.where(wanted == place, inverse[place], 0) for place in range(len(masks)))


def spread_kernel(parts, table_ref, mine_ref, other_ref, *out_refs):
    held, _, width = mine_ref.shape
    cols = 2 * held * width
    for place in range(2 * held):
        index = table_ref[place]
        piece = jnp.where(index < held, mine_ref[index & (held - 1)], other_ref[index & (held - 1)])
        piece = piece.astype(jnp.float32)
        for out_ref, (begin, count, times) in zip(out_refs, parts):
            for time in range(times):
                row, column = begin + time * count, time * cols + place * width
                out_ref[:, column : column + width] = piece[row : row + count]


def spread_columns(mine, other, table, parts):
    held, rows, width = mine.shape
    cols = 2 * held * width
    begin, placed, shapes = 0, [], []
    for count, times in parts:
        placed.append((begin, count, times))
        shapes.append(jax.ShapeDtypeStruct((count, times * cols), jnp.float32))
        begin += count * times
    return pl.pallas_call(
        partial(spread_kernel, placed),
        out_shape=shapes,
        grid_spec=pltpu.PrefetchScalarGridSpec(
            num_scalar_prefetch=1,
            grid=(1,),
            in_specs=[resident((held, rows, width))] * 2,
            out_specs=[resident(shape.shape) for shape in shapes],
        ),
        cost_estimate=nothing(),
        name="spread_columns",
    )(table, mine, other)


def head_steps(value):
    blocks = lax.axis_size("blk")
    group, block = lax.axis_index("dp"), lax.axis_index("blk")
    half = blocks // 2
    steps = dp_masks()[1:]
    masks = relative_masks([step >> 1 for step in steps])
    taken = [[chunk(value, (group >> 1) ^ mask, 1, 1)] for mask in masks]
    size = len(masks)
    for step in steps:
        size = size // 2
        send = jnp.concatenate([summed(taken[place]) for place in range(size, 2 * size)], axis=1)
        (came,) = yield [send], by_mask(step, 0)
        taken = [taken[place] + [came[:, place : place + 1]] for place in range(size)]
    side = block >> (bits_of(blocks) - 1)
    away = [chunk(term, (1 - side) * half, half, 0) for term in taken[0]]
    (came,) = yield [summed(away)], by_mask(0, half)
    terms = [chunk(term, side * half, half, 0) for term in taken[0]] + [came]
    place = block & (half - 1)
    pieces = [summed([chunk(term, place, 1, 0) for term in terms])]
    for k in range(1, half):
        send = summed([chunk(term, place ^ k, 1, 0) for term in terms])
        (came,) = yield [send], by_mask(0, k)
        pieces.append(came)
    value = jnp.concatenate(pieces, axis=1)
    for step in steps[::-1]:
        (came,) = yield [value], by_mask(step, 0)
        value = jnp.concatenate([value, came], axis=0)
    (other,) = yield [value], by_mask(1, 0)
    return value, other


def heads_kernel(table_ref, mine_ref, other_ref, *out_refs):
    pieces = pl.num_programs(0)
    place, core = table_ref[pieces], table_ref[pieces + 1]
    half = mine_ref.shape[1]
    rows = out_refs[0].shape[0]
    width = mine_ref.shape[3] // 3
    for chip in range(half):
        mine = mine_ref[0, chip ^ place].astype(jnp.float32)
        other = other_ref[0, chip ^ place].astype(jnp.float32)
        for c in range(2):
            value = jnp.where(core == c, mine, other)
            column = (2 * chip + c) * width
            for kind in range(3):
                out_refs[kind][:, column : column + width] = value[:rows, kind * width : (kind + 1) * width]


def spread_heads(mine, other, rows):
    blocks = lax.axis_size("blk")
    group, block = lax.axis_index("dp"), lax.axis_index("blk")
    pieces, half, held_rows, width = mine.shape
    table = relative_table([step >> 1 for step in dp_masks()[1:]], group >> 1)
    table = jnp.concatenate([table, jnp.stack([block & (half - 1), group & 1])])
    held = pl.BlockSpec((1, half, held_rows, width), lambda i, table: (table[i], 0, 0, 0))
    cols = 2 * half * width // 3
    return pl.pallas_call(
        heads_kernel,
        out_shape=(jax.ShapeDtypeStruct((pieces * rows, cols), jnp.float32),) * 3,
        grid_spec=pltpu.PrefetchScalarGridSpec(
            num_scalar_prefetch=1,
            grid=(pieces,),
            in_specs=[held, held],
            out_specs=[pl.BlockSpec((rows, cols), lambda i, table: (i, 0))] * 3,
        ),
        cost_estimate=nothing(),
        name="spread_heads",
    )(table, mine, other)


def head_lanes(value, head):
    lane = lax.broadcasted_iota(jnp.int32, value.shape, 1) // HD
    return jnp.where(lane == head, value, jnp.zeros_like(value))

def nt_dot(left, right):
    return lax.dot_general(left, right, (((1,),(1,)),((),())), preferred_element_type=jnp.float32)

def nn_dot(left, right):
    return lax.dot_general(left, right, (((1,),(0,)),((),())), preferred_element_type=jnp.float32)

def allowed_pairs(code_k, code_q, block_k, tile):
    key_pos = block_k + lax.broadcasted_iota(jnp.int32, tile, 0)
    query_pos = pl.program_id(0) * QUERY_TILE + lax.broadcasted_iota(jnp.int32, tile, 1)
    return (code_k == code_q) | (key_pos == query_pos)

def forward_kernel(range_ref, q_ref, k_ref, v_ref, cq_ref, ck_ref, ctx_ref, lse_ref, m_ref, l_ref, acc_ref, vt_ref):
    nh = q_ref.shape[1] // HD
    step = pl.program_id(0)

    @pl.when(step == 0)
    def _():
        vt_ref[...] = v_ref[...].T

    m_ref[...] = jnp.full(m_ref.shape, neg_fill, jnp.float32)
    l_ref[...] = jnp.zeros(l_ref.shape, jnp.float32)
    acc_ref[...] = jnp.zeros(acc_ref.shape, jnp.float32)
    code_q = cq_ref[...]
    scaled = (q_ref[...].astype(jnp.float32) * HD ** (-0.5)).astype(jnp.bfloat16)
    def body(kb, _):
        start = pl.multiple_of(range_ref[step, 0] * KEY_UNIT + kb * KEY_TILE, KEY_UNIT)
        keys = k_ref[pl.ds(start, KEY_TILE), :]
        open_pair = allowed_pairs(ck_ref[pl.ds(start, KEY_TILE), :], code_q, start, (KEY_TILE, QUERY_TILE))
        bias = jnp.where(open_pair, 0.0, neg_fill)
        rows = [slice(h * HD, (h + 1) * HD) for h in range(nh)]
        scores = [nt_dot(keys[:, rows[h]], scaled[:, rows[h]]) + bias for h in range(nh)]
        probs, scales = [], []
        for h in range(nh):
            m_old = m_ref[h : h + 1, :]
            m_new = jnp.maximum(m_old, jnp.max(scores[h], axis=0, keepdims=True))
            p = jnp.exp(scores[h] - m_new)
            alpha = jnp.exp(m_old - m_new)
            l_ref[h : h + 1, :] = l_ref[h : h + 1, :] * alpha + jnp.sum(p, axis=0, keepdims=True)
            m_ref[h : h + 1, :] = m_new
            probs.append(p.astype(jnp.bfloat16))
            scales.append(alpha)
        for h in range(nh):
            part = nn_dot(vt_ref[rows[h], pl.ds(start, KEY_TILE)], probs[h])
            acc_ref[rows[h], :] = acc_ref[rows[h], :] * scales[h] + part
        return 0
    lax.fori_loop(0, range_ref[step, 1], body, 0)
    for h in range(nh):
        rows = slice(h*HD, (h+1)*HD)
        acc_ref[rows, :] = acc_ref[rows, :] / l_ref[h:h+1, :]
    ctx_ref[...] = acc_ref[...].T.astype(jnp.bfloat16)
    lse_ref[...] = m_ref[...] + jnp.log(l_ref[...])

def attention_forward(ranges, q, k, v, code_q, code_k):
    N, W = q.shape
    nh = W // HD
    full = lambda shape: pl.BlockSpec(shape, lambda i, r: (0,)*len(shape))
    return pl.pallas_call(
        forward_kernel,
        out_shape=(jax.ShapeDtypeStruct((N, W), jnp.bfloat16), jax.ShapeDtypeStruct((nh, N), jnp.float32)),
        grid_spec=pltpu.PrefetchScalarGridSpec(
            num_scalar_prefetch=1, grid=(N//QUERY_TILE,),
            in_specs=[pl.BlockSpec((QUERY_TILE, W), lambda i, r: (i, 0)), full((N, W)), full((N, W)),
                      pl.BlockSpec((1, QUERY_TILE), lambda i, r: (0, i)), full((N, 1))],
            out_specs=[pl.BlockSpec((QUERY_TILE, W), lambda i, r: (i, 0)), pl.BlockSpec((nh, QUERY_TILE), lambda i, r: (0, i))],
            scratch_shapes=[pltpu.VMEM((nh, QUERY_TILE), jnp.float32), pltpu.VMEM((nh, QUERY_TILE), jnp.float32), pltpu.VMEM((W, QUERY_TILE), jnp.float32), pltpu.VMEM((W, N), jnp.bfloat16)]),
        cost_estimate=nothing(),
        name="attention_forward",
    )(ranges, q, k, v, code_q, code_k)

def backward_kernel(range_ref, row_ref, q_ref, ctx_ref, lse_ref, k_ref, v_ref, cq_ref, ck_ref,
                    *refs):
    pieces = row_ref.shape[0]
    do_refs, (dq_ref, dk_ref, dv_ref, dqt_ref, dk_acc, dv_acc, kt_ref, do_ref) = refs[:pieces], refs[pieces:]
    nh = q_ref.shape[1] // HD
    step = pl.program_id(0)
    @pl.when(step == 0)
    def _():
        dk_acc[...] = jnp.zeros(dk_acc.shape, jnp.float32)
        dv_acc[...] = jnp.zeros(dv_acc.shape, jnp.float32)
        kt_ref[...] = k_ref[...].T
        for k, piece_ref in enumerate(do_refs):
            rows = piece_ref.shape[0]
            do_ref[pl.ds(pl.multiple_of(row_ref[k] * rows, rows), rows), :] = piece_ref[...]

    dqt_ref[...] = jnp.zeros(dqt_ref.shape, jnp.float32)
    code_q = cq_ref[...]
    scaled = (q_ref[...].astype(jnp.float32) * HD ** (-0.5)).astype(jnp.bfloat16)
    grads = do_ref[pl.ds(pl.multiple_of(step * QUERY_TILE, QUERY_TILE), QUERY_TILE), :]
    product = (grads.astype(jnp.float32) * ctx_ref[...].astype(jnp.float32)).T
    deltas = [jnp.sum(product[h*HD:(h+1)*HD, :], axis=0, keepdims=True) for h in range(nh)]
    q_all = jnp.concatenate([head_lanes(scaled, h) for h in range(nh)], axis=0)
    do_all = jnp.concatenate([head_lanes(grads, h) for h in range(nh)], axis=0)
    def body(kb, _):
        start = pl.multiple_of(range_ref[step, 0] * KEY_UNIT + kb * KEY_TILE, KEY_UNIT)
        keys = k_ref[pl.ds(start, KEY_TILE), :]
        values = v_ref[pl.ds(start, KEY_TILE), :]
        open_pair = allowed_pairs(ck_ref[pl.ds(start, KEY_TILE), :], code_q, start, (KEY_TILE, QUERY_TILE))
        bias = jnp.where(open_pair, 0.0, neg_fill)
        cols = [slice(h * QUERY_TILE, (h + 1) * QUERY_TILE) for h in range(nh)]
        scores = [nt_dot(keys, q_all[cols[h], :]) + bias for h in range(nh)]
        dps = [nt_dot(values, do_all[cols[h], :]) for h in range(nh)]
        ps = [jnp.exp(scores[h] - lse_ref[h : h + 1, :]) for h in range(nh)]
        dss = [(ps[h] * (dps[h] - deltas[h])).astype(jnp.bfloat16) for h in range(nh)]
        ps = [p.astype(jnp.bfloat16) for p in ps]
        for h in range(nh):
            rows = slice(h * HD, (h + 1) * HD)
            dqt_ref[rows, :] += nn_dot(kt_ref[rows, pl.ds(start, KEY_TILE)], dss[h])
        dv_acc[pl.ds(start, KEY_TILE), :] += nn_dot(jnp.concatenate(ps, axis=1), do_all)
        dk_acc[pl.ds(start, KEY_TILE), :] += nn_dot(jnp.concatenate(dss, axis=1), q_all)
        return 0
    lax.fori_loop(0, range_ref[step, 1], body, 0)
    dq_ref[...] = (dqt_ref[...] * HD ** (-0.5)).T.astype(jnp.bfloat16)
    @pl.when(step == pl.num_programs(0) - 1)
    def _():
        dk_ref[...] = dk_acc[...].astype(jnp.bfloat16)
        dv_ref[...] = dv_acc[...].astype(jnp.bfloat16)

def attention_backward(ranges, places, q, pieces, ctx, lse, k, v, code_q, code_k):
    cells, width = q.shape
    heads = width // HD

    def row():
        return pl.BlockSpec((QUERY_TILE, width), lambda i, *_: (i, 0))

    out = jax.ShapeDtypeStruct((cells, width), jnp.bfloat16)
    return pl.pallas_call(
        backward_kernel,
        out_shape=(out, out, out),
        grid_spec=pltpu.PrefetchScalarGridSpec(
            num_scalar_prefetch=2,
            grid=(cells // QUERY_TILE,),
            in_specs=[
                row(),
                row(),
                pl.BlockSpec((heads, QUERY_TILE), lambda i, *_: (0, i)),
                resident((cells, width)),
                resident((cells, width)),
                pl.BlockSpec((1, QUERY_TILE), lambda i, *_: (0, i)),
                resident((cells, 1)),
            ]
            + [resident(piece.shape) for piece in pieces],
            out_specs=[row(), resident((cells, width)), resident((cells, width))],
            scratch_shapes=[
                pltpu.VMEM((width, QUERY_TILE), jnp.float32),
                pltpu.VMEM((cells, width), jnp.float32),
                pltpu.VMEM((cells, width), jnp.float32),
                pltpu.VMEM((width, cells), jnp.bfloat16),
                pltpu.VMEM((cells, width), jnp.bfloat16),
            ],
        ),
        cost_estimate=nothing(),
        name="attention_backward",
    )(ranges, places, q, ctx, lse, k, v, code_q, code_k, *pieces)


def slide_tables(lengths_row, mask_all):
    cells = mask_all.shape[0]
    ends = jnp.cumsum(lengths_row)
    starts = ends - lengths_row
    slide = slide_index(jnp.arange(cells, dtype=jnp.int32), lengths_row)
    first = jnp.arange(cells // QUERY_TILE, dtype=jnp.int32) * QUERY_TILE
    first_slide = slide_index(first, lengths_row)
    last_slide = slide_index(first + (QUERY_TILE - 1), lengths_row)
    order = jnp.arange(lengths_row.shape[0], dtype=jnp.int32)

    def picked(table, index):
        return jnp.sum(jnp.where(index[:, None] == order[None, :], table[None, :], 0), axis=1)

    low = picked(starts, first_slide) // KEY_UNIT
    high = picked(ends, last_slide)
    tiles = (high - low * KEY_UNIT + KEY_TILE - 1) // KEY_TILE
    low = jnp.minimum(low, (cells - tiles * KEY_TILE) // KEY_UNIT)
    ranges = jnp.stack([low, tiles], axis=1).astype(jnp.int32)
    open_code = jnp.where(mask_all == 1, slide, -1)
    return ranges, slide[None, :], open_code[:, None]


def moved(value, target):
    groups, blocks = lax.axis_size("dp"), lax.axis_size("blk")
    pairs = []
    for g in range(groups):
        for b in range(blocks):
            there = target(g, b)
            if there is not None:
                pairs.append((g * blocks + b, there[0] * blocks + there[1]))
    return lax.ppermute(value, MESH_AXES, pairs)


def at_home(g, b):
    return (g & 1) == b >> (bits_of(lax.axis_size("blk")) - 1)


def head_block(g, b):
    return (b & (lax.axis_size("blk") // 2 - 1)) * 2 + (g & 1)


def worker_of(g, block_of_heads):
    half = lax.axis_size("blk") // 2
    return (g - g % 2) + block_of_heads % 2, (g % 2) * half + block_of_heads // 2


def owner_of(g, b, index):
    return (g - g % 2) + b // (lax.axis_size("blk") // 2), index


def pair_masks():
    return [1 << t for t in range(bits_of(lax.axis_size("blk")) - 1)]


def with_meta(cells, mask, lengths):
    count = lengths.shape[0]
    meta = jnp.concatenate([mask, lengths >> 7, lengths & 127]).astype(cells.dtype)
    meta = jnp.pad(meta, (0, cells.shape[1] - mask.shape[0] - 2 * count))
    return jnp.concatenate([cells, jnp.pad(meta[None], ((0, 7), (0, 0)))], axis=0)


def from_meta(meta, rows, count):
    meta = meta.astype(jnp.int32)
    high = meta[0, rows : rows + count]
    return meta[:, :rows].reshape(-1), high * 128 + meta[0, rows + count : rows + 2 * count]


def from_home(value):
    return moved(value, lambda g, b: (g ^ 1, b) if at_home(g, b) else None)


def paired(value, mask):
    return moved(value, lambda g, b: (g, b ^ mask) if at_home(g, b) else None)


def group_rows(own, use):
    blocks = lax.axis_size("blk")
    block = lax.axis_index("blk")
    mirror = moved(own, lambda g, b: None if at_home(g, b) else (g, blocks - 1 - b))
    held, rows = None, []
    for mirrored in (False, True):
        pieces = [(mirror if mirrored else own, 0)]
        for mask in pair_masks():
            pieces += [(paired(piece, mask), place ^ mask) for piece, place in pieces]
        pieces = [
            (piece, from_home(tied(piece, held) if mirrored else piece), blocks - 1 - (block ^ place) if mirrored else block ^ place)
            for piece, place in pieces
        ]
        held = use(pieces, held)
        rows += pieces
    return held, rows


def entry_kernel(count, place_ref, *refs):
    pieces, refs = refs[: 2 * count], refs[2 * count :]
    gain_ref, shift_ref = refs[:2]
    weights = refs[2:5]
    normed_ref, *out_refs = refs[-4:]
    step, home = pl.program_id(0), place_ref[count]
    rows = normed_ref.shape[0]
    for k in range(count):

        @pl.when(step == k)
        def _(k=k):
            value = jnp.where(home == 1, pieces[2 * k][:rows], pieces[2 * k + 1][:rows])
            unit, _ = norm_parts(value.astype(jnp.float32))
            normed_ref[...] = (unit * gain_ref[...] + shift_ref[...]).astype(jnp.bfloat16)

    for weight_ref, out_ref in zip(weights, out_refs):
        out_ref[...] = nn_dot(normed_ref[...], weight_ref[...]).astype(jnp.bfloat16)


def head_columns(weight):
    width = weight.shape[1] // lax.axis_size("blk")
    if width % 128 == 0:
        return weight, pl.BlockSpec((weight.shape[0], width), lambda i, place: (0, place[place.shape[0] - 1]))
    mine = head_block(lax.axis_index("dp"), lax.axis_index("blk")) * width
    return lax.dynamic_slice_in_dim(weight, mine, width, 1), resident((weight.shape[0], width))


def entry(pieces, gain, shift, weights, held):
    blocks, count = lax.axis_size("blk"), len(pieces)
    group, block = lax.axis_index("dp"), lax.axis_index("blk")
    rows, model = pieces[0][0].shape[0] - 8, pieces[0][0].shape[1]
    width = model // blocks
    home = at_home(group, block).astype(jnp.int32)
    table = jnp.stack([place for _, _, place in pieces] + [home, head_block(group, block)])
    narrow = pl.BlockSpec((rows, width), lambda i, place: (place[i], 0))
    shapes = [jax.ShapeDtypeStruct((blocks * rows, cols), jnp.bfloat16) for cols in (model,) + (width,) * 3]
    operands = [value for mine, other, _ in pieces for value in (mine, other)]
    specs = [resident(value.shape) for value in operands] + [resident((1, model))] * 2
    operands += [gain[None], shift[None]]
    for weight in weights:
        weight, spec = head_columns(weight)
        operands.append(weight)
        specs.append(spec)
    aliases = {}
    if held is not None:
        aliases = {1 + len(operands) + i: i for i in range(4)}
        operands += list(held)
        specs += [pl.BlockSpec(memory_space=pl.ANY)] * 4
    return pl.pallas_call(
        partial(entry_kernel, count),
        grid_spec=pltpu.PrefetchScalarGridSpec(
            num_scalar_prefetch=1,
            grid=(count,),
            in_specs=specs,
            out_specs=[pl.BlockSpec((rows, model), lambda i, place: (place[i], 0)), narrow, narrow, narrow],
        ),
        out_shape=shapes,
        input_output_aliases=aliases,
        cost_estimate=nothing(),
        name="entry",
    )(table, *operands)


def project_back_kernel(place_ref, normed_ref, dq_ref, dk_ref, dv_ref, wq_ref, wk_ref, wv_ref,
                        rows_ref, grad_ref, gain_ref, shift_ref, acc_ref, sum_ref):
    step = pl.program_id(0)
    width = dq_ref.shape[1]

    @pl.when(step == 0)
    def _():
        acc_ref[...] = jnp.zeros(acc_ref.shape, jnp.float32)
        sum_ref[...] = jnp.zeros(sum_ref.shape, jnp.float32)

    total = jnp.zeros(rows_ref.shape, jnp.float32)
    for kind, (grad, weight_ref) in enumerate(((dq_ref, wq_ref), (dk_ref, wk_ref), (dv_ref, wv_ref))):
        cols = slice(kind * width, (kind + 1) * width)
        total += nt_dot(grad[...], weight_ref[...])
        acc_ref[:, cols] += tn_dot(normed_ref[...], grad[...])
        sum_ref[:1, cols] += jnp.sum(grad[...].astype(jnp.float32), axis=0, keepdims=True)
    rows_ref[...] = total.astype(jnp.bfloat16)

    @pl.when(step == pl.num_programs(0) - 1)
    def _():
        grad_ref[...] = acc_ref[...].astype(jnp.bfloat16)
        gain = jnp.zeros((acc_ref.shape[0], width), jnp.float32)
        shift = jnp.zeros((acc_ref.shape[0], width), jnp.float32)
        for kind, weight_ref in enumerate((wq_ref, wk_ref, wv_ref)):
            cols = slice(kind * width, (kind + 1) * width)
            weight = weight_ref[...].astype(jnp.float32)
            gain += weight * acc_ref[:, cols]
            shift += weight * sum_ref[:1, cols]
        gain_ref[...] = lane_sums(gain)
        shift_ref[...] = lane_sums(shift)


def lane_sums(value):
    ones = jnp.ones((8, value.shape[1]), jnp.bfloat16)
    total = jnp.zeros((8, value.shape[0]), jnp.float32)
    for _ in range(3):
        part = value.astype(jnp.bfloat16)
        value = value - part.astype(jnp.float32)
        total += nt_dot(ones, part)
    return total


def project_back(normed, grads, weights):
    cells, width = grads[0].shape
    model = weights[0].shape[0]
    columns = [head_columns(weight) for weight in weights]
    table = head_block(lax.axis_index("dp"), lax.axis_index("blk"))[None]
    wide = pl.BlockSpec((ROW_TILE, model), lambda i, place: (i, 0))
    return pl.pallas_call(
        project_back_kernel,
        grid_spec=pltpu.PrefetchScalarGridSpec(
            num_scalar_prefetch=1,
            grid=(cells // ROW_TILE,),
            in_specs=[wide]
            + [pl.BlockSpec((ROW_TILE, width), lambda i, place: (i, 0))] * 3
            + [spec for _, spec in columns],
            out_specs=[wide, resident((model, 3 * width)), resident((8, model)), resident((8, model))],
            scratch_shapes=[pltpu.VMEM((model, 3 * width), jnp.float32), pltpu.VMEM((8, 3 * width), jnp.float32)],
        ),
        out_shape=[
            jax.ShapeDtypeStruct((cells, model), jnp.bfloat16),
            jax.ShapeDtypeStruct((model, 3 * width), jnp.bfloat16),
            jax.ShapeDtypeStruct((8, model), jnp.float32),
            jax.ShapeDtypeStruct((8, model), jnp.float32),
        ],
        cost_estimate=nothing(),
        name="project_back",
    )(table, normed, *grads, *[weight for weight, _ in columns])


def heads_at_owner():
    blocks, block = lax.axis_size("blk"), lax.axis_index("blk")
    return jnp.stack([(block - k) & (blocks - 1) for k in range(blocks)])


def rows_at_worker():
    blocks = lax.axis_size("blk")
    mine = head_block(lax.axis_index("dp"), lax.axis_index("blk"))
    return jnp.stack([(mine + k) & (blocks - 1) for k in range(blocks)])


def rows_to_owners(context):
    blocks = lax.axis_size("blk")
    places = rows_at_worker()
    rows = context.shape[0] // blocks
    return [
        moved(
            chunk(context, places[k] * rows, rows, 0),
            lambda g, b: owner_of(g, b, (head_block(g, b) + k) % blocks),
        )
        for k in range(blocks)
    ]


def heads_to_workers(pieces):
    blocks = lax.axis_size("blk")
    return [
        moved(piece, lambda g, b: worker_of(g, (b - k) % blocks)) for k, piece in enumerate(pieces)
    ]


def row_steps(partial_rows):
    blocks = lax.axis_size("blk")
    group, block = lax.axis_index("dp"), lax.axis_index("blk")
    rows = partial_rows.shape[0] // blocks
    home = at_home(group, block)
    (other,) = yield [partial_rows], lambda value: moved(
        value, lambda g, b: None if at_home(g, b) else (g ^ 1, b)
    )

    def taken(place):
        return [chunk(part, place * rows, rows, 0)[None] for part in (partial_rows, other)]

    mine = {r: (taken(block ^ r), taken(blocks - 1 - (block ^ r))) for r in range(blocks // 2)}
    for mask in reversed(pair_masks()):
        send = jnp.concatenate([summed(part) for r in range(mask) for part in mine[r + mask]], axis=0)
        (came,) = yield [send], lambda value, mask=mask: moved(
            value, lambda g, b: (g, b ^ mask) if at_home(g, b) else None
        )
        mine = {
            r: tuple(mine[r][k] + [came[2 * r + k : 2 * r + k + 1]] for k in range(2))
            for r in range(mask)
        }
    own, mirror = mine[0]
    (far,) = yield [summed(mirror)], lambda value: moved(
        value, lambda g, b: (g, blocks - 1 - b) if at_home(g, b) else None
    )
    return jnp.where(home, summed(own), far)[0]


def norm_parts(values):
    center = values - jnp.mean(values, axis=-1, keepdims=True)
    spread = jnp.mean(center * center, axis=-1, keepdims=True)
    scale = lax.rsqrt(spread + ln_eps)
    return center * scale, scale


def nothing():
    return pl.CostEstimate(flops=0, bytes_accessed=0, transcendentals=0)


def resident(shape):
    return pl.BlockSpec(shape, lambda *_: (0,) * len(shape))


def feed_kernel(head_ref, *refs):
    pieces = head_ref.shape[0]
    context_refs, (cell_ref, weight_ref), refs = refs[:pieces], refs[pieces : pieces + 2], refs[pieces + 2 :]
    context_ref, hidden_ref, refs = refs[6], refs[7], refs[:6] + refs[8:]

    @pl.when(pl.program_id(0) == 0)
    def _():
        width = weight_ref.shape[0] // pieces
        total = cell_ref[...].astype(jnp.float32)
        for k in range(pieces):
            begin = head_ref[k] * width
            piece = context_refs[k][...]
            total += nn_dot(piece, weight_ref[pl.ds(pl.multiple_of(begin, width), width), :])
            if width % 128 == 0:
                context_ref[:, pl.ds(pl.multiple_of(begin, width), width)] = piece
        hidden_ref[...] = total

    feed_body(hidden_ref, *refs)


def feed_body(hidden_ref, gain_ref, shift_ref, up_ref, up_bias_ref, down_ref, down_bias_ref,
                normed_ref, active_ref, slope_ref, two_ref, two_b_ref, acc_ref):
    step = pl.program_id(0)

    @pl.when(step == 0)
    def _():
        unit, _ = norm_parts(hidden_ref[...])
        normed_ref[...] = (unit * gain_ref[...] + shift_ref[...]).astype(jnp.bfloat16)
        acc_ref[...] = hidden_ref[...] + down_bias_ref[...]

    inner = nn_dot(normed_ref[...], up_ref[...]) + up_bias_ref[...]
    chance = 0.5 + 0.5 * lax.erf(inner * 2.0**-0.5)
    active = (inner * chance).astype(jnp.bfloat16)
    active_ref[...] = active
    slope = chance + inner * jnp.exp(-0.5 * inner * inner) * (2.0 * math.pi) ** -0.5
    slope_ref[...] = slope.astype(jnp.bfloat16)
    acc_ref[...] += nn_dot(active, down_ref[...])

    @pl.when(step == pl.num_programs(0) - 1)
    def _():
        two_ref[...] = acc_ref[...]
        two_b_ref[...] = acc_ref[...].astype(jnp.bfloat16)


def feed_forward(heads, contexts, cells, out_weight, gain, shift, up_weight, up_bias, down_weight, down_bias):
    rows, model = cells.shape
    inner = up_weight.shape[1]
    tile = FEED_TILE
    across = pl.BlockSpec((rows, tile), lambda j, heads: (0, j))
    return pl.pallas_call(
        feed_kernel,
        grid_spec=pltpu.PrefetchScalarGridSpec(
            num_scalar_prefetch=1,
            grid=(inner // tile,),
            in_specs=[resident(part.shape) for part in contexts]
            + [
                resident((rows, model)),
                resident((model, model)),
                resident((1, model)),
                resident((1, model)),
                pl.BlockSpec((model, tile), lambda j, heads: (0, j)),
                pl.BlockSpec((1, tile), lambda j, heads: (0, j)),
                pl.BlockSpec((tile, model), lambda j, heads: (j, 0)),
                resident((1, model)),
            ],
            out_specs=[
                resident((rows, model)),
                resident((rows, model)),
                resident((rows, model)),
                across,
                across,
                resident((rows, model)),
                resident((rows, model)),
            ],
            scratch_shapes=[pltpu.VMEM((rows, model), jnp.float32)],
        ),
        out_shape=[
            jax.ShapeDtypeStruct((rows, model), jnp.bfloat16),
            jax.ShapeDtypeStruct((rows, model), jnp.float32),
            jax.ShapeDtypeStruct((rows, model), jnp.bfloat16),
            jax.ShapeDtypeStruct((rows, inner), jnp.bfloat16),
            jax.ShapeDtypeStruct((rows, inner), jnp.bfloat16),
            jax.ShapeDtypeStruct((rows, model), jnp.float32),
            jax.ShapeDtypeStruct((rows, model), jnp.bfloat16),
        ],
        cost_estimate=nothing(),
        name="feed_forward",
    )(
        heads, *contexts, cells, out_weight, gain[None], shift[None], up_weight, up_bias[None], down_weight,
        down_bias[None],
    )


def feed_back_kernel(head_ref, two_ref, branch_ref, slope_ref, down_ref, up_ref, hidden_ref, gain_ref, weight_ref,
                     inner_ref, bias_ref, hidden_grad_ref, hidden_grad_b_ref, gain_grad_ref, shift_grad_ref,
                     *rest):
    piece_refs, acc_ref = rest[:-1], rest[-1]
    step = pl.program_id(0)

    @pl.when(step == 0)
    def _():
        acc_ref[...] = jnp.zeros(acc_ref.shape, jnp.float32)

    inner = (nt_dot(branch_ref[...], down_ref[...]) * slope_ref[...].astype(jnp.float32)).astype(jnp.bfloat16)
    inner_ref[...] = inner
    bias_ref[...] = jnp.sum(inner.astype(jnp.float32), axis=0, keepdims=True)
    acc_ref[...] += nt_dot(inner, up_ref[...])

    @pl.when(step == pl.num_programs(0) - 1)
    def _():
        unit, scale = norm_parts(hidden_ref[...])
        grad = acc_ref[...]
        gain_grad_ref[...] = jnp.sum(grad * unit, axis=0, keepdims=True)
        shift_grad_ref[...] = jnp.sum(grad, axis=0, keepdims=True)
        grad = grad * gain_ref[...]
        mean = jnp.mean(grad, axis=-1, keepdims=True)
        slant = jnp.mean(grad * unit, axis=-1, keepdims=True)
        total = two_ref[...] + scale * (grad - mean - unit * slant)
        hidden_grad_ref[...] = total
        total = total.astype(jnp.bfloat16)
        hidden_grad_b_ref[...] = total
        for k, piece_ref in enumerate(piece_refs):
            width = piece_ref.shape[1]
            begin = pl.multiple_of(head_ref[k] * width, width)
            piece_ref[...] = nt_dot(total, weight_ref[pl.ds(begin, width), :]).astype(jnp.bfloat16)


def feed_back(heads, grad_two, grad_branch, slope, down_weight, up_weight, hidden, gain, out_weight):
    rows, model = hidden.shape
    inner = up_weight.shape[1]
    tile = FEED_TILE
    count = heads.shape[0]
    return pl.pallas_call(
        feed_back_kernel,
        grid_spec=pltpu.PrefetchScalarGridSpec(
            num_scalar_prefetch=1,
            grid=(inner // tile,),
            in_specs=[
                resident((rows, model)),
                resident((rows, model)),
                pl.BlockSpec((rows, tile), lambda j, heads: (0, j)),
                pl.BlockSpec((tile, model), lambda j, heads: (j, 0)),
                pl.BlockSpec((model, tile), lambda j, heads: (0, j)),
                resident((rows, model)),
                resident((1, model)),
                resident((model, model)),
            ],
            out_specs=[
                pl.BlockSpec((rows, tile), lambda j, heads: (0, j)),
                pl.BlockSpec((1, tile), lambda j, heads: (0, j)),
                resident((rows, model)),
                resident((rows, model)),
                resident((1, model)),
                resident((1, model)),
            ]
            + [resident((rows, model // count))] * count,
            scratch_shapes=[pltpu.VMEM((rows, model), jnp.float32)],
        ),
        out_shape=[
            jax.ShapeDtypeStruct((rows, inner), jnp.bfloat16),
            jax.ShapeDtypeStruct((1, inner), jnp.float32),
            jax.ShapeDtypeStruct((rows, model), jnp.float32),
            jax.ShapeDtypeStruct((rows, model), jnp.bfloat16),
            jax.ShapeDtypeStruct((1, model), jnp.float32),
            jax.ShapeDtypeStruct((1, model), jnp.float32),
        ]
        + [jax.ShapeDtypeStruct((rows, model // count), jnp.bfloat16)] * count,
        cost_estimate=nothing(),
        name="feed_back",
    )(heads, grad_two, grad_branch, slope, down_weight, up_weight, hidden, gain[None], out_weight)


def tn_dot(left, right):
    return lax.dot_general(left, right, (((0,), (0,)), ((), ())), preferred_element_type=jnp.float32)


def weights_kernel(lefts_at, ready, place_ref, column_ref, *refs):
    count = len(lefts_at)
    scratch = 0 if ready else count
    lefts = refs[: max(lefts_at) + 1]
    rights = refs[len(lefts) : len(lefts) + count]
    refs, ordered = refs[len(lefts) + count : len(refs) - scratch], refs[len(refs) - scratch :]
    vector_ref, (keep_ref, send_ref) = refs[:-2], refs[-2:]
    held, grouped, _, width = keep_ref.shape
    if ready:
        ordered = rights
    else:

        @pl.when(pl.program_id(0) == 0)
        def _():
            for right_ref, ordered_ref in zip(rights, ordered):
                for piece in range(2 * held):
                    begin = pl.multiple_of(column_ref[piece] * width, width)
                    ordered_ref[:, piece * width : (piece + 1) * width] = right_ref[:, pl.ds(begin, width)]

    begin = 0
    for at, ordered_ref in zip(lefts_at, ordered):
        total = lefts[at].shape[1]
        tile = min(total, 256)
        rows = min(tile, total // grouped)
        for first in range(0, total, tile):
            value = tn_dot(lefts[at][:, first : first + tile], ordered_ref[...]).astype(jnp.bfloat16)
            for inside in range(0, tile, rows):
                z, row = divmod(first + inside, total // grouped)
                part = value[inside : inside + rows]
                place = slice(begin + row, begin + row + rows)
                for piece in range(held):
                    keep_ref[piece, z, place, :] = part[:, piece * width : (piece + 1) * width]
                    other = held + piece
                    send_ref[piece, z, place, :] = part[:, other * width : (other + 1) * width]
        begin += total // grouped

    if vector_ref:
        keep_ref[:, :, begin:, :] = vector_ref[0][0]
        send_ref[:, :, begin:, :] = vector_ref[0][1]


def relative_columns(value, steps):
    group = lax.axis_index("dp")
    masks = relative_masks(steps)
    size = value.shape[1] // len(masks)
    return jnp.concatenate([chunk(value, (group ^ mask) * size, size, 1) for mask in masks], axis=1)


def weight_pieces(pairs, steps, vector=None):
    blocks, block = lax.axis_size("blk"), lax.axis_index("blk")
    pieces, group = lax.axis_size("dp"), lax.axis_index("dp")
    width = D // pieces
    masks = relative_masks(blk_masks())
    sizes = [left.shape[1] // blocks for left, _, _ in pairs]
    places = jnp.stack([block ^ mask for mask in masks])
    columns = jnp.stack([group ^ mask for mask in relative_masks(steps)])
    cells = pairs[0][1].shape[0]
    lefts, lefts_at = [], []
    for left, _, _ in pairs:
        if not any(left is seen for seen in lefts):
            lefts.append(left)
        lefts_at.append(next(i for i, seen in enumerate(lefts) if left is seen))
    rights = [right for _, right, _ in pairs]
    parts = [part for _, _, part in pairs]
    grouped = max(1, 128 // min(sizes))
    ready = grouped > 1 or width % 128 != 0
    if ready:
        rights = [
            relative_columns(right[:, part * D : (part + 1) * D], steps) for right, part in zip(rights, parts)
        ]
        parts = [0] * len(parts)
        lefts = [
            jnp.concatenate(
                [chunk(left, (block ^ mask) * (left.shape[1] // blocks), left.shape[1] // blocks, 1) for mask in masks],
                axis=1,
            )
            for left in lefts
        ]
        places = jnp.arange(blocks, dtype=jnp.int32)
    rows = sum(sizes) + (0 if vector is None else vector.shape[3])
    out = pl.BlockSpec((pieces // 2, grouped, rows, width), lambda z, place, column: (0, z, 0, 0))
    specs = [
        pl.BlockSpec((cells, left.shape[1] // blocks * grouped), lambda z, place, column: (0, place[z]))
        for left in lefts
    ]
    specs += [pl.BlockSpec((cells, D), lambda z, place, column, part=part: (0, part)) for part in parts]
    operands = lefts + rights
    if vector is not None:
        specs.append(
            pl.BlockSpec(
                (2, pieces // 2, grouped, vector.shape[3], width), lambda z, place, column: (0, 0, z, 0, 0)
            )
        )
        operands.append(vector)
    shape = jax.ShapeDtypeStruct((pieces // 2, blocks, rows, width), jnp.bfloat16)
    return pl.pallas_call(
        partial(weights_kernel, lefts_at, ready),
        grid_spec=pltpu.PrefetchScalarGridSpec(
            num_scalar_prefetch=2,
            grid=(blocks // grouped,),
            in_specs=specs,
            out_specs=[out, out],
            scratch_shapes=[pltpu.VMEM((cells, D), jnp.bfloat16) for _ in pairs if not ready],
        ),
        out_shape=[shape, shape],
        cost_estimate=nothing(),
        name="weight_pieces",
    )(places, columns, *operands)


def weight_steps(keep, send, flipped, parts):
    steps = dp_order(flipped)
    (came,) = yield [send], by_mask(steps[0], 0)
    size = keep.shape[0]
    terms = [[keep[place], came[place]] for place in range(size)]
    for mask in steps[1:]:
        size = size // 2
        came = yield [summed(terms[place]) for place in range(size, 2 * size)], by_mask(mask, 0)
        terms = [terms[place] + [came[place]] for place in range(size)]
    terms = terms[0]
    size = keep.shape[1]
    for mask in blk_masks():
        size = size // 2
        (came,) = yield [summed([term[size : 2 * size] for term in terms])], by_mask(0, mask)
        terms = [term[:size] for term in terms] + [came]
    value = summed(terms)
    for mask in steps[:0:-1]:
        (came,) = yield [value], by_mask(mask, 0)
        value = jnp.concatenate([value, came], axis=0)
    (came,) = yield [value], by_mask(steps[0], 0)
    return spread_columns(value, came, relative_table(steps, lax.axis_index("dp")), parts)


def local(
    cell_states,
    slide_lengths,
    cell_mask,
    latent_noise,
    train_step,
    attn_gain,
    attn_shift,
    query_weight,
    key_weight,
    value_weight,
    out_weight,
    ffn_gain,
    ffn_shift,
    up_weight,
    up_bias,
    down_weight,
    down_bias,
    encode_weight,
    encode_bias,
    decode_weight,
    prior_means,
    prior_logits,
    out_grad,
):
    rows_here = cell_states.shape[0]
    blocks = lax.axis_size("blk")
    group, block = lax.axis_index("dp"), lax.axis_index("blk")
    width = D // blocks
    x_float = cell_states.astype(jnp.float32)
    _, norm_back = jax.vjp(layer_norm, x_float, attn_gain, attn_shift)
    weights = (query_weight, key_weight, value_weight)
    held, pieces = group_rows(
        with_meta(cell_states, cell_mask, slide_lengths[0]),
        lambda pieces, held: entry(pieces, attn_gain, attn_shift, weights, held),
    )
    normed_b, queries, keys, values = held
    meta = jnp.zeros((blocks, D), jnp.bfloat16)
    order = jnp.arange(blocks, dtype=jnp.int32)
    for mine, other, place in pieces:
        row = jnp.where(at_home(group, block), mine[rows_here], other[rows_here])
        meta = jnp.where(order[:, None] == place, row[None], meta)
    mask_all, lengths_row = from_meta(meta, rows_here, slide_lengths.shape[1])
    ranges, query_code, key_code = slide_tables(lengths_row, mask_all)
    context_here, log_total = attention_forward(ranges, queries, keys, values, query_code, key_code)
    contexts = rows_to_owners(context_here)
    owner_heads = heads_at_owner()
    context_b, hidden, normed_two_b, activated_b, slope_b, hidden_two, hidden_two_b = feed_forward(
        owner_heads, contexts, cell_states, out_weight, ffn_gain, ffn_shift, up_weight, up_bias, down_weight,
        down_bias,
    )
    if width % 128:
        context_b = jnp.zeros((rows_here, D), jnp.bfloat16)
        for k in range(blocks):
            context_b = lax.dynamic_update_slice_in_dim(context_b, contexts[k], owner_heads[k] * width, 1)
    encoded = plain_dot(hidden_two_b, encode_weight) + encode_bias
    latent_mean = encoded[:, :LAT]
    latent_logvar = encoded[:, LAT:]
    spread = jnp.exp(0.5 * latent_logvar)
    noise_float = latent_noise.astype(jnp.float32)
    latent_b = (latent_mean + spread * noise_float).astype(jnp.bfloat16)
    output = hidden_two + plain_dot(latent_b, decode_weight)
    (kl_dim, categorical), kl_back = jax.vjp(
        kl_terms, latent_mean, latent_logvar, prior_means, prior_logits
    )
    real = cell_mask.astype(jnp.float32)
    sums = jnp.concatenate(
        [
            jnp.sum(kl_dim * real[:, None], axis=0),
            jnp.sum(categorical * real)[None],
            jnp.sum(real)[None],
            jnp.zeros((126,), jnp.float32),
        ]
    )
    sums = summed_everywhere(sums)
    kl_sum, cat_sum, count = sums[:LAT], sums[LAT], sums[LAT + 1]
    kbar = kl_sum / count
    floored = jnp.sum(jnp.maximum(kbar, free_floor))
    cat_mean = cat_sum / count
    beta = jnp.minimum(1.0, (train_step[0].astype(jnp.float32) + 1.0) / WARM)
    active = (kbar > free_floor).astype(jnp.float32)
    grad_latent = cols_dot(out_grad, decode_weight)
    grad_mean, grad_logvar, grad_means, grad_prior = kl_back(
        (beta * real[:, None] * active[None, :], beta * real)
    )
    grad_mean = grad_mean + grad_latent
    grad_logvar = grad_logvar + grad_latent * 0.5 * spread * noise_float
    grad_encoded_b = jnp.concatenate([grad_mean, grad_logvar], axis=1).astype(jnp.bfloat16)
    grad_encode_bias = jnp.sum(grad_encoded_b.astype(jnp.float32), axis=0)
    grad_two = out_grad.astype(jnp.float32) + cols_dot(grad_encoded_b, encode_weight)
    grad_down_bias = jnp.sum(grad_two, axis=0)
    grad_branch_b = grad_two.astype(jnp.bfloat16)

    straight, flipped = dp_order(False), dp_order(True)
    block_rows = D // blocks
    down = Exchange(
        weight_steps(
            *weight_pieces(
                [(activated_b, grad_branch_b, 0), (hidden_two_b, grad_encoded_b, 0), (latent_b, out_grad, 0)],
                straight,
            ),
            False,
            [(4 * block_rows, 1), (block_rows, 1), (block_rows // 2, 1)],
        )
    )
    back = feed_back(
        owner_heads, grad_two, tied(grad_branch_b, down.last), slope_b, down_weight, up_weight, hidden, ffn_gain,
        out_weight,
    )
    grad_inner_b, grad_up_bias, grad_hidden, grad_attn_b, grad_ffn_gain, grad_ffn_shift = back[:6]
    grads_here = heads_to_workers(back[6:])
    by_block = lambda part: part.reshape(blocks, -1)
    means_block = jnp.moveaxis(grad_means.reshape(K, blocks, LAT // blocks), 1, 0)
    vectors = [
        by_block(grad_ffn_gain),
        by_block(grad_ffn_shift),
        by_block(grad_up_bias),
        by_block(grad_down_bias),
        by_block(grad_encode_bias),
        by_block(means_block),
        by_block(grad_prior),
    ]
    sizes = [part.shape[1] for part in vectors]
    vector = jnp.concatenate([part.astype(jnp.bfloat16) for part in vectors], axis=1)
    vector_rows = -(-sum(sizes) // (8 * D)) * 8
    vector = jnp.pad(vector, ((0, 0), (0, vector_rows * D - sum(sizes))))
    vector = relative_columns(vector.reshape(blocks * vector_rows, D), flipped)
    devices_along = lax.axis_size("dp")
    vector = vector.reshape(blocks, vector_rows, 2, devices_along // 2, D // devices_along)
    vector = jnp.transpose(vector, (2, 3, 0, 1, 4))
    vector = jnp.concatenate([chunk(vector, block ^ mask, 1, 2) for mask in relative_masks(blk_masks())], axis=2)
    up_pieces = weight_pieces(
        [(normed_two_b, tied(grad_inner_b, back[6:]), part) for part in range(4)] + [(context_b, grad_attn_b, 0)],
        flipped,
        vector,
    )
    up = Exchange(
        weight_steps(
            *tied(up_pieces, grads_here), True, [(block_rows, 4), (block_rows, 1), (vector_rows, 1)]
        )
    )
    token = down.advance(up.last, hold=True)
    token = up.advance(token, hold=True)
    grads = attention_backward(
        ranges, rows_at_worker(), tied(queries, token), grads_here, context_here, log_total, keys, values, query_code,
        key_code,
    )
    grads = tied(grads, (down.flight, up.flight))
    down.release(grads[0])
    up.release(grads[0])
    partial_rows, grad_heads, part_gain, part_shift = project_back(normed_b, grads, weights)
    partial_rows, grad_heads = tied((partial_rows, grad_heads), (down.flight, up.flight))
    row_sum = Exchange(row_steps(partial_rows))
    part_shift = part_shift[0]
    part_gain = (part_gain[0] - attn_shift * part_shift) / attn_gain
    token = up.advance(grad_heads)
    token = down.advance(token)
    extra = jnp.concatenate([by_block(part_gain), by_block(part_shift)], axis=1)
    extra_size = extra.shape[1]
    extra = jnp.pad(extra, ((0, 0), (0, 3 * width - extra_size))).astype(jnp.bfloat16)
    pieces = lax.axis_size("dp") // 2
    piece_rows = block_rows // pieces
    grad_heads = grad_heads.reshape(blocks, pieces, piece_rows, 3 * width)
    extra = jnp.broadcast_to(extra[:, None, None, :], (blocks, pieces, 8, 3 * width))
    attn = Exchange(head_steps(jnp.concatenate([grad_heads, extra], axis=2)))
    token = attn.last
    order = [row_sum, attn, down, row_sum, up, attn]
    live = [down, row_sum, up, attn]
    for bundle in order:
        token = bundle.advance(token)
    while any(bundle.result is None for bundle in live):
        for bundle in live:
            if bundle.result is None:
                token = bundle.advance(token)
    grad_normed = row_sum.result.astype(jnp.float32)
    grad_from_norm, _, _ = norm_back(grad_normed)
    states_grad = grad_hidden + grad_from_norm
    mine, other = attn.result
    attn_vector = jnp.sum((mine[0].astype(jnp.float32) + other[0].astype(jnp.float32)), axis=0)[piece_rows]
    main = spread_heads(mine, other, piece_rows)
    down_sum, encode_sum, decode_sum = down.result
    up_sum, out_sum, vector_sum = up.result
    flat = vector_sum.reshape(-1)
    small, begin = [], 0
    for size in sizes:
        small.append(flat[begin : begin + size])
        begin += size
    totals = (
        attn_vector[: extra_size // 2],
        attn_vector[extra_size // 2 : extra_size],
        main[0],
        main[1],
        main[2],
        out_sum,
        small[0],
        small[1],
        up_sum,
        small[2],
        down_sum,
        small[3],
        encode_sum,
        small[4],
        decode_sum,
        small[5].reshape(K, LAT // blocks),
        small[6],
    )
    kl_out = (floored / LAT + cat_mean).reshape(1)
    return (output.astype(jnp.bfloat16), states_grad, kl_out) + tuple(totals)


def solution(mesh):
    in_specs = (
        P(("dp", "blk"), None),
        P("dp", None),
        P(("dp", "blk")),
        P(("dp", "blk"), None),
        P(),
        P(),
        P(),
        P(),
        P(),
        P(),
        P(),
        P(),
        P(),
        P(),
        P(),
        P(),
        P(),
        P(),
        P(),
        P(),
        P(),
        P(),
        P(("dp", "blk"), None),
    )
    out_specs = (
        P(("dp", "blk"), None),
        P(("dp", "blk"), None),
        P(),
        P("blk"),
        P("blk"),
        P("blk", None),
        P("blk", None),
        P("blk", None),
        P("blk", None),
        P("blk"),
        P("blk"),
        P("blk", None),
        P("blk"),
        P("blk", None),
        P("blk"),
        P("blk", None),
        P("blk"),
        P("blk", None),
        P(None, "blk"),
        P("blk"),
    )
    return jax.shard_map(local, mesh=mesh, in_specs=in_specs, out_specs=out_specs, check_vma=False)
```

```python
import math
from functools import partial

import jax
import jax.numpy as jnp
from jax import lax
from jax.experimental import pallas as pl
from jax.experimental.pallas import tpu as pltpu
from jax.sharding import PartitionSpec as P

D = 1024
H = 16
HD = 64
LAT = 512
K = 16
WARM = 2000


ln_eps = 1e-05
free_floor = 1.3
neg_fill = -1e30

QUERY_TILE = 256
KEY_TILE = 384
ROW_TILE = 512
KEY_UNIT = 128
FEED_TILE = 1024


def layer_norm(values, gain, shift):
    center = values - jnp.mean(values, axis=-1, keepdims=True)
    spread = jnp.mean(center * center, axis=-1, keepdims=True)
    return center * lax.rsqrt(spread + ln_eps) * gain + shift


def slide_index(position, lengths_row):
    ends = jnp.cumsum(lengths_row)
    return jnp.sum((position[:, None] >= ends[None, :]).astype(jnp.int32), axis=1)


def exact_dot(left, right):
    return jnp.dot(left, right, precision=lax.Precision.HIGHEST, preferred_element_type=jnp.float32)


def kl_terms(latent_mean, latent_logvar, prior_means, prior_logits):
    log_prior = jax.nn.log_softmax(prior_logits)
    logits = exact_dot(latent_mean, prior_means.T) * LAT ** (-0.5) + log_prior[None, :]
    resp = jax.nn.softmax(logits, axis=-1)
    log_resp = jax.nn.log_softmax(logits, axis=-1)
    mixed_mean = exact_dot(resp, prior_means)
    mixed_square = exact_dot(resp, prior_means * prior_means)
    kl_dim = 0.5 * (
        jnp.exp(latent_logvar)
        + latent_mean * latent_mean
        - 2.0 * latent_mean * mixed_mean
        + mixed_square
        - 1.0
        - latent_logvar
    )
    categorical = jnp.sum(resp * (log_resp - log_prior[None, :]), axis=-1)
    return (kl_dim, categorical)


def plain_dot(left, right):
    return jnp.dot(left, right, preferred_element_type=jnp.float32)


def rows_dot(left, right):
    return lax.dot_general(
        left, right, (((0,), (0,)), ((), ())), preferred_element_type=jnp.float32
    )


def cols_dot(left, right):
    return lax.dot_general(
        left, right, (((1,), (1,)), ((), ())), preferred_element_type=jnp.float32
    )


MESH_AXES = ("dp", "blk")


def swapped(value, dp_mask, blk_mask):
    groups, blocks = lax.axis_size("dp"), lax.axis_size("blk")
    pairs = [
        (g * blocks + b, (g ^ dp_mask) * blocks + (b ^ blk_mask))
        for g in range(groups)
        for b in range(blocks)
    ]
    return lax.ppermute(value, MESH_AXES, pairs)


def bits_of(count):
    return count.bit_length() - 1


def dp_masks():
    return [1 << t for t in range(bits_of(lax.axis_size("dp")))]


def blk_masks():
    return [(2 << t) - 1 for t in range(bits_of(lax.axis_size("blk")))]


def tree_sum(value, masks):
    places = [(0, 0)]
    for dp_mask, blk_mask in masks:
        places = places + [(dp ^ dp_mask, blk ^ blk_mask) for dp, blk in places]
    terms = [value] + [swapped(value, dp, blk) for dp, blk in places[1:]]
    while len(terms) > 1:
        terms = [terms[i] + terms[i + 1] for i in range(0, len(terms), 2)]
    return terms[0]


def summed_everywhere(value):
    value = tree_sum(value, [(1, 0)])
    value = tree_sum(value, [(mask, 0) for mask in dp_masks()[1:]])
    return tree_sum(value, [(0, mask) for mask in blk_masks()])


def added(left, right):
    return (left.astype(jnp.float32) + right.astype(jnp.float32)).astype(jnp.bfloat16)


def summed(terms):
    total = terms[0].astype(jnp.float32)
    for term in terms[1:]:
        total = total + term.astype(jnp.float32)
    return total.astype(jnp.bfloat16)


def chunk(value, start, size, axis):
    return lax.dynamic_slice_in_dim(value, start, size, axis)


def tied(value, other):
    return lax.optimization_barrier((value, other))[0]


class Exchange:
    def __init__(self, steps):
        self.steps = steps
        self.result = None
        self.last = None
        self.flight = None
        self._take(lambda: next(self.steps))

    def _take(self, step, hold=False):
        try:
            values, permute = step()
            first = len(values) // 2 if hold else len(values)
            self.last = values
            self.flight = [permute(value) for value in values[:first]]
            self.held = (values[first:], permute)
        except StopIteration as end:
            self.result = end.value
            self.last = end.value
            self.flight = None

    def advance(self, token, hold=False):
        came = tied(self.flight, token)
        self._take(lambda: self.steps.send(came), hold)
        return self.last

    def release(self, token):
        values, permute = self.held
        self.flight = self.flight + [permute(tied(value, token)) for value in values]


def by_mask(dp_mask, blk_mask):
    return lambda value: swapped(value, dp_mask, blk_mask)


def dp_order(flipped):
    masks = dp_masks()
    return masks[:1] + masks[1:][::-1] if flipped else masks


def relative_masks(steps):
    places = [0]
    for step in steps[::-1]:
        places = places + [place ^ step for place in places]
    return places


def relative_table(steps, mine):
    masks = relative_masks(steps)
    inverse = [masks.index(place) for place in range(len(masks))]
    order = jnp.arange(len(masks), dtype=jnp.int32)
    wanted = order ^ mine
    return sum(jnp.where(wanted == place, inverse[place], 0) for place in range(len(masks)))


def spread_kernel(parts, table_ref, mine_ref, other_ref, *out_refs):
    held, _, width = mine_ref.shape
    cols = 2 * held * width
    for place in range(2 * held):
        index = table_ref[place]
        piece = jnp.where(index < held, mine_ref[index & (held - 1)], other_ref[index & (held - 1)])
        piece = piece.astype(jnp.float32)
        for out_ref, (begin, count, times) in zip(out_refs, parts):
            for time in range(times):
                row, column = begin + time * count, time * cols + place * width
                out_ref[:, column : column + width] = piece[row : row + count]


def spread_columns(mine, other, table, parts):
    held, rows, width = mine.shape
    cols = 2 * held * width
    begin, placed, shapes = 0, [], []
    for count, times in parts:
        placed.append((begin, count, times))
        shapes.append(jax.ShapeDtypeStruct((count, times * cols), jnp.float32))
        begin += count * times
    return pl.pallas_call(
        partial(spread_kernel, placed),
        out_shape=shapes,
        grid_spec=pltpu.PrefetchScalarGridSpec(
            num_scalar_prefetch=1,
            grid=(1,),
            in_specs=[resident((held, rows, width))] * 2,
            out_specs=[resident(shape.shape) for shape in shapes],
        ),
        cost_estimate=nothing(),
        name="spread_columns",
    )(table, mine, other)


def head_steps(value):
    blocks = lax.axis_size("blk")
    group, block = lax.axis_index("dp"), lax.axis_index("blk")
    half = blocks // 2
    steps = dp_masks()[1:]
    masks = relative_masks([step >> 1 for step in steps])
    taken = [[chunk(value, (group >> 1) ^ mask, 1, 1)] for mask in masks]
    size = len(masks)
    for step in steps:
        size = size // 2
        send = jnp.concatenate([summed(taken[place]) for place in range(size, 2 * size)], axis=1)
        (came,) = yield [send], by_mask(step, 0)
        taken = [taken[place] + [came[:, place : place + 1]] for place in range(size)]
    side = block >> (bits_of(blocks) - 1)
    away = [chunk(term, (1 - side) * half, half, 0) for term in taken[0]]
    (came,) = yield [summed(away)], by_mask(0, half)
    terms = [chunk(term, side * half, half, 0) for term in taken[0]] + [came]
    place = block & (half - 1)
    pieces = [summed([chunk(term, place, 1, 0) for term in terms])]
    for k in range(1, half):
        send = summed([chunk(term, place ^ k, 1, 0) for term in terms])
        (came,) = yield [send], by_mask(0, k)
        pieces.append(came)
    value = jnp.concatenate(pieces, axis=1)
    for step in steps[::-1]:
        (came,) = yield [value], by_mask(step, 0)
        value = jnp.concatenate([value, came], axis=0)
    (other,) = yield [value], by_mask(1, 0)
    return value, other


def heads_kernel(table_ref, mine_ref, other_ref, *out_refs):
    pieces = pl.num_programs(0)
    place, core = table_ref[pieces], table_ref[pieces + 1]
    half = mine_ref.shape[1]
    rows = out_refs[0].shape[0]
    width = mine_ref.shape[3] // 3
    for chip in range(half):
        mine = mine_ref[0, chip ^ place].astype(jnp.float32)
        other = other_ref[0, chip ^ place].astype(jnp.float32)
        for c in range(2):
            value = jnp.where(core == c, mine, other)
            column = (2 * chip + c) * width
            for kind in range(3):
                out_refs[kind][:, column : column + width] = value[:rows, kind * width : (kind + 1) * width]


def spread_heads(mine, other, rows):
    blocks = lax.axis_size("blk")
    group, block = lax.axis_index("dp"), lax.axis_index("blk")
    pieces, half, held_rows, width = mine.shape
    table = relative_table([step >> 1 for step in dp_masks()[1:]], group >> 1)
    table = jnp.concatenate([table, jnp.stack([block & (half - 1), group & 1])])
    held = pl.BlockSpec((1, half, held_rows, width), lambda i, table: (table[i], 0, 0, 0))
    cols = 2 * half * width // 3
    return pl.pallas_call(
        heads_kernel,
        out_shape=(jax.ShapeDtypeStruct((pieces * rows, cols), jnp.float32),) * 3,
        grid_spec=pltpu.PrefetchScalarGridSpec(
            num_scalar_prefetch=1,
            grid=(pieces,),
            in_specs=[held, held],
            out_specs=[pl.BlockSpec((rows, cols), lambda i, table: (i, 0))] * 3,
        ),
        cost_estimate=nothing(),
        name="spread_heads",
    )(table, mine, other)


def head_lanes(value, head):
    lane = lax.broadcasted_iota(jnp.int32, value.shape, 1) // HD
    return jnp.where(lane == head, value, jnp.zeros_like(value))

def nt_dot(left, right):
    return lax.dot_general(left, right, (((1,),(1,)),((),())), preferred_element_type=jnp.float32)

def nn_dot(left, right):
    return lax.dot_general(left, right, (((1,),(0,)),((),())), preferred_element_type=jnp.float32)

def allowed_pairs(code_k, code_q, block_k, tile):
    key_pos = block_k + lax.broadcasted_iota(jnp.int32, tile, 0)
    query_pos = pl.program_id(0) * QUERY_TILE + lax.broadcasted_iota(jnp.int32, tile, 1)
    return (code_k == code_q) | (key_pos == query_pos)

def forward_kernel(range_ref, q_ref, k_ref, v_ref, cq_ref, ck_ref, ctx_ref, lse_ref, m_ref, l_ref, acc_ref, vt_ref):
    nh = q_ref.shape[1] // HD
    step = pl.program_id(0)

    @pl.when(step == 0)
    def _():
        vt_ref[...] = v_ref[...].T

    m_ref[...] = jnp.full(m_ref.shape, neg_fill, jnp.float32)
    l_ref[...] = jnp.zeros(l_ref.shape, jnp.float32)
    acc_ref[...] = jnp.zeros(acc_ref.shape, jnp.float32)
    code_q = cq_ref[...]
    scaled = (q_ref[...].astype(jnp.float32) * HD ** (-0.5)).astype(jnp.bfloat16)
    def body(kb, _):
        start = pl.multiple_of(range_ref[step, 0] * KEY_UNIT + kb * KEY_TILE, KEY_UNIT)
        keys = k_ref[pl.ds(start, KEY_TILE), :]
        open_pair = allowed_pairs(ck_ref[pl.ds(start, KEY_TILE), :], code_q, start, (KEY_TILE, QUERY_TILE))
        bias = jnp.where(open_pair, 0.0, neg_fill)
        rows = [slice(h * HD, (h + 1) * HD) for h in range(nh)]
        scores = [nt_dot(keys[:, rows[h]], scaled[:, rows[h]]) + bias for h in range(nh)]
        probs, scales = [], []
        for h in range(nh):
            m_old = m_ref[h : h + 1, :]
            m_new = jnp.maximum(m_old, jnp.max(scores[h], axis=0, keepdims=True))
            p = jnp.exp(scores[h] - m_new)
            alpha = jnp.exp(m_old - m_new)
            l_ref[h : h + 1, :] = l_ref[h : h + 1, :] * alpha + jnp.sum(p, axis=0, keepdims=True)
            m_ref[h : h + 1, :] = m_new
            probs.append(p.astype(jnp.bfloat16))
            scales.append(alpha)
        for h in range(nh):
            part = nn_dot(vt_ref[rows[h], pl.ds(start, KEY_TILE)], probs[h])
            acc_ref[rows[h], :] = acc_ref[rows[h], :] * scales[h] + part
        return 0
    lax.fori_loop(0, range_ref[step, 1], body, 0)
    for h in range(nh):
        rows = slice(h*HD, (h+1)*HD)
        acc_ref[rows, :] = acc_ref[rows, :] / l_ref[h:h+1, :]
    ctx_ref[...] = acc_ref[...].T.astype(jnp.bfloat16)
    lse_ref[...] = m_ref[...] + jnp.log(l_ref[...])

def attention_forward(ranges, q, k, v, code_q, code_k):
    N, W = q.shape
    nh = W // HD
    full = lambda shape: pl.BlockSpec(shape, lambda i, r: (0,)*len(shape))
    return pl.pallas_call(
        forward_kernel,
        out_shape=(jax.ShapeDtypeStruct((N, W), jnp.bfloat16), jax.ShapeDtypeStruct((nh, N), jnp.float32)),
        grid_spec=pltpu.PrefetchScalarGridSpec(
            num_scalar_prefetch=1, grid=(N//QUERY_TILE,),
            in_specs=[pl.BlockSpec((QUERY_TILE, W), lambda i, r: (i, 0)), full((N, W)), full((N, W)),
                      pl.BlockSpec((1, QUERY_TILE), lambda i, r: (0, i)), full((N, 1))],
            out_specs=[pl.BlockSpec((QUERY_TILE, W), lambda i, r: (i, 0)), pl.BlockSpec((nh, QUERY_TILE), lambda i, r: (0, i))],
            scratch_shapes=[pltpu.VMEM((nh, QUERY_TILE), jnp.float32), pltpu.VMEM((nh, QUERY_TILE), jnp.float32), pltpu.VMEM((W, QUERY_TILE), jnp.float32), pltpu.VMEM((W, N), jnp.bfloat16)]),
        cost_estimate=nothing(),
        name="attention_forward",
    )(ranges, q, k, v, code_q, code_k)

def backward_kernel(range_ref, row_ref, q_ref, ctx_ref, lse_ref, k_ref, v_ref, cq_ref, ck_ref,
                    *refs):
    pieces = row_ref.shape[0]
    do_refs, (dq_ref, dk_ref, dv_ref, dqt_ref, dk_acc, dv_acc, kt_ref, do_ref) = refs[:pieces], refs[pieces:]
    nh = q_ref.shape[1] // HD
    step = pl.program_id(0)
    @pl.when(step == 0)
    def _():
        dk_acc[...] = jnp.zeros(dk_acc.shape, jnp.float32)
        dv_acc[...] = jnp.zeros(dv_acc.shape, jnp.float32)
        kt_ref[...] = k_ref[...].T
        for k, piece_ref in enumerate(do_refs):
            rows = piece_ref.shape[0]
            do_ref[pl.ds(pl.multiple_of(row_ref[k] * rows, rows), rows), :] = piece_ref[...]

    dqt_ref[...] = jnp.zeros(dqt_ref.shape, jnp.float32)
    code_q = cq_ref[...]
    scaled = (q_ref[...].astype(jnp.float32) * HD ** (-0.5)).astype(jnp.bfloat16)
    grads = do_ref[pl.ds(pl.multiple_of(step * QUERY_TILE, QUERY_TILE), QUERY_TILE), :]
    product = (grads.astype(jnp.float32) * ctx_ref[...].astype(jnp.float32)).T
    deltas = [jnp.sum(product[h*HD:(h+1)*HD, :], axis=0, keepdims=True) for h in range(nh)]
    q_all = jnp.concatenate([head_lanes(scaled, h) for h in range(nh)], axis=0)
    do_all = jnp.concatenate([head_lanes(grads, h) for h in range(nh)], axis=0)
    def body(kb, _):
        start = pl.multiple_of(range_ref[step, 0] * KEY_UNIT + kb * KEY_TILE, KEY_UNIT)
        keys = k_ref[pl.ds(start, KEY_TILE), :]
        values = v_ref[pl.ds(start, KEY_TILE), :]
        open_pair = allowed_pairs(ck_ref[pl.ds(start, KEY_TILE), :], code_q, start, (KEY_TILE, QUERY_TILE))
        bias = jnp.where(open_pair, 0.0, neg_fill)
        cols = [slice(h * QUERY_TILE, (h + 1) * QUERY_TILE) for h in range(nh)]
        scores = [nt_dot(keys, q_all[cols[h], :]) + bias for h in range(nh)]
        dps = [nt_dot(values, do_all[cols[h], :]) for h in range(nh)]
        ps = [jnp.exp(scores[h] - lse_ref[h : h + 1, :]) for h in range(nh)]
        dss = [(ps[h] * (dps[h] - deltas[h])).astype(jnp.bfloat16) for h in range(nh)]
        ps = [p.astype(jnp.bfloat16) for p in ps]
        for h in range(nh):
            rows = slice(h * HD, (h + 1) * HD)
            dqt_ref[rows, :] += nn_dot(kt_ref[rows, pl.ds(start, KEY_TILE)], dss[h])
        dv_acc[pl.ds(start, KEY_TILE), :] += nn_dot(jnp.concatenate(ps, axis=1), do_all)
        dk_acc[pl.ds(start, KEY_TILE), :] += nn_dot(jnp.concatenate(dss, axis=1), q_all)
        return 0
    lax.fori_loop(0, range_ref[step, 1], body, 0)
    dq_ref[...] = (dqt_ref[...] * HD ** (-0.5)).T.astype(jnp.bfloat16)
    @pl.when(step == pl.num_programs(0) - 1)
    def _():
        dk_ref[...] = dk_acc[...].astype(jnp.bfloat16)
        dv_ref[...] = dv_acc[...].astype(jnp.bfloat16)

def attention_backward(ranges, places, q, pieces, ctx, lse, k, v, code_q, code_k):
    cells, width = q.shape
    heads = width // HD

    def row():
        return pl.BlockSpec((QUERY_TILE, width), lambda i, *_: (i, 0))

    out = jax.ShapeDtypeStruct((cells, width), jnp.bfloat16)
    return pl.pallas_call(
        backward_kernel,
        out_shape=(out, out, out),
        grid_spec=pltpu.PrefetchScalarGridSpec(
            num_scalar_prefetch=2,
            grid=(cells // QUERY_TILE,),
            in_specs=[
                row(),
                row(),
                pl.BlockSpec((heads, QUERY_TILE), lambda i, *_: (0, i)),
                resident((cells, width)),
                resident((cells, width)),
                pl.BlockSpec((1, QUERY_TILE), lambda i, *_: (0, i)),
                resident((cells, 1)),
            ]
            + [resident(piece.shape) for piece in pieces],
            out_specs=[row(), resident((cells, width)), resident((cells, width))],
            scratch_shapes=[
                pltpu.VMEM((width, QUERY_TILE), jnp.float32),
                pltpu.VMEM((cells, width), jnp.float32),
                pltpu.VMEM((cells, width), jnp.float32),
                pltpu.VMEM((width, cells), jnp.bfloat16),
                pltpu.VMEM((cells, width), jnp.bfloat16),
            ],
        ),
        cost_estimate=nothing(),
        name="attention_backward",
    )(ranges, places, q, ctx, lse, k, v, code_q, code_k, *pieces)


def slide_tables(lengths_row, mask_all):
    cells = mask_all.shape[0]
    ends = jnp.cumsum(lengths_row)
    starts = ends - lengths_row
    slide = slide_index(jnp.arange(cells, dtype=jnp.int32), lengths_row)
    first = jnp.arange(cells // QUERY_TILE, dtype=jnp.int32) * QUERY_TILE
    first_slide = slide_index(first, lengths_row)
    last_slide = slide_index(first + (QUERY_TILE - 1), lengths_row)
    order = jnp.arange(lengths_row.shape[0], dtype=jnp.int32)

    def picked(table, index):
        return jnp.sum(jnp.where(index[:, None] == order[None, :], table[None, :], 0), axis=1)

    low = picked(starts, first_slide) // KEY_UNIT
    high = picked(ends, last_slide)
    tiles = (high - low * KEY_UNIT + KEY_TILE - 1) // KEY_TILE
    low = jnp.minimum(low, (cells - tiles * KEY_TILE) // KEY_UNIT)
    ranges = jnp.stack([low, tiles], axis=1).astype(jnp.int32)
    open_code = jnp.where(mask_all == 1, slide, -1)
    return ranges, slide[None, :], open_code[:, None]


def moved(value, target):
    groups, blocks = lax.axis_size("dp"), lax.axis_size("blk")
    pairs = []
    for g in range(groups):
        for b in range(blocks):
            there = target(g, b)
            if there is not None:
                pairs.append((g * blocks + b, there[0] * blocks + there[1]))
    return lax.ppermute(value, MESH_AXES, pairs)


def at_home(g, b):
    return (g & 1) == b >> (bits_of(lax.axis_size("blk")) - 1)


def head_block(g, b):
    return (b & (lax.axis_size("blk") // 2 - 1)) * 2 + (g & 1)


def worker_of(g, block_of_heads):
    half = lax.axis_size("blk") // 2
    return (g - g % 2) + block_of_heads % 2, (g % 2) * half + block_of_heads // 2


def owner_of(g, b, index):
    return (g - g % 2) + b // (lax.axis_size("blk") // 2), index


def pair_masks():
    return [1 << t for t in range(bits_of(lax.axis_size("blk")) - 1)]


def with_meta(cells, mask, lengths):
    count = lengths.shape[0]
    meta = jnp.concatenate([mask, lengths >> 7, lengths & 127]).astype(cells.dtype)
    meta = jnp.pad(meta, (0, cells.shape[1] - mask.shape[0] - 2 * count))
    return jnp.concatenate([cells, jnp.pad(meta[None], ((0, 7), (0, 0)))], axis=0)


def from_meta(meta, rows, count):
    meta = meta.astype(jnp.int32)
    high = meta[0, rows : rows + count]
    return meta[:, :rows].reshape(-1), high * 128 + meta[0, rows + count : rows + 2 * count]


def from_home(value):
    return moved(value, lambda g, b: (g ^ 1, b) if at_home(g, b) else None)


def paired(value, mask):
    return moved(value, lambda g, b: (g, b ^ mask) if at_home(g, b) else None)


def group_rows(own, use):
    blocks = lax.axis_size("blk")
    block = lax.axis_index("blk")
    mirror = moved(own, lambda g, b: None if at_home(g, b) else (g, blocks - 1 - b))
    held, rows = None, []
    for mirrored in (False, True):
        pieces = [(mirror if mirrored else own, 0)]
        for mask in pair_masks():
            pieces += [(paired(piece, mask), place ^ mask) for piece, place in pieces]
        pieces = [
            (piece, from_home(tied(piece, held) if mirrored and place else piece), blocks - 1 - (block ^ place) if mirrored else block ^ place)
            for piece, place in pieces
        ]
        held = use(pieces, held)
        rows += pieces
    return held, rows


def entry_kernel(count, place_ref, *refs):
    pieces, refs = refs[: 2 * count], refs[2 * count :]
    gain_ref, shift_ref = refs[:2]
    weights = refs[2:5]
    normed_ref, *out_refs = refs[-4:]
    step, home = pl.program_id(0), place_ref[count]
    rows = normed_ref.shape[0]
    for k in range(count):

        @pl.when(step == k)
        def _(k=k):
            value = jnp.where(home == 1, pieces[2 * k][:rows], pieces[2 * k + 1][:rows])
            unit, _ = norm_parts(value.astype(jnp.float32))
            normed_ref[...] = (unit * gain_ref[...] + shift_ref[...]).astype(jnp.bfloat16)

    for weight_ref, out_ref in zip(weights, out_refs):
        out_ref[...] = nn_dot(normed_ref[...], weight_ref[...]).astype(jnp.bfloat16)


def head_columns(weight):
    width = weight.shape[1] // lax.axis_size("blk")
    if width % 128 == 0:
        return weight, pl.BlockSpec((weight.shape[0], width), lambda i, place: (0, place[place.shape[0] - 1]))
    mine = head_block(lax.axis_index("dp"), lax.axis_index("blk")) * width
    return lax.dynamic_slice_in_dim(weight, mine, width, 1), resident((weight.shape[0], width))


def entry(pieces, gain, shift, weights, held):
    blocks, count = lax.axis_size("blk"), len(pieces)
    group, block = lax.axis_index("dp"), lax.axis_index("blk")
    rows, model = pieces[0][0].shape[0] - 8, pieces[0][0].shape[1]
    width = model // blocks
    home = at_home(group, block).astype(jnp.int32)
    table = jnp.stack([place for _, _, place in pieces] + [home, head_block(group, block)])
    narrow = pl.BlockSpec((rows, width), lambda i, place: (place[i], 0))
    shapes = [jax.ShapeDtypeStruct((blocks * rows, cols), jnp.bfloat16) for cols in (model,) + (width,) * 3]
    operands = [value for mine, other, _ in pieces for value in (mine, other)]
    specs = [resident(value.shape) for value in operands] + [resident((1, model))] * 2
    operands += [gain[None], shift[None]]
    for weight in weights:
        weight, spec = head_columns(weight)
        operands.append(weight)
        specs.append(spec)
    aliases = {}
    if held is not None:
        aliases = {1 + len(operands) + i: i for i in range(4)}
        operands += list(held)
        specs += [pl.BlockSpec(memory_space=pl.ANY)] * 4
    return pl.pallas_call(
        partial(entry_kernel, count),
        grid_spec=pltpu.PrefetchScalarGridSpec(
            num_scalar_prefetch=1,
            grid=(count,),
            in_specs=specs,
            out_specs=[pl.BlockSpec((rows, model), lambda i, place: (place[i], 0)), narrow, narrow, narrow],
        ),
        out_shape=shapes,
        input_output_aliases=aliases,
        cost_estimate=nothing(),
        name="entry",
    )(table, *operands)


def project_back_kernel(place_ref, normed_ref, dq_ref, dk_ref, dv_ref, wq_ref, wk_ref, wv_ref,
                        rows_ref, grad_ref, gain_ref, shift_ref, acc_ref, sum_ref):
    step = pl.program_id(0)
    width = dq_ref.shape[1]

    @pl.when(step == 0)
    def _():
        acc_ref[...] = jnp.zeros(acc_ref.shape, jnp.float32)
        sum_ref[...] = jnp.zeros(sum_ref.shape, jnp.float32)

    total = jnp.zeros(rows_ref.shape, jnp.float32)
    for kind, (grad, weight_ref) in enumerate(((dq_ref, wq_ref), (dk_ref, wk_ref), (dv_ref, wv_ref))):
        cols = slice(kind * width, (kind + 1) * width)
        total += nt_dot(grad[...], weight_ref[...])
        acc_ref[:, cols] += tn_dot(normed_ref[...], grad[...])
        sum_ref[:1, cols] += jnp.sum(grad[...].astype(jnp.float32), axis=0, keepdims=True)
    rows_ref[...] = total.astype(jnp.bfloat16)

    @pl.when(step == pl.num_programs(0) - 1)
    def _():
        grad_ref[...] = acc_ref[...].astype(jnp.bfloat16)
        gain = jnp.zeros((acc_ref.shape[0], width), jnp.float32)
        shift = jnp.zeros((acc_ref.shape[0], width), jnp.float32)
        for kind, weight_ref in enumerate((wq_ref, wk_ref, wv_ref)):
            cols = slice(kind * width, (kind + 1) * width)
            weight = weight_ref[...].astype(jnp.float32)
            gain += weight * acc_ref[:, cols]
            shift += weight * sum_ref[:1, cols]
        gain_ref[...] = lane_sums(gain)
        shift_ref[...] = lane_sums(shift)


def lane_sums(value):
    ones = jnp.ones((8, value.shape[1]), jnp.bfloat16)
    total = jnp.zeros((8, value.shape[0]), jnp.float32)
    for _ in range(3):
        part = value.astype(jnp.bfloat16)
        value = value - part.astype(jnp.float32)
        total += nt_dot(ones, part)
    return total


def project_back(normed, grads, weights):
    cells, width = grads[0].shape
    model = weights[0].shape[0]
    columns = [head_columns(weight) for weight in weights]
    table = head_block(lax.axis_index("dp"), lax.axis_index("blk"))[None]
    wide = pl.BlockSpec((ROW_TILE, model), lambda i, place: (i, 0))
    return pl.pallas_call(
        project_back_kernel,
        grid_spec=pltpu.PrefetchScalarGridSpec(
            num_scalar_prefetch=1,
            grid=(cells // ROW_TILE,),
            in_specs=[wide]
            + [pl.BlockSpec((ROW_TILE, width), lambda i, place: (i, 0))] * 3
            + [spec for _, spec in columns],
            out_specs=[wide, resident((model, 3 * width)), resident((8, model)), resident((8, model))],
            scratch_shapes=[pltpu.VMEM((model, 3 * width), jnp.float32), pltpu.VMEM((8, 3 * width), jnp.float32)],
        ),
        out_shape=[
            jax.ShapeDtypeStruct((cells, model), jnp.bfloat16),
            jax.ShapeDtypeStruct((model, 3 * width), jnp.bfloat16),
            jax.ShapeDtypeStruct((8, model), jnp.float32),
            jax.ShapeDtypeStruct((8, model), jnp.float32),
        ],
        cost_estimate=nothing(),
        name="project_back",
    )(table, normed, *grads, *[weight for weight, _ in columns])


def heads_at_owner():
    blocks, block = lax.axis_size("blk"), lax.axis_index("blk")
    return jnp.stack([(block - k) & (blocks - 1) for k in range(blocks)])


def rows_at_worker():
    blocks = lax.axis_size("blk")
    mine = head_block(lax.axis_index("dp"), lax.axis_index("blk"))
    return jnp.stack([(mine + k) & (blocks - 1) for k in range(blocks)])


def rows_to_owners(context):
    blocks = lax.axis_size("blk")
    places = rows_at_worker()
    rows = context.shape[0] // blocks
    return [
        moved(
            chunk(context, places[k] * rows, rows, 0),
            lambda g, b: owner_of(g, b, (head_block(g, b) + k) % blocks),
        )
        for k in range(blocks)
    ]


def heads_to_workers(pieces):
    blocks = lax.axis_size("blk")
    return [
        moved(piece, lambda g, b: worker_of(g, (b - k) % blocks)) for k, piece in enumerate(pieces)
    ]


def row_steps(partial_rows):
    blocks = lax.axis_size("blk")
    group, block = lax.axis_index("dp"), lax.axis_index("blk")
    rows = partial_rows.shape[0] // blocks
    home = at_home(group, block)
    (other,) = yield [partial_rows], lambda value: moved(
        value, lambda g, b: None if at_home(g, b) else (g ^ 1, b)
    )

    def taken(place):
        return [chunk(part, place * rows, rows, 0)[None] for part in (partial_rows, other)]

    mine = {r: (taken(block ^ r), taken(blocks - 1 - (block ^ r))) for r in range(blocks // 2)}
    for mask in reversed(pair_masks()):
        send = jnp.concatenate([summed(part) for r in range(mask) for part in mine[r + mask]], axis=0)
        (came,) = yield [send], lambda value, mask=mask: moved(
            value, lambda g, b: (g, b ^ mask) if at_home(g, b) else None
        )
        mine = {
            r: tuple(mine[r][k] + [came[2 * r + k : 2 * r + k + 1]] for k in range(2))
            for r in range(mask)
        }
    own, mirror = mine[0]
    (far,) = yield [summed(mirror)], lambda value: moved(
        value, lambda g, b: (g, blocks - 1 - b) if at_home(g, b) else None
    )
    return jnp.where(home, summed(own), far)[0]


def norm_parts(values):
    center = values - jnp.mean(values, axis=-1, keepdims=True)
    spread = jnp.mean(center * center, axis=-1, keepdims=True)
    scale = lax.rsqrt(spread + ln_eps)
    return center * scale, scale


def nothing():
    return pl.CostEstimate(flops=0, bytes_accessed=0, transcendentals=0)


def resident(shape):
    return pl.BlockSpec(shape, lambda *_: (0,) * len(shape))


def feed_kernel(head_ref, *refs):
    pieces = head_ref.shape[0]
    context_refs, (cell_ref, weight_ref), refs = refs[:pieces], refs[pieces : pieces + 2], refs[pieces + 2 :]
    context_ref, hidden_ref, refs = refs[6], refs[7], refs[:6] + refs[8:]

    @pl.when(pl.program_id(0) == 0)
    def _():
        width = weight_ref.shape[0] // pieces
        total = cell_ref[...].astype(jnp.float32)
        for k in range(pieces):
            begin = head_ref[k] * width
            piece = context_refs[k][...]
            total += nn_dot(piece, weight_ref[pl.ds(pl.multiple_of(begin, width), width), :])
            if width % 128 == 0:
                context_ref[:, pl.ds(pl.multiple_of(begin, width), width)] = piece
        hidden_ref[...] = total

    feed_body(hidden_ref, *refs)


def feed_body(hidden_ref, gain_ref, shift_ref, up_ref, up_bias_ref, down_ref, down_bias_ref,
                normed_ref, active_ref, slope_ref, two_ref, two_b_ref, acc_ref):
    step = pl.program_id(0)

    @pl.when(step == 0)
    def _():
        unit, _ = norm_parts(hidden_ref[...])
        normed_ref[...] = (unit * gain_ref[...] + shift_ref[...]).astype(jnp.bfloat16)
        acc_ref[...] = hidden_ref[...] + down_bias_ref[...]

    inner = nn_dot(normed_ref[...], up_ref[...]) + up_bias_ref[...]
    chance = 0.5 + 0.5 * lax.erf(inner * 2.0**-0.5)
    active = (inner * chance).astype(jnp.bfloat16)
    active_ref[...] = active
    slope = chance + inner * jnp.exp(-0.5 * inner * inner) * (2.0 * math.pi) ** -0.5
    slope_ref[...] = slope.astype(jnp.bfloat16)
    acc_ref[...] += nn_dot(active, down_ref[...])

    @pl.when(step == pl.num_programs(0) - 1)
    def _():
        two_ref[...] = acc_ref[...]
        two_b_ref[...] = acc_ref[...].astype(jnp.bfloat16)


def feed_forward(heads, contexts, cells, out_weight, gain, shift, up_weight, up_bias, down_weight, down_bias):
    rows, model = cells.shape
    inner = up_weight.shape[1]
    tile = FEED_TILE
    across = pl.BlockSpec((rows, tile), lambda j, heads: (0, j))
    return pl.pallas_call(
        feed_kernel,
        grid_spec=pltpu.PrefetchScalarGridSpec(
            num_scalar_prefetch=1,
            grid=(inner // tile,),
            in_specs=[resident(part.shape) for part in contexts]
            + [
                resident((rows, model)),
                resident((model, model)),
                resident((1, model)),
                resident((1, model)),
                pl.BlockSpec((model, tile), lambda j, heads: (0, j)),
                pl.BlockSpec((1, tile), lambda j, heads: (0, j)),
                pl.BlockSpec((tile, model), lambda j, heads: (j, 0)),
                resident((1, model)),
            ],
            out_specs=[
                resident((rows, model)),
                resident((rows, model)),
                resident((rows, model)),
                across,
                across,
                resident((rows, model)),
                resident((rows, model)),
            ],
            scratch_shapes=[pltpu.VMEM((rows, model), jnp.float32)],
        ),
        out_shape=[
            jax.ShapeDtypeStruct((rows, model), jnp.bfloat16),
            jax.ShapeDtypeStruct((rows, model), jnp.float32),
            jax.ShapeDtypeStruct((rows, model), jnp.bfloat16),
            jax.ShapeDtypeStruct((rows, inner), jnp.bfloat16),
            jax.ShapeDtypeStruct((rows, inner), jnp.bfloat16),
            jax.ShapeDtypeStruct((rows, model), jnp.float32),
            jax.ShapeDtypeStruct((rows, model), jnp.bfloat16),
        ],
        cost_estimate=nothing(),
        name="feed_forward",
    )(
        heads, *contexts, cells, out_weight, gain[None], shift[None], up_weight, up_bias[None], down_weight,
        down_bias[None],
    )


def feed_back_kernel(head_ref, two_ref, branch_ref, slope_ref, down_ref, up_ref, hidden_ref, gain_ref, weight_ref,
                     inner_ref, bias_ref, hidden_grad_ref, hidden_grad_b_ref, gain_grad_ref, shift_grad_ref,
                     *rest):
    piece_refs, acc_ref = rest[:-1], rest[-1]
    step = pl.program_id(0)

    @pl.when(step == 0)
    def _():
        acc_ref[...] = jnp.zeros(acc_ref.shape, jnp.float32)

    inner = (nt_dot(branch_ref[...], down_ref[...]) * slope_ref[...].astype(jnp.float32)).astype(jnp.bfloat16)
    inner_ref[...] = inner
    bias_ref[...] = jnp.sum(inner.astype(jnp.float32), axis=0, keepdims=True)
    acc_ref[...] += nt_dot(inner, up_ref[...])

    @pl.when(step == pl.num_programs(0) - 1)
    def _():
        unit, scale = norm_parts(hidden_ref[...])
        grad = acc_ref[...]
        gain_grad_ref[...] = jnp.sum(grad * unit, axis=0, keepdims=True)
        shift_grad_ref[...] = jnp.sum(grad, axis=0, keepdims=True)
        grad = grad * gain_ref[...]
        mean = jnp.mean(grad, axis=-1, keepdims=True)
        slant = jnp.mean(grad * unit, axis=-1, keepdims=True)
        total = two_ref[...] + scale * (grad - mean - unit * slant)
        hidden_grad_ref[...] = total
        total = total.astype(jnp.bfloat16)
        hidden_grad_b_ref[...] = total
        for k, piece_ref in enumerate(piece_refs):
            width = piece_ref.shape[1]
            begin = pl.multiple_of(head_ref[k] * width, width)
            piece_ref[...] = nt_dot(total, weight_ref[pl.ds(begin, width), :]).astype(jnp.bfloat16)


def feed_back(heads, grad_two, grad_branch, slope, down_weight, up_weight, hidden, gain, out_weight):
    rows, model = hidden.shape
    inner = up_weight.shape[1]
    tile = FEED_TILE
    count = heads.shape[0]
    return pl.pallas_call(
        feed_back_kernel,
        grid_spec=pltpu.PrefetchScalarGridSpec(
            num_scalar_prefetch=1,
            grid=(inner // tile,),
            in_specs=[
                resident((rows, model)),
                resident((rows, model)),
                pl.BlockSpec((rows, tile), lambda j, heads: (0, j)),
                pl.BlockSpec((tile, model), lambda j, heads: (j, 0)),
                pl.BlockSpec((model, tile), lambda j, heads: (0, j)),
                resident((rows, model)),
                resident((1, model)),
                resident((model, model)),
            ],
            out_specs=[
                pl.BlockSpec((rows, tile), lambda j, heads: (0, j)),
                pl.BlockSpec((1, tile), lambda j, heads: (0, j)),
                resident((rows, model)),
                resident((rows, model)),
                resident((1, model)),
                resident((1, model)),
            ]
            + [resident((rows, model // count))] * count,
            scratch_shapes=[pltpu.VMEM((rows, model), jnp.float32)],
        ),
        out_shape=[
            jax.ShapeDtypeStruct((rows, inner), jnp.bfloat16),
            jax.ShapeDtypeStruct((1, inner), jnp.float32),
            jax.ShapeDtypeStruct((rows, model), jnp.float32),
            jax.ShapeDtypeStruct((rows, model), jnp.bfloat16),
            jax.ShapeDtypeStruct((1, model), jnp.float32),
            jax.ShapeDtypeStruct((1, model), jnp.float32),
        ]
        + [jax.ShapeDtypeStruct((rows, model // count), jnp.bfloat16)] * count,
        cost_estimate=nothing(),
        name="feed_back",
    )(heads, grad_two, grad_branch, slope, down_weight, up_weight, hidden, gain[None], out_weight)


def tn_dot(left, right):
    return lax.dot_general(left, right, (((0,), (0,)), ((), ())), preferred_element_type=jnp.float32)


def weights_kernel(lefts_at, ready, place_ref, column_ref, *refs):
    count = len(lefts_at)
    scratch = 0 if ready else count
    lefts = refs[: max(lefts_at) + 1]
    rights = refs[len(lefts) : len(lefts) + count]
    refs, ordered = refs[len(lefts) + count : len(refs) - scratch], refs[len(refs) - scratch :]
    vector_ref, (keep_ref, send_ref) = refs[:-2], refs[-2:]
    held, grouped, _, width = keep_ref.shape
    if ready:
        ordered = rights
    else:

        @pl.when(pl.program_id(0) == 0)
        def _():
            for right_ref, ordered_ref in zip(rights, ordered):
                for piece in range(2 * held):
                    begin = pl.multiple_of(column_ref[piece] * width, width)
                    ordered_ref[:, piece * width : (piece + 1) * width] = right_ref[:, pl.ds(begin, width)]

    begin = 0
    for at, ordered_ref in zip(lefts_at, ordered):
        total = lefts[at].shape[1]
        tile = min(total, 256)
        rows = min(tile, total // grouped)
        for first in range(0, total, tile):
            value = tn_dot(lefts[at][:, first : first + tile], ordered_ref[...]).astype(jnp.bfloat16)
            for inside in range(0, tile, rows):
                z, row = divmod(first + inside, total // grouped)
                part = value[inside : inside + rows]
                place = slice(begin + row, begin + row + rows)
                for piece in range(held):
                    keep_ref[piece, z, place, :] = part[:, piece * width : (piece + 1) * width]
                    other = held + piece
                    send_ref[piece, z, place, :] = part[:, other * width : (other + 1) * width]
        begin += total // grouped

    if vector_ref:
        keep_ref[:, :, begin:, :] = vector_ref[0][0]
        send_ref[:, :, begin:, :] = vector_ref[0][1]


def relative_columns(value, steps):
    group = lax.axis_index("dp")
    masks = relative_masks(steps)
    size = value.shape[1] // len(masks)
    return jnp.concatenate([chunk(value, (group ^ mask) * size, size, 1) for mask in masks], axis=1)


def weight_pieces(pairs, steps, vector=None):
    blocks, block = lax.axis_size("blk"), lax.axis_index("blk")
    pieces, group = lax.axis_size("dp"), lax.axis_index("dp")
    width = D // pieces
    masks = relative_masks(blk_masks())
    sizes = [left.shape[1] // blocks for left, _, _ in pairs]
    places = jnp.stack([block ^ mask for mask in masks])
    columns = jnp.stack([group ^ mask for mask in relative_masks(steps)])
    cells = pairs[0][1].shape[0]
    lefts, lefts_at = [], []
    for left, _, _ in pairs:
        if not any(left is seen for seen in lefts):
            lefts.append(left)
        lefts_at.append(next(i for i, seen in enumerate(lefts) if left is seen))
    rights = [right for _, right, _ in pairs]
    parts = [part for _, _, part in pairs]
    grouped = max(1, 128 // min(sizes))
    ready = grouped > 1 or width % 128 != 0
    if ready:
        rights = [
            relative_columns(right[:, part * D : (part + 1) * D], steps) for right, part in zip(rights, parts)
        ]
        parts = [0] * len(parts)
        lefts = [
            jnp.concatenate(
                [chunk(left, (block ^ mask) * (left.shape[1] // blocks), left.shape[1] // blocks, 1) for mask in masks],
                axis=1,
            )
            for left in lefts
        ]
        places = jnp.arange(blocks, dtype=jnp.int32)
    rows = sum(sizes) + (0 if vector is None else vector.shape[3])
    out = pl.BlockSpec((pieces // 2, grouped, rows, width), lambda z, place, column: (0, z, 0, 0))
    specs = [
        pl.BlockSpec((cells, left.shape[1] // blocks * grouped), lambda z, place, column: (0, place[z]))
        for left in lefts
    ]
    specs += [pl.BlockSpec((cells, D), lambda z, place, column, part=part: (0, part)) for part in parts]
    operands = lefts + rights
    if vector is not None:
        specs.append(
            pl.BlockSpec(
                (2, pieces // 2, grouped, vector.shape[3], width), lambda z, place, column: (0, 0, z, 0, 0)
            )
        )
        operands.append(vector)
    shape = jax.ShapeDtypeStruct((pieces // 2, blocks, rows, width), jnp.bfloat16)
    return pl.pallas_call(
        partial(weights_kernel, lefts_at, ready),
        grid_spec=pltpu.PrefetchScalarGridSpec(
            num_scalar_prefetch=2,
            grid=(blocks // grouped,),
            in_specs=specs,
            out_specs=[out, out],
            scratch_shapes=[pltpu.VMEM((cells, D), jnp.bfloat16) for _ in pairs if not ready],
        ),
        out_shape=[shape, shape],
        cost_estimate=nothing(),
        name="weight_pieces",
    )(places, columns, *operands)


def weight_steps(keep, send, flipped, parts):
    steps = dp_order(flipped)
    (came,) = yield [send], by_mask(steps[0], 0)
    size = keep.shape[0]
    terms = [[keep[place], came[place]] for place in range(size)]
    for mask in steps[1:]:
        size = size // 2
        came = yield [summed(terms[place]) for place in range(size, 2 * size)], by_mask(mask, 0)
        terms = [terms[place] + [came[place]] for place in range(size)]
    terms = terms[0]
    size = keep.shape[1]
    for mask in blk_masks():
        size = size // 2
        (came,) = yield [summed([term[size : 2 * size] for term in terms])], by_mask(0, mask)
        terms = [term[:size] for term in terms] + [came]
    value = summed(terms)
    for mask in steps[:0:-1]:
        (came,) = yield [value], by_mask(mask, 0)
        value = jnp.concatenate([value, came], axis=0)
    (came,) = yield [value], by_mask(steps[0], 0)
    return spread_columns(value, came, relative_table(steps, lax.axis_index("dp")), parts)


def local(
    cell_states,
    slide_lengths,
    cell_mask,
    latent_noise,
    train_step,
    attn_gain,
    attn_shift,
    query_weight,
    key_weight,
    value_weight,
    out_weight,
    ffn_gain,
    ffn_shift,
    up_weight,
    up_bias,
    down_weight,
    down_bias,
    encode_weight,
    encode_bias,
    decode_weight,
    prior_means,
    prior_logits,
    out_grad,
):
    rows_here = cell_states.shape[0]
    blocks = lax.axis_size("blk")
    group, block = lax.axis_index("dp"), lax.axis_index("blk")
    width = D // blocks
    x_float = cell_states.astype(jnp.float32)
    _, norm_back = jax.vjp(layer_norm, x_float, attn_gain, attn_shift)
    weights = (query_weight, key_weight, value_weight)
    held, pieces = group_rows(
        with_meta(cell_states, cell_mask, slide_lengths[0]),
        lambda pieces, held: entry(pieces, attn_gain, attn_shift, weights, held),
    )
    normed_b, queries, keys, values = held
    meta = jnp.zeros((blocks, D), jnp.bfloat16)
    order = jnp.arange(blocks, dtype=jnp.int32)
    for mine, other, place in pieces:
        row = jnp.where(at_home(group, block), mine[rows_here], other[rows_here])
        meta = jnp.where(order[:, None] == place, row[None], meta)
    mask_all, lengths_row = from_meta(meta, rows_here, slide_lengths.shape[1])
    ranges, query_code, key_code = slide_tables(lengths_row, mask_all)
    context_here, log_total = attention_forward(ranges, queries, keys, values, query_code, key_code)
    contexts = rows_to_owners(context_here)
    owner_heads = heads_at_owner()
    context_b, hidden, normed_two_b, activated_b, slope_b, hidden_two, hidden_two_b = feed_forward(
        owner_heads, contexts, cell_states, out_weight, ffn_gain, ffn_shift, up_weight, up_bias, down_weight,
        down_bias,
    )
    if width % 128:
        context_b = jnp.zeros((rows_here, D), jnp.bfloat16)
        for k in range(blocks):
            context_b = lax.dynamic_update_slice_in_dim(context_b, contexts[k], owner_heads[k] * width, 1)
    encoded = plain_dot(hidden_two_b, encode_weight) + encode_bias
    latent_mean = encoded[:, :LAT]
    latent_logvar = encoded[:, LAT:]
    spread = jnp.exp(0.5 * latent_logvar)
    noise_float = latent_noise.astype(jnp.float32)
    latent_b = (latent_mean + spread * noise_float).astype(jnp.bfloat16)
    output = hidden_two + plain_dot(latent_b, decode_weight)
    (kl_dim, categorical), kl_back = jax.vjp(
        kl_terms, latent_mean, latent_logvar, prior_means, prior_logits
    )
    real = cell_mask.astype(jnp.float32)
    sums = jnp.concatenate(
        [
            jnp.sum(kl_dim * real[:, None], axis=0),
            jnp.sum(categorical * real)[None],
            jnp.sum(real)[None],
            jnp.zeros((126,), jnp.float32),
        ]
    )
    sums = summed_everywhere(sums)
    kl_sum, cat_sum, count = sums[:LAT], sums[LAT], sums[LAT + 1]
    kbar = kl_sum / count
    floored = jnp.sum(jnp.maximum(kbar, free_floor))
    cat_mean = cat_sum / count
    beta = jnp.minimum(1.0, (train_step[0].astype(jnp.float32) + 1.0) / WARM)
    active = (kbar > free_floor).astype(jnp.float32)
    grad_latent = cols_dot(out_grad, decode_weight)
    grad_mean, grad_logvar, grad_means, grad_prior = kl_back(
        (beta * real[:, None] * active[None, :], beta * real)
    )
    grad_mean = grad_mean + grad_latent
    grad_logvar = grad_logvar + grad_latent * 0.5 * spread * noise_float
    grad_encoded_b = jnp.concatenate([grad_mean, grad_logvar], axis=1).astype(jnp.bfloat16)
    grad_encode_bias = jnp.sum(grad_encoded_b.astype(jnp.float32), axis=0)
    grad_two = out_grad.astype(jnp.float32) + cols_dot(grad_encoded_b, encode_weight)
    grad_down_bias = jnp.sum(grad_two, axis=0)
    grad_branch_b = grad_two.astype(jnp.bfloat16)

    straight, flipped = dp_order(False), dp_order(True)
    block_rows = D // blocks
    down = Exchange(
        weight_steps(
            *weight_pieces(
                [(activated_b, grad_branch_b, 0), (hidden_two_b, grad_encoded_b, 0), (latent_b, out_grad, 0)],
                straight,
            ),
            False,
            [(4 * block_rows, 1), (block_rows, 1), (block_rows // 2, 1)],
        )
    )
    back = feed_back(
        owner_heads, grad_two, tied(grad_branch_b, down.last), slope_b, down_weight, up_weight, hidden, ffn_gain,
        out_weight,
    )
    grad_inner_b, grad_up_bias, grad_hidden, grad_attn_b, grad_ffn_gain, grad_ffn_shift = back[:6]
    grads_here = heads_to_workers(back[6:])
    by_block = lambda part: part.reshape(blocks, -1)
    means_block = jnp.moveaxis(grad_means.reshape(K, blocks, LAT // blocks), 1, 0)
    vectors = [
        by_block(grad_ffn_gain),
        by_block(grad_ffn_shift),
        by_block(grad_up_bias),
        by_block(grad_down_bias),
        by_block(grad_encode_bias),
        by_block(means_block),
        by_block(grad_prior),
    ]
    sizes = [part.shape[1] for part in vectors]
    vector = jnp.concatenate([part.astype(jnp.bfloat16) for part in vectors], axis=1)
    vector_rows = -(-sum(sizes) // (8 * D)) * 8
    vector = jnp.pad(vector, ((0, 0), (0, vector_rows * D - sum(sizes))))
    vector = relative_columns(vector.reshape(blocks * vector_rows, D), flipped)
    devices_along = lax.axis_size("dp")
    vector = vector.reshape(blocks, vector_rows, 2, devices_along // 2, D // devices_along)
    vector = jnp.transpose(vector, (2, 3, 0, 1, 4))
    vector = jnp.concatenate([chunk(vector, block ^ mask, 1, 2) for mask in relative_masks(blk_masks())], axis=2)
    up_pieces = weight_pieces(
        [(normed_two_b, tied(grad_inner_b, back[6:]), part) for part in range(4)] + [(context_b, grad_attn_b, 0)],
        flipped,
        vector,
    )
    up = Exchange(
        weight_steps(
            *tied(up_pieces, grads_here), True, [(block_rows, 4), (block_rows, 1), (vector_rows, 1)]
        )
    )
    token = down.advance(up.last, hold=True)
    token = up.advance(token, hold=True)
    grads = attention_backward(
        ranges, rows_at_worker(), tied(queries, token), grads_here, context_here, log_total, keys, values, query_code,
        key_code,
    )
    grads = tied(grads, (down.flight, up.flight))
    down.release(grads[0])
    up.release(grads[0])
    partial_rows, grad_heads, part_gain, part_shift = project_back(normed_b, grads, weights)
    partial_rows, grad_heads = tied((partial_rows, grad_heads), (down.flight, up.flight))
    row_sum = Exchange(row_steps(partial_rows))
    part_shift = part_shift[0]
    part_gain = (part_gain[0] - attn_shift * part_shift) / attn_gain
    token = up.advance(grad_heads)
    token = down.advance(token)
    extra = jnp.concatenate([by_block(part_gain), by_block(part_shift)], axis=1)
    extra_size = extra.shape[1]
    extra = jnp.pad(extra, ((0, 0), (0, 3 * width - extra_size))).astype(jnp.bfloat16)
    pieces = lax.axis_size("dp") // 2
    piece_rows = block_rows // pieces
    grad_heads = grad_heads.reshape(blocks, pieces, piece_rows, 3 * width)
    extra = jnp.broadcast_to(extra[:, None, None, :], (blocks, pieces, 8, 3 * width))
    attn = Exchange(head_steps(jnp.concatenate([grad_heads, extra], axis=2)))
    token = attn.last
    order = [row_sum, attn, down, row_sum, up, attn]
    live = [down, row_sum, up, attn]
    for bundle in order:
        token = bundle.advance(token)
    while any(bundle.result is None for bundle in live):
        for bundle in live:
            if bundle.result is None:
                token = bundle.advance(token)
    grad_normed = row_sum.result.astype(jnp.float32)
    grad_from_norm, _, _ = norm_back(grad_normed)
    states_grad = grad_hidden + grad_from_norm
    mine, other = attn.result
    attn_vector = jnp.sum((mine[0].astype(jnp.float32) + other[0].astype(jnp.float32)), axis=0)[piece_rows]
    main = spread_heads(mine, other, piece_rows)
    down_sum, encode_sum, decode_sum = down.result
    up_sum, out_sum, vector_sum = up.result
    flat = vector_sum.reshape(-1)
    small, begin = [], 0
    for size in sizes:
        small.append(flat[begin : begin + size])
        begin += size
    totals = (
        attn_vector[: extra_size // 2],
        attn_vector[extra_size // 2 : extra_size],
        main[0],
        main[1],
        main[2],
        out_sum,
        small[0],
        small[1],
        up_sum,
        small[2],
        down_sum,
        small[3],
        encode_sum,
        small[4],
        decode_sum,
        small[5].reshape(K, LAT // blocks),
        small[6],
    )
    kl_out = (floored / LAT + cat_mean).reshape(1)
    return (output.astype(jnp.bfloat16), states_grad, kl_out) + tuple(totals)


def solution(mesh):
    in_specs = (
        P(("dp", "blk"), None),
        P("dp", None),
        P(("dp", "blk")),
        P(("dp", "blk"), None),
        P(),
        P(),
        P(),
        P(),
        P(),
        P(),
        P(),
        P(),
        P(),
        P(),
        P(),
        P(),
        P(),
        P(),
        P(),
        P(),
        P(),
        P(),
        P(("dp", "blk"), None),
    )
    out_specs = (
        P(("dp", "blk"), None),
        P(("dp", "blk"), None),
        P(),
        P("blk"),
        P("blk"),
        P("blk", None),
        P("blk", None),
        P("blk", None),
        P("blk", None),
        P("blk"),
        P("blk"),
        P("blk", None),
        P("blk"),
        P("blk", None),
        P("blk"),
        P("blk", None),
        P("blk"),
        P("blk", None),
        P(None, "blk"),
        P("blk"),
    )
    return jax.shard_map(local, mesh=mesh, in_specs=in_specs, out_specs=out_specs, check_vma=False)
```
